32 devices in a mesh: gx: 16 (over z, y, core), gy: 2 (over x).
Axes of the slice: x: 2, y: 2, z: 4, core: 2. Of those that a mesh axis runs over, the one named last changes fastest.
Arguments:
- forcing: float32 [128, 16, 128], P('gx', 'gy'), may hold values from -12 to 12
- kappa: float32 [16, 2, 16], P('gx', 'gy'), may hold values from 0.25 to 4
- sigma: float32 [16, 2, 16], P('gx', 'gy'), may hold values from 0.5 to 8
Outputs:
- solution: float32 [128, 16, 128], P('gx', 'gy')
- residual: float32 [128, 16, 128], P('gx', 'gy')
- rel_residual: float32 [], replicated
The draws below stay inside these ranges and needn't reach their ends.
All inputs are finite; a program needn't handle non-finite values.
Results may differ from the reference program's by a relative error of at most 0.0003.
Values sent between devices are 32-bit elements; how exact they have to be, the bound alone decides.
No kernel may reach another device: no remote copies, remote signals or barrier semaphores. Data moves between devices by JAX's collectives and lax.ppermute only.
A program may use at most 64 MiB of HBM per device.

```python
import math
import jax
import jax.numpy as jnp
import numpy as np
from jax import lax

FINE = 8
EZ = 16
NEX = 16
NEY = 2
NODES_X = 128
NODES_Y = 16
NODES_Z = 128


def draw_forcing(key, part):
    keys = jax.random.split(key, 2)
    shape = (NODES_X, NODES_Y, NODES_Z)
    cells = (NODES_X // FINE, NODES_Y // FINE, NODES_Z // FINE)
    level = 10.0 ** jax.random.uniform(keys[1], cells, jnp.float32)
    level = jnp.repeat(jnp.repeat(jnp.repeat(level, FINE, 0), FINE, 1), FINE, 2)
    across = (jnp.arange(NODES_X, dtype=jnp.float32) / NODES_X)[:, None, None]
    rough = jnp.clip(jax.random.normal(keys[0], shape, jnp.float32), -4.0, 4.0)
    values = 0.1 * rough * level * 3.0 ** across
    return values.astype(jnp.float32)


def steps_of(rng, extent, pieces, least, largest):
    level, own = 1.0, jax.random.fold_in(rng, 6)
    for dim, parts in pieces:
        steps = jnp.exp(jax.random.uniform(jax.random.fold_in(own, dim), (parts,), jnp.float32, least / len(pieces), largest / len(pieces)))
        level = level * jnp.repeat(steps, extent[dim] // parts).reshape([-1 if axis == dim else 1 for axis in range(len(extent))])
    return level


def setup_inputs(seed: int = 0) -> dict:
    key_list = jax.random.split(jax.random.key(seed), 4)
    forcing = draw_forcing(jax.random.fold_in(key_list[3], 71), 0)
    kappa = jnp.clip(jnp.exp(math.log(4.0) - 2.7725887 * jax.random.uniform(key_list[1], (NEX, NEY, EZ), jnp.float32) ** steps_of(key_list[1], (NEX, NEY, EZ), ((0, 16), (1, 2)), -0.2, 0.2)), 0.25, 4.0)
    sigma = jnp.clip(jnp.exp(math.log(8.0) - 2.7725887 * jax.random.uniform(key_list[2], (NEX, NEY, EZ), jnp.float32) ** steps_of(key_list[2], (NEX, NEY, EZ), ((0, 16), (1, 2)), -0.2, 0.2)), 0.5, 8.0)
    return dict(forcing=forcing, kappa=kappa, sigma=sigma)


def legendre_table(points, order):
    columns = [points * 0.0 + 1.0, points]
    for degree in range(2, order + 1):
        columns.append(((2 * degree - 1) * points * columns[-1] - (degree - 1) * columns[-2]) / degree)
    return np.stack(columns, axis=1)

def lobatto(count):
    order = count - 1
    points = np.cos(np.pi * np.arange(count) / order)
    for sweep in range(60):
        table = legendre_table(points, order)
        points = points - (points * table[:, order] - table[:, order - 1]) / (count * table[:, order])
    table = legendre_table(points, order)
    weights = 2.0 / (order * count * table[:, order] ** 2)
    values = table[:, order]
    points, weights, values = (points[::-1], weights[::-1], values[::-1])
    spread = points[:, None] - points[None, :] + np.eye(count)
    deriv = values[:, None] / values[None, :] / spread * (1.0 - np.eye(count))
    corner = order * (order + 1) / 4.0
    ends = np.array([-corner] + [0.0] * (count - 2) + [corner])
    return (points, weights, deriv + np.eye(count) * ends[None, :])

def lagrange(fine_points, coarse_points):
    columns = []
    for column in range(len(coarse_points)):
        value = fine_points * 0.0 + 1.0
        for other in range(len(coarse_points)):
            if other != column:
                value = value * (fine_points - coarse_points[other]) / (coarse_points[column] - coarse_points[other])
        columns.append(value)
    return np.stack(columns, axis=1)

def edge_factor(count, blocks):
    index = jnp.arange(count)
    single = jnp.where((index == 0) | (index == count - 1), 0.5, 1.0).astype(jnp.float32)
    return jnp.tile(single, blocks)

def multiplicity(count, blocks):
    first = edge_factor(count, blocks[0])
    second = edge_factor(count, blocks[1])
    third = edge_factor(count, blocks[2])
    return first[:, None, None] * second[None, :, None] * third[None, None, :]

def element_apply(field, kappa, sigma, deriv, weights):
    count = deriv.shape[0]
    ex, ey, ez = kappa.shape
    high = lax.Precision.HIGHEST
    block = field.reshape(ex, count, ey, count, ez, count)
    mass = (weights[:, None, None] * weights[None, :, None] * weights[None, None, :])[None, :, None, :, None, :]
    first = jnp.einsum('ai,eifjgk->eafjgk', deriv, block, precision=high)
    total = jnp.einsum('ai,eafjgk->eifjgk', deriv, first * mass, precision=high)
    second = jnp.einsum('aj,eifjgk->eifagk', deriv, block, precision=high)
    total = total + jnp.einsum('aj,eifagk->eifjgk', deriv, second * mass, precision=high)
    third = jnp.einsum('ak,eifjgk->eifjga', deriv, block, precision=high)
    total = total + jnp.einsum('ak,eifjga->eifjgk', deriv, third * mass, precision=high)
    coeff = kappa[:, None, :, None, :, None]
    shift = sigma[:, None, :, None, :, None]
    return (coeff * total + shift * mass * block).reshape(field.shape)

def element_diagonal(kappa, sigma, deriv, weights):
    count = deriv.shape[0]
    ex, ey, ez = kappa.shape
    stiff = lax.optimization_barrier(jnp.sum(deriv * deriv * weights[:, None], axis=0))
    term = stiff[:, None, None] * weights[None, :, None] * weights[None, None, :]
    term = term + weights[:, None, None] * stiff[None, :, None] * weights[None, None, :]
    term = term + weights[:, None, None] * weights[None, :, None] * stiff[None, None, :]
    mass = weights[:, None, None] * weights[None, :, None] * weights[None, None, :]
    coeff = kappa[:, None, :, None, :, None]
    shift = sigma[:, None, :, None, :, None]
    full = coeff * term[None, :, None, :, None, :] + shift * mass[None, :, None, :, None, :]
    return full.reshape(ex * count, ey * count, ez * count)

def fold_axis(field, dim, count):
    size = field.shape[dim]
    position = jnp.arange(size) % count
    shape = [1, 1, 1]
    shape[dim] = size
    first = (position == 0).reshape(shape)
    last = (position == count - 1).reshape(shape)
    before = jnp.roll(field, 1, dim)
    after = jnp.roll(field, -1, dim)
    return field + jnp.where(first, before, 0.0) + jnp.where(last, after, 0.0)

def assemble(field, count):
    return fold_axis(fold_axis(fold_axis(field, 0, count), 1, count), 2, count)

def restrict(field, interp, blocks, fine_count, coarse_count):
    high = lax.Precision.HIGHEST
    block = field.reshape(blocks[0], fine_count, blocks[1], fine_count, blocks[2], fine_count)
    one = jnp.einsum('ia,eifjgk->eafjgk', interp, block, precision=high)
    two = jnp.einsum('jb,eafjgk->eafbgk', interp, one, precision=high)
    three = jnp.einsum('kc,eafbgk->eafbgc', interp, two, precision=high)
    return three.reshape(blocks[0] * coarse_count, blocks[1] * coarse_count, blocks[2] * coarse_count)

def prolong(field, interp, blocks, fine_count, coarse_count):
    high = lax.Precision.HIGHEST
    block = field.reshape(blocks[0], coarse_count, blocks[1], coarse_count, blocks[2], coarse_count)
    one = jnp.einsum('ia,eafbgc->eifbgc', interp, block, precision=high)
    two = jnp.einsum('jb,eifbgc->eifjgc', interp, one, precision=high)
    three = jnp.einsum('kc,eifjgc->eifjgk', interp, two, precision=high)
    return three.reshape(blocks[0] * fine_count, blocks[1] * fine_count, blocks[2] * fine_count)

def reference(forcing, kappa, sigma):
    blocks = kappa.shape
    counts = [8, 4, 2]
    tables = [lobatto(count) for count in counts]
    derivs = [jnp.asarray(table[2], jnp.float32) for table in tables]
    weights = [jnp.asarray(table[1], jnp.float32) for table in tables]
    interps = [jnp.asarray(lagrange(tables[level][0], tables[level + 1][0]), jnp.float32) for level in range(2)]
    mults = [multiplicity(count, blocks) for count in counts]
    diags = [assemble(element_diagonal(kappa, sigma, derivs[level], weights[level]), counts[level]) for level in range(3)]
    center = 1.65
    half = 1.35
    ratio = center / half

    def operate(field, level):
        return assemble(element_apply(field, kappa, sigma, derivs[level], weights[level]), counts[level])

    def smooth(resid, level, steps, keep_last):
        rho = 1.0 / ratio
        direction = resid / (center * diags[level])
        iterate = direction
        for step in range(steps):
            if step > 0:
                rho_next = 1.0 / (2.0 * ratio - rho)
                direction = rho_next * rho * direction + 2.0 * rho_next / half * resid / diags[level]
                iterate = iterate + direction
                rho = rho_next
            if step < steps - 1 or keep_last:
                resid = resid - operate(direction, level)
        return (iterate, resid)

    def vcycle(resid, level):
        if level == 2:
            iterate, unused = smooth(resid, level, 2, False)
            return iterate
        iterate, resid = smooth(resid, level, 2, True)
        coarse = assemble(restrict(mults[level] * resid, interps[level], blocks, counts[level], counts[level + 1]), counts[level + 1])
        correction = prolong(vcycle(coarse, level + 1), interps[level], blocks, counts[level], counts[level + 1])
        iterate = iterate + correction
        resid = resid - operate(correction, level)
        return iterate + resid / (center * diags[level])
    load = assemble(forcing, 8)
    first = vcycle(load, 0)
    image_first = operate(first, 0)
    second = vcycle(load - image_first, 0)
    combined = first + second
    image = operate(combined, 0)
    weight = mults[0]
    coef = jnp.sum(weight * load * image) / jnp.sum(weight * image * image)
    solution = coef * combined
    residual = load - coef * image
    rel_residual = jnp.sqrt(jnp.sum(weight * residual * residual) / jnp.sum(weight * load * load))
    return (solution, residual, rel_residual)
```

```python
import jax
import jax.numpy as jnp
import numpy as np
from jax import lax
from jax.experimental import pallas as pl
from jax.experimental.pallas import tpu as pltpu
from jax.sharding import PartitionSpec as P


def with_halo(cells, sides, width):
    for axis, dim in sides:
        count = lax.axis_size(axis)
        head = lax.slice_in_dim(cells, 0, width, axis=dim)
        tail = lax.slice_in_dim(cells, cells.shape[dim] - width, cells.shape[dim], axis=dim)
        cells = jnp.concatenate(
            [
                lax.ppermute(tail, axis, [(i, (i + 1) % count) for i in range(count)]),
                cells,
                lax.ppermute(head, axis, [((i + 1) % count, i) for i in range(count)]),
            ],
            axis=dim,
        )
    return cells


def legendre_table(points, order):
    columns = [points * 0.0 + 1.0, points]
    for degree in range(2, order + 1):
        columns.append(
            ((2 * degree - 1) * points * columns[-1] - (degree - 1) * columns[-2]) / degree
        )
    return np.stack(columns, axis=1)


def lobatto(count):
    order = count - 1
    points = np.cos(np.pi * np.arange(count) / order)
    for sweep in range(60):
        table = legendre_table(points, order)
        points = points - (points * table[:, order] - table[:, order - 1]) / (
            count * table[:, order]
        )
    table = legendre_table(points, order)
    weights = 2.0 / (order * count * table[:, order] ** 2)
    values = table[:, order]
    points, weights, values = (points[::-1], weights[::-1], values[::-1])
    spread = points[:, None] - points[None, :] + np.eye(count)
    deriv = values[:, None] / values[None, :] / spread * (1.0 - np.eye(count))
    corner = order * (order + 1) / 4.0
    ends = np.array([-corner] + [0.0] * (count - 2) + [corner])
    return (points, weights, deriv + np.eye(count) * ends[None, :])


def lagrange(fine_points, coarse_points):
    columns = []
    for column in range(len(coarse_points)):
        value = fine_points * 0.0 + 1.0
        for other in range(len(coarse_points)):
            if other != column:
                value = (
                    value
                    * (fine_points - coarse_points[other])
                    / (coarse_points[column] - coarse_points[other])
                )
        columns.append(value)
    return np.stack(columns, axis=1)


def edge_factor(count, blocks):
    index = jnp.arange(count)
    single = jnp.where((index == 0) | (index == count - 1), 0.5, 1.0).astype(jnp.float32)
    return jnp.tile(single, blocks)


def multiplicity(count, blocks):
    first = edge_factor(count, blocks[0])
    second = edge_factor(count, blocks[1])
    third = edge_factor(count, blocks[2])
    return first[:, None, None] * second[None, :, None] * third[None, None, :]


def element_apply(field, kappa, sigma, deriv, weights):
    count = deriv.shape[0]
    ex, ey, ez = kappa.shape
    high = lax.Precision.HIGHEST
    block = field.reshape(ex, count, ey, count, ez, count)
    mass = (weights[:, None, None] * weights[None, :, None] * weights[None, None, :])[
        None, :, None, :, None, :
    ]
    first = jnp.einsum("ai,eifjgk->eafjgk", deriv, block, precision=high)
    total = jnp.einsum("ai,eafjgk->eifjgk", deriv, first * mass, precision=high)
    second = jnp.einsum("aj,eifjgk->eifagk", deriv, block, precision=high)
    total = total + jnp.einsum("aj,eifagk->eifjgk", deriv, second * mass, precision=high)
    third = jnp.einsum("ak,eifjgk->eifjga", deriv, block, precision=high)
    total = total + jnp.einsum("ak,eifjga->eifjgk", deriv, third * mass, precision=high)
    coeff = kappa[:, None, :, None, :, None]
    shift = sigma[:, None, :, None, :, None]
    return (coeff * total + shift * mass * block).reshape(field.shape)


def element_diagonal(kappa, sigma, deriv, weights):
    count = deriv.shape[0]
    ex, ey, ez = kappa.shape
    stiff = jnp.sum(deriv * deriv * weights[:, None], axis=0)
    term = stiff[:, None, None] * weights[None, :, None] * weights[None, None, :]
    term = term + weights[:, None, None] * stiff[None, :, None] * weights[None, None, :]
    term = term + weights[:, None, None] * weights[None, :, None] * stiff[None, None, :]
    mass = weights[:, None, None] * weights[None, :, None] * weights[None, None, :]
    coeff = kappa[:, None, :, None, :, None]
    shift = sigma[:, None, :, None, :, None]
    full = coeff * term[None, :, None, :, None, :] + shift * mass[None, :, None, :, None, :]
    return full.reshape(ex * count, ey * count, ez * count)


def fold_axis(field, dim, count):
    size = field.shape[dim]
    position = jnp.arange(size) % count
    shape = [1, 1, 1]
    shape[dim] = size
    first = (position == 0).reshape(shape)
    last = (position == count - 1).reshape(shape)
    before = jnp.roll(field, 1, dim)
    after = jnp.roll(field, -1, dim)
    return field + jnp.where(first, before, 0.0) + jnp.where(last, after, 0.0)


def fold_padded(padded, dim, count):
    size = padded.shape[dim] - 2
    center = lax.slice_in_dim(padded, 1, size + 1, axis=dim)
    before = lax.slice_in_dim(padded, 0, size, axis=dim)
    after = lax.slice_in_dim(padded, 2, size + 2, axis=dim)
    position = jnp.arange(size) % count
    shape = [1, 1, 1]
    shape[dim] = size
    first = (position == 0).reshape(shape)
    last = (position == count - 1).reshape(shape)
    return center + jnp.where(first, before, 0.0) + jnp.where(last, after, 0.0)


def assemble(field, count, finest):
    if finest:
        padded = with_halo(field, (("gx", 0), ("gy", 1)), 1)
        field = fold_padded(fold_padded(padded, 0, count), 1, count)
    else:
        padded = with_halo(field, (("gx", 0), ("gy", 1)), 1)
        field = fold_padded(fold_padded(padded, 0, count), 1, count)
    return fold_axis(field, 2, count)


def restrict(field, interp, blocks, fine_count, coarse_count):
    high = lax.Precision.HIGHEST
    block = field.reshape(blocks[0], fine_count, blocks[1], fine_count, blocks[2], fine_count)
    one = jnp.einsum("ia,eifjgk->eafjgk", interp, block, precision=high)
    two = jnp.einsum("jb,eafjgk->eafbgk", interp, one, precision=high)
    three = jnp.einsum("kc,eafbgk->eafbgc", interp, two, precision=high)
    return three.reshape(
        blocks[0] * coarse_count, blocks[1] * coarse_count, blocks[2] * coarse_count
    )


def prolong(field, interp, blocks, fine_count, coarse_count):
    high = lax.Precision.HIGHEST
    block = field.reshape(blocks[0], coarse_count, blocks[1], coarse_count, blocks[2], coarse_count)
    one = jnp.einsum("ia,eafbgc->eifbgc", interp, block, precision=high)
    two = jnp.einsum("jb,eifbgc->eifjgc", interp, one, precision=high)
    three = jnp.einsum("kc,eifjgc->eifjgk", interp, two, precision=high)
    return three.reshape(blocks[0] * fine_count, blocks[1] * fine_count, blocks[2] * fine_count)


def distributed(forcing, kappa, sigma):
    blocks = kappa.shape
    counts = [8, 4, 2]
    tables = [lobatto(count) for count in counts]
    derivs = [jnp.asarray(table[2], jnp.float32) for table in tables]
    weights = [jnp.asarray(table[1], jnp.float32) for table in tables]
    interps = [
        jnp.asarray(lagrange(tables[level][0], tables[level + 1][0]), jnp.float32)
        for level in range(2)
    ]
    mults = [multiplicity(count, blocks) for count in counts]
    diags = [
        assemble(
            element_diagonal(kappa, sigma, derivs[level], weights[level]), counts[level], level == 0
        )
        for level in range(3)
    ]
    center = 1.65
    half = 1.35
    ratio = center / half

    def operate(field, level):
        return assemble(
            element_apply(field, kappa, sigma, derivs[level], weights[level]),
            counts[level],
            level == 0,
        )

    def smooth(resid, level, steps, keep_last):
        rho = 1.0 / ratio
        direction = resid / (center * diags[level])
        iterate = direction
        for step in range(steps):
            if step > 0:
                rho_next = 1.0 / (2.0 * ratio - rho)
                direction = (
                    rho_next * rho * direction + 2.0 * rho_next / half * resid / diags[level]
                )
                iterate = iterate + direction
                rho = rho_next
            if step < steps - 1 or keep_last:
                resid = resid - operate(direction, level)
        return (iterate, resid)

    def vcycle(resid, level):
        if level == 2:
            iterate, unused = smooth(resid, level, 2, False)
            return iterate
        iterate, resid = smooth(resid, level, 2, True)
        coarse = assemble(
            restrict(
                mults[level] * resid, interps[level], blocks, counts[level], counts[level + 1]
            ),
            counts[level + 1],
            False,
        )
        correction = prolong(
            vcycle(coarse, level + 1), interps[level], blocks, counts[level], counts[level + 1]
        )
        iterate = iterate + correction
        resid = resid - operate(correction, level)
        return iterate + resid / (center * diags[level])

    load = assemble(forcing, 8, True)
    first = vcycle(load, 0)
    image_first = operate(first, 0)
    second = vcycle(load - image_first, 0)
    combined = first + second
    image = operate(combined, 0)
    weight = mults[0]
    load_sq, load_image, image_sq = lax.psum(
        (
            jnp.sum(weight * load * load),
            jnp.sum(weight * load * image),
            jnp.sum(weight * image * image),
        ),
        ("gx", "gy"),
    )
    coef = load_image / image_sq
    solution = coef * combined
    residual = load - coef * image
    rel_residual = jnp.sqrt((load_sq - load_image * load_image / image_sq) / load_sq)
    return (solution, residual, rel_residual)


THETA = 1.65
DELTA = 1.35
RATIO = THETA / DELTA
RHO0 = 1.0 / RATIO
RHO1 = 1.0 / (2.0 * RATIO - RHO0)
KEEP = RHO1 * RHO0
PUSH = 2.0 * RHO1 / DELTA
LANES = 128
SUBS = 8


def triple(first, second, third):
    return np.kron(first, np.kron(second, third))


def split_const(matrix):
    high = matrix.astype(jnp.bfloat16)
    low = (matrix - high.astype(np.float64)).astype(jnp.bfloat16)
    return high, low


def stacked(matrix):
    high, low = split_const(matrix)
    return np.concatenate([high, high, low], axis=1)


class Tables:
    def __init__(self):
        self.tables = [lobatto(count) for count in (8, 4, 2)]
        self.weights = [table[1] for table in self.tables]
        self.stiff = [table[2].T @ np.diag(table[1]) @ table[2] for table in self.tables]
        interps = [
            lagrange(self.tables[level][0], self.tables[level + 1][0]) for level in range(2)
        ]
        order = [0, 7, 1, 2, 3, 4, 5, 6]
        w, k = np.diag(self.weights[0]), self.stiff[0]
        plane = np.kron(k, w) + np.kron(w, k)
        both = np.kron(w, w)
        flip = k[:4, ::-1][:, :4]
        even = 0.5 * (k[:4, :4] + flip)
        odd = 0.5 * (k[:4, :4] - flip)
        half = 0.5 * w[:4, :4]
        columns = np.concatenate(
            [np.arange(8) + 64 * kk + 8 * i for kk in range(4) for i in order]
        )
        self.even = stacked((np.kron(even, both) + np.kron(half, plane))[:, columns])
        self.odd = stacked((np.kron(odd, both) + np.kron(half, plane))[:, columns])
        factor = [np.where((np.arange(n) == 0) | (np.arange(n) == n - 1), 0.5, 1.0) for n in (8, 4)]
        down = [interps[level].T * factor[level][None, :] for level in range(2)]
        full = np.concatenate([np.arange(8) + 64 * kk + 8 * i for kk in range(8) for i in order])
        high, low = split_const(triple(down[0], down[0], down[0])[:, full])
        self.down0 = np.concatenate([high, low], axis=0)
        self.up0 = stacked(triple(interps[0], interps[0], interps[0]))
        w, k = np.diag(self.weights[1]), self.stiff[1]
        self.op1 = stacked(triple(k, w, w) + triple(w, k, w) + triple(w, w, k))
        self.down1 = triple(down[1], down[1], down[1]).astype(np.float32)
        self.up1 = triple(interps[1], interps[1], interps[1]).astype(np.float32)
        w, k = np.diag(self.weights[2]), self.stiff[2]
        self.op2 = (triple(k, w, w) + triple(w, k, w) + triple(w, w, k)).astype(np.float32)
        self.squares = [
            np.sum(table[2] * table[2] * table[1][:, None], axis=0) for table in self.tables
        ]
        wide = lambda column: np.repeat(np.asarray(column, np.float32)[:, None], LANES, axis=1)
        mass, point = [], []
        for level in (1, 2):
            a, b = self.weights[level], self.squares[level]
            mass.append(wide(triple(a, a, a)))
            point.append(wide(triple(b, a, a) + triple(a, b, a) + triple(a, a, b)))
        self.rows = np.concatenate(
            [wide(self.weights[0]), wide(self.squares[0]), mass[0], point[0], mass[1], point[1],
             wide(factor[0])], axis=0)


PAIRS = ((0, 7), (1, 2), (3, 4), (5, 6))


def kernel(nx, ny, tables, meta, near, far, even, odd, down0, up0, op1, down1, up1, op2, rows,
           sol_ref, res_ref, rel_ref, b_ref, r_ref, d_ref, z_ref, v_ref, re_ref, ro_ref,
           be_ref, bo_ref, c_ref, lane_ref):
    groups = nx // SUBS
    tiles = ny * groups
    wide = tiles * LANES
    own_x, own_y = meta[0], meta[1]
    sub = lax.broadcasted_iota(jnp.int32, (SUBS, LANES), 0)
    lane = lax.broadcasted_iota(jnp.int32, (SUBS, LANES), 1) % SUBS
    w = [float(x) for x in tables.weights[0]]
    q = [float(x) for x in tables.squares[0]]
    f = [0.5 if k in (0, 7) else 1.0 for k in range(8)]

    def cols(x):
        return [x[:, t * LANES:(t + 1) * LANES] for t in range(tiles)]

    def join(parts):
        return jnp.concatenate(parts, axis=1)

    def across(x):
        return join([x] * tiles)

    sub_w = across(sub)

    def shift_y(parts, step):
        return [parts[((t // groups - step) % ny) * groups + t % groups] for t in range(tiles)]

    def x_up(x):
        parts, out = cols(x), []
        for t in range(tiles):
            prev = parts[(t // groups) * groups + (t % groups - 1) % groups]
            out.append(jnp.where(lane == 0, pltpu.roll(prev, LANES - SUBS + 1, 1),
                                 pltpu.roll(parts[t], 1, 1)))
        return join(out)

    def x_down(x):
        parts, out = cols(x), []
        for t in range(tiles):
            succ = parts[(t // groups) * groups + (t % groups + 1) % groups]
            out.append(jnp.where(lane == SUBS - 1, pltpu.roll(succ, SUBS - 1, 1),
                                 pltpu.roll(parts[t], LANES - 1, 1)))
        return join(out)

    def z_up(x):
        return join([pltpu.roll(p, SUBS, 1) for p in cols(x)])

    def z_down(x):
        return join([pltpu.roll(p, LANES - SUBS, 1) for p in cols(x)])

    def y_fold(x, first, last, low, high):
        before = join(shift_y(cols(x), 1))
        after = join(shift_y(cols(x), -1))
        return x + jnp.where(first, pltpu.roll(before, low, 0),
                             jnp.where(last, pltpu.roll(after, high, 0), 0.0))

    def fold_y8(x):
        return y_fold(x, sub_w == 0, sub_w == 7, 1, 7)

    def row(k, i):
        return pl.ds(k * 64 + i * 8, 8)

    even_own = (own_x & 1) == 0
    for t in range(tiles):
        y_index, high = t // groups, t % groups
        slots = []
        for c in range(0, SUBS, 2):
            delta = (high * SUBS + c) ^ own_x
            slot, bit = jnp.int32(0), 0
            if ny > 1:
                slot, bit = y_index ^ own_y, 1
            step = nx // 2
            while step > 1:
                flag = jnp.where((delta & step) != 0, 1, 0)
                slot = slot + flag * (1 << bit)
                bit += 1
                step //= 2
            slots.append(slot)
        for i in range(8):
            block = []
            for slot in slots:
                a, b = near[slot, i], far[slot, i]
                block.append(jnp.where(even_own, a, b))
                block.append(jnp.where(even_own, b, a))
            for step in (1, 2, 4):
                out = list(block)
                for c in range(SUBS):
                    if not c & step:
                        a, b = block[c], block[c + step]
                        keep = (lane & step) == 0
                        out[c] = jnp.where(keep, a, pltpu.roll(b, step, 1))
                        out[c + step] = jnp.where(keep, pltpu.roll(a, LANES - step, 1), b)
                block = out
            for k in range(7):
                v_ref[row(k, i), t * LANES:(t + 1) * LANES] = block[k]
            v_ref[row(7, i), t * LANES:(t + 1) * LANES] = pltpu.roll(block[0], LANES - SUBS, 1)
            if i == 0:
                lane_ref[0:8, t * LANES:(t + 1) * LANES] = block[7]
    kap1 = lane_ref[0:1, :]
    sig1 = lane_ref[1:2, :]
    kap = jnp.broadcast_to(kap1, (SUBS, wide))
    sig = jnp.broadcast_to(sig1, (SUBS, wide))
    w_j = across(rows[0:8, :])
    q_j = across(rows[8:16, :])
    f_j = across(rows[160:168, :])
    sig_w = sig * w_j

    def store_split(kk, index, low_pair, high_pair):
        a = jnp.concatenate(low_pair, axis=0)
        b = jnp.concatenate(high_pair, axis=0)
        for ref, value in ((be_ref, a + b), (bo_ref, a - b)):
            high = value.astype(jnp.bfloat16)
            low = (value - high.astype(jnp.float32)).astype(jnp.bfloat16)
            at = kk * 64 + index * 16
            ref[at:at + 16, :] = high
            ref[256 + at:272 + at, :] = low
            ref[512 + at:528 + at, :] = high

    def fold_pairs(kk, get, index):
        out = []
        for i in PAIRS[index]:
            a, b = get(kk, i), get(7 - kk, i)
            out.append((a, b))
        return out

    def assemble_pairs(kk, index, values, with_z=True):
        vals = [list(v) for v in values]
        if kk == 0 and with_z:
            for v in vals:
                a, b = v
                v[0] = a + z_up(b)
                v[1] = b + z_down(a)
        if index == 0:
            for s in range(2):
                a, b = vals[0][s], vals[1][s]
                vals[0][s] = a + x_up(b)
                vals[1][s] = b + x_down(a)
        return [[fold_y8(x) for x in v] for v in vals]

    def point(k, i):
        s1 = q[k] * w[i] + w[k] * q[i]
        s2 = w[k] * w[i]
        return kap * (s1 * w_j + s2 * q_j) + s2 * sig_w

    for kk in range(4):
        for index, pair in enumerate(PAIRS):
            diag = assemble_pairs(kk, index, fold_pairs(kk, point, index))
            load = assemble_pairs(
                kk, index, fold_pairs(kk, lambda k, i: v_ref[row(k, i), :], index), with_z=False)
            dirs = []
            for s, k in enumerate((kk, 7 - kk)):
                group = []
                for n, i in enumerate(pair):
                    inverse = 1.0 / diag[n][s]
                    b_ref[row(k, i), :] = load[n][s]
                    r_ref[row(k, i), :] = load[n][s]
                    first = load[n][s] * inverse * (1.0 / THETA)
                    d_ref[row(k, i), :] = first
                    z_ref[row(k, i), :] = jnp.zeros_like(first)
                    group.append((first, inverse))
                dirs.append([g[0] for g in group])
                for n, i in enumerate(pair):
                    v_ref[row(k, i), :] = group[n][1]
            store_split(kk, index, dirs[0], dirs[1])

    def tile_rows(x):
        return jnp.concatenate([x] * tiles, axis=1)

    def fold1(x):
        first = x[0:16] + z_up16(x[48:64])
        last = x[48:64] + z_down16(x[0:16])
        pieces = [first[0:8], first[8:16], x[16:24], x[24:32], x[32:40], x[40:48],
                  last[0:8], last[8:16]]
        out = []
        for k in range(4):
            a, b = pieces[2 * k], pieces[2 * k + 1]
            lower = sub_w < 4
            na = a + jnp.where(lower, x_up(pltpu.roll(b, 4, 0)), 0.0)
            nb = b + jnp.where(lower, 0.0, x_down(pltpu.roll(a, 4, 0)))
            out += [na, nb]
        j = sub_w % 4
        out = [y_fold(x, j == 0, j == 3, 5, 3) for x in out]
        return jnp.concatenate(out, axis=0)

    def z_up16(x):
        return jnp.concatenate([z_up(x[0:8]), z_up(x[8:16])], axis=0)

    def z_down16(x):
        return jnp.concatenate([z_down(x[0:8]), z_down(x[8:16])], axis=0)

    def fold2(x):
        other = pltpu.roll(x, 4, 0)
        x = x + jnp.where(sub_w < 4, z_up(other), z_down(other))
        i = (sub_w // 2) % 2
        x = x + jnp.where(i == 0, x_up(pltpu.roll(x, 6, 0)), x_down(pltpu.roll(x, 2, 0)))
        j = sub_w % 2
        return y_fold(x, j == 0, j == 1, 7, 1)

    def cat3(x):
        high = x.astype(jnp.bfloat16)
        low = (x - high.astype(jnp.float32)).astype(jnp.bfloat16)
        return jnp.concatenate([high, low, high], axis=0)

    def dot(a, b):
        return jnp.dot(a, b, preferred_element_type=jnp.float32)

    def dot_high(a, b):
        return jnp.dot(a, b, preferred_element_type=jnp.float32, precision=lax.Precision.HIGHEST)

    mass1 = tile_rows(rows[16:80, :])
    point1 = tile_rows(rows[80:144, :])
    mass2 = tile_rows(rows[144:152, :])
    point2 = tile_rows(rows[152:160, :])
    inv1_ref, mass1_ref = lane_ref.at[8:72, :], lane_ref.at[72:136, :]
    inv1_ref[...] = 1.0 / fold1(kap1 * point1 + sig1 * mass1)
    mass1_ref[...] = sig1 * mass1
    inv2 = 1.0 / fold2(kap1 * point2 + sig1 * mass2)
    lane_ref[136:144, :] = inv2
    lane_ref[144:152, :] = sig1 * mass2

    def apply1(v):
        return fold1(kap1 * dot(op1[...], cat3(v)) + mass1_ref[...] * v)

    def apply2(v):
        return fold2(kap1 * dot_high(op2[...], v) + lane_ref[144:152, :] * v)

    def coarse(resid):
        inverse = inv1_ref[...]
        d = resid * inverse * (1.0 / THETA)
        x = d
        resid = resid - apply1(d)
        d = KEEP * d + PUSH * (resid * inverse)
        x = x + d
        resid = resid - apply1(d)
        low = fold2(dot_high(down1[...], resid))
        inverse2 = lane_ref[136:144, :]
        d = low * inverse2 * (1.0 / THETA)
        y = d
        low = low - apply2(d)
        y = y + KEEP * d + PUSH * (low * inverse2)
        e = dot_high(up1[...], y)
        x = x + e
        resid = resid - apply1(e)
        return x + resid * inverse * (1.0 / THETA)

    def multiply():
        re_ref[...] = dot(even[...], be_ref[...])
        ro_ref[...] = dot(odd[...], bo_ref[...])

    def image(kk, index):
        values = []
        for i in PAIRS[index]:
            e = re_ref[row(kk, i), :]
            o = ro_ref[row(kk, i), :]
            scale = sig_w * (w[kk] * w[i])
            values.append((kap * (e + o) + scale * d_ref[row(kk, i), :],
                           kap * (e - o) + scale * d_ref[row(7 - kk, i), :]))
        return assemble_pairs(kk, index, values)

    def sweep(update):
        multiply()
        for kk in range(4):
            for index, pair in enumerate(PAIRS):
                out = image(kk, index)
                dirs = []
                for s, k in enumerate((kk, 7 - kk)):
                    dirs.append([update(k, i, out[n][s]) for n, i in enumerate(pair)])
                yield kk, index, dirs

    def second_direction(k, i, value):
        r = r_ref[row(k, i), :] - value
        r_ref[row(k, i), :] = r
        first = d_ref[row(k, i), :]
        d = KEEP * first + PUSH * (r * v_ref[row(k, i), :])
        z_ref[row(k, i), :] = z_ref[row(k, i), :] + (first + d)
        return d

    def residual_only(k, i, value):
        r = r_ref[row(k, i), :] - value
        r_ref[row(k, i), :] = r
        return r

    def last_direction(k, i, value):
        r = r_ref[row(k, i), :] - value
        r_ref[row(k, i), :] = r
        d = r * v_ref[row(k, i), :] * (1.0 / THETA)
        z_ref[row(k, i), :] = z_ref[row(k, i), :] + d
        return d

    def first_direction(k, i, value):
        r = r_ref[row(k, i), :] - value
        r_ref[row(k, i), :] = r
        return r * v_ref[row(k, i), :] * (1.0 / THETA)

    def run(update, keep):
        for kk, index, dirs in sweep(update):
            if keep:
                for s, k in enumerate((kk, 7 - kk)):
                    for n, i in enumerate(PAIRS[index]):
                        d_ref[row(k, i), :] = dirs[s][n]
                store_split(kk, index, dirs[0], dirs[1])
            else:
                for s, k in enumerate((kk, 7 - kk)):
                    value = jnp.concatenate(dirs[s], axis=0)
                    high = value.astype(jnp.bfloat16)
                    low = (value - high.astype(jnp.float32)).astype(jnp.bfloat16)
                    at = k * 64 + index * 16
                    c_ref[at:at + 16, :] = high
                    c_ref[512 + at:528 + at, :] = low

    def cycle(step, carry):
        run(second_direction, True)
        run(residual_only, False)
        both = dot(down0[...], c_ref[0:512, :])
        low = both[0:64] + both[64:128] + dot(down0[0:64, :], c_ref[512:1024, :])
        correction = coarse(fold1(low))
        d_ref[...] = dot(up0[...], cat3(correction))
        for kk in range(4):
            for index, pair in enumerate(PAIRS):
                dirs = [[d_ref[row(k, i), :] for i in pair] for k in (kk, 7 - kk)]
                for s, k in enumerate((kk, 7 - kk)):
                    for n, i in enumerate(pair):
                        z_ref[row(k, i), :] = z_ref[row(k, i), :] + dirs[s][n]
                store_split(kk, index, dirs[0], dirs[1])
        run(last_direction, True)
        run(first_direction, True)
        return carry

    lax.fori_loop(0, 2, cycle, 0)

    zero = jnp.zeros((SUBS, wide), jnp.float32)
    bw, ww, bb = zero, zero, zero
    for k in range(8):
        for i in range(8):
            b = b_ref[row(k, i), :]
            image_all = b - r_ref[row(k, i), :]
            fb = b * (f[k] * f[i])
            bw = bw + fb * image_all
            ww = ww + image_all * image_all * (f[k] * f[i])
            bb = bb + fb * b
    bw, ww, bb = jnp.sum(bw * f_j), jnp.sum(ww * f_j), jnp.sum(bb * f_j)
    coef = bw / ww
    rr = zero
    for k in range(8):
        for i in range(8):
            b = b_ref[row(k, i), :]
            res = b - coef * (b - r_ref[row(k, i), :])
            rr = rr + res * res * (f[k] * f[i])
    rr = jnp.sum(rr * f_j)
    rel_ref[...] = jnp.sqrt(jnp.full((SUBS, LANES), rr / bb, jnp.float32))
    start = pl.multiple_of((own_y * groups + own_x // SUBS) * LANES, LANES)
    place = own_x % SUBS
    window = pl.ds(start, LANES)
    for i in range(8):
        sol = jnp.zeros((SUBS, LANES), jnp.float32)
        res = sol
        for k in range(8):
            b = b_ref[row(k, i), window]
            z = z_ref[row(k, i), window]
            r = b - coef * (b - r_ref[row(k, i), window])
            turn = (k - place) % LANES
            sol = jnp.where(lane == k, pltpu.roll(z, turn, 1), sol)
            res = jnp.where(lane == k, pltpu.roll(r, turn, 1), res)
        sol_ref[i] = coef * sol
        res_ref[i] = res


def solve_all(nx, ny, meta, near, far, interpret=False):
    tables = Tables()
    wide = ny * nx // SUBS * LANES
    consts = [tables.even, tables.odd, tables.down0, tables.up0, tables.op1, tables.down1,
              tables.up1, tables.op2, tables.rows]
    vmem = pl.BlockSpec(memory_space=pltpu.VMEM)
    field = pltpu.VMEM((512, wide), jnp.float32)
    return pl.pallas_call(
        lambda *refs: kernel(nx, ny, tables, *refs),
        in_specs=[pl.BlockSpec(memory_space=pltpu.SMEM)] + [vmem] * 11,
        out_specs=[vmem] * 3,
        out_shape=[
            jax.ShapeDtypeStruct(near.shape[1:], jnp.float32),
            jax.ShapeDtypeStruct(near.shape[1:], jnp.float32),
            jax.ShapeDtypeStruct((SUBS, LANES), jnp.float32),
        ],
        scratch_shapes=[
            field, field, field, field, field,
            pltpu.VMEM((256, wide), jnp.float32), pltpu.VMEM((256, wide), jnp.float32),
            pltpu.VMEM((768, wide), jnp.bfloat16), pltpu.VMEM((768, wide), jnp.bfloat16),
            pltpu.VMEM((1024, wide), jnp.bfloat16), pltpu.VMEM((152, wide), jnp.float32),
        ],
        name="solve_all",
        interpret=interpret,
    )(meta, near, far, *[jnp.asarray(c) for c in consts])


def packed_block(forcing, kappa, sigma):
    field = fold_axis(forcing, 2, SUBS)
    shape = field.shape
    index = [lax.broadcasted_iota(jnp.int32, shape, dim) for dim in range(3)]
    last = (index[2] % SUBS == SUBS - 1) & (index[0] == 0)
    wide = lambda value: jnp.repeat(value.reshape(-1), SUBS)[None, None, :]
    field = jnp.where(last & (index[1] == 0), wide(kappa), field)
    return jnp.where(last & (index[1] == 1), wide(sigma), field)


def gathered(forcing, kappa, sigma):
    nx, ny = lax.axis_size("gx"), lax.axis_size("gy")
    block = packed_block(forcing, kappa, sigma)[None]
    if ny > 1:
        other = lax.ppermute(block, "gy", [(i, i ^ 1) for i in range(ny)])
        block = jnp.concatenate([block, other], axis=0)
    step = nx // 2
    while step:
        other = lax.ppermute(block, "gx", [(i, i ^ step) for i in range(nx)])
        if step > 1:
            block = jnp.concatenate([block, other], axis=0)
        step //= 2
    meta = jnp.stack([lax.axis_index("gx"), lax.axis_index("gy")]).astype(jnp.int32)
    sol, res, rel = solve_all(nx, ny, meta, block, other)
    return sol, res, rel[0, 0]


def fits_one_device(mesh):
    nx, ny = mesh.shape["gx"], mesh.shape["gy"]
    power = nx & (nx - 1) == 0
    return power and nx % SUBS == 0 and ny <= 2 and nx * ny <= 64


def solution(mesh):
    spec = P("gx", "gy", None)
    small = fits_one_device(mesh)

    def local(forcing, kappa, sigma):
        plain = forcing.shape == (SUBS, SUBS, LANES) and kappa.shape == (1, 1, LANES // SUBS)
        return (gathered if small and plain else distributed)(forcing, kappa, sigma)

    return jax.shard_map(
        local, mesh=mesh, in_specs=(spec, spec, spec), out_specs=(spec, spec, P()),
        check_vma=False,
    )
```

```python
import jax
import jax.numpy as jnp
import numpy as np
from jax import lax
from jax.experimental import pallas as pl
from jax.experimental.pallas import tpu as pltpu
from jax.sharding import PartitionSpec as P


def with_halo(cells, sides, width):
    for axis, dim in sides:
        count = lax.axis_size(axis)
        head = lax.slice_in_dim(cells, 0, width, axis=dim)
        tail = lax.slice_in_dim(cells, cells.shape[dim] - width, cells.shape[dim], axis=dim)
        cells = jnp.concatenate(
            [
                lax.ppermute(tail, axis, [(i, (i + 1) % count) for i in range(count)]),
                cells,
                lax.ppermute(head, axis, [((i + 1) % count, i) for i in range(count)]),
            ],
            axis=dim,
        )
    return cells


def legendre_table(points, order):
    columns = [points * 0.0 + 1.0, points]
    for degree in range(2, order + 1):
        columns.append(
            ((2 * degree - 1) * points * columns[-1] - (degree - 1) * columns[-2]) / degree
        )
    return np.stack(columns, axis=1)


def lobatto(count):
    order = count - 1
    points = np.cos(np.pi * np.arange(count) / order)
    for sweep in range(60):
        table = legendre_table(points, order)
        points = points - (points * table[:, order] - table[:, order - 1]) / (
            count * table[:, order]
        )
    table = legendre_table(points, order)
    weights = 2.0 / (order * count * table[:, order] ** 2)
    values = table[:, order]
    points, weights, values = (points[::-1], weights[::-1], values[::-1])
    spread = points[:, None] - points[None, :] + np.eye(count)
    deriv = values[:, None] / values[None, :] / spread * (1.0 - np.eye(count))
    corner = order * (order + 1) / 4.0
    ends = np.array([-corner] + [0.0] * (count - 2) + [corner])
    return (points, weights, deriv + np.eye(count) * ends[None, :])


def lagrange(fine_points, coarse_points):
    columns = []
    for column in range(len(coarse_points)):
        value = fine_points * 0.0 + 1.0
        for other in range(len(coarse_points)):
            if other != column:
                value = (
                    value
                    * (fine_points - coarse_points[other])
                    / (coarse_points[column] - coarse_points[other])
                )
        columns.append(value)
    return np.stack(columns, axis=1)


def edge_factor(count, blocks):
    index = jnp.arange(count)
    single = jnp.where((index == 0) | (index == count - 1), 0.5, 1.0).astype(jnp.float32)
    return jnp.tile(single, blocks)


def multiplicity(count, blocks):
    first = edge_factor(count, blocks[0])
    second = edge_factor(count, blocks[1])
    third = edge_factor(count, blocks[2])
    return first[:, None, None] * second[None, :, None] * third[None, None, :]


def element_apply(field, kappa, sigma, deriv, weights):
    count = deriv.shape[0]
    ex, ey, ez = kappa.shape
    high = lax.Precision.HIGHEST
    block = field.reshape(ex, count, ey, count, ez, count)
    mass = (weights[:, None, None] * weights[None, :, None] * weights[None, None, :])[
        None, :, None, :, None, :
    ]
    first = jnp.einsum("ai,eifjgk->eafjgk", deriv, block, precision=high)
    total = jnp.einsum("ai,eafjgk->eifjgk", deriv, first * mass, precision=high)
    second = jnp.einsum("aj,eifjgk->eifagk", deriv, block, precision=high)
    total = total + jnp.einsum("aj,eifagk->eifjgk", deriv, second * mass, precision=high)
    third = jnp.einsum("ak,eifjgk->eifjga", deriv, block, precision=high)
    total = total + jnp.einsum("ak,eifjga->eifjgk", deriv, third * mass, precision=high)
    coeff = kappa[:, None, :, None, :, None]
    shift = sigma[:, None, :, None, :, None]
    return (coeff * total + shift * mass * block).reshape(field.shape)


def element_diagonal(kappa, sigma, deriv, weights):
    count = deriv.shape[0]
    ex, ey, ez = kappa.shape
    stiff = jnp.sum(deriv * deriv * weights[:, None], axis=0)
    term = stiff[:, None, None] * weights[None, :, None] * weights[None, None, :]
    term = term + weights[:, None, None] * stiff[None, :, None] * weights[None, None, :]
    term = term + weights[:, None, None] * weights[None, :, None] * stiff[None, None, :]
    mass = weights[:, None, None] * weights[None, :, None] * weights[None, None, :]
    coeff = kappa[:, None, :, None, :, None]
    shift = sigma[:, None, :, None, :, None]
    full = coeff * term[None, :, None, :, None, :] + shift * mass[None, :, None, :, None, :]
    return full.reshape(ex * count, ey * count, ez * count)


def fold_axis(field, dim, count):
    size = field.shape[dim]
    position = jnp.arange(size) % count
    shape = [1, 1, 1]
    shape[dim] = size
    first = (position == 0).reshape(shape)
    last = (position == count - 1).reshape(shape)
    before = jnp.roll(field, 1, dim)
    after = jnp.roll(field, -1, dim)
    return field + jnp.where(first, before, 0.0) + jnp.where(last, after, 0.0)


def fold_padded(padded, dim, count):
    size = padded.shape[dim] - 2
    center = lax.slice_in_dim(padded, 1, size + 1, axis=dim)
    before = lax.slice_in_dim(padded, 0, size, axis=dim)
    after = lax.slice_in_dim(padded, 2, size + 2, axis=dim)
    position = jnp.arange(size) % count
    shape = [1, 1, 1]
    shape[dim] = size
    first = (position == 0).reshape(shape)
    last = (position == count - 1).reshape(shape)
    return center + jnp.where(first, before, 0.0) + jnp.where(last, after, 0.0)


def assemble(field, count, finest):
    if finest:
        padded = with_halo(field, (("gx", 0), ("gy", 1)), 1)
        field = fold_padded(fold_padded(padded, 0, count), 1, count)
    else:
        padded = with_halo(field, (("gx", 0), ("gy", 1)), 1)
        field = fold_padded(fold_padded(padded, 0, count), 1, count)
    return fold_axis(field, 2, count)


def restrict(field, interp, blocks, fine_count, coarse_count):
    high = lax.Precision.HIGHEST
    block = field.reshape(blocks[0], fine_count, blocks[1], fine_count, blocks[2], fine_count)
    one = jnp.einsum("ia,eifjgk->eafjgk", interp, block, precision=high)
    two = jnp.einsum("jb,eafjgk->eafbgk", interp, one, precision=high)
    three = jnp.einsum("kc,eafbgk->eafbgc", interp, two, precision=high)
    return three.reshape(
        blocks[0] * coarse_count, blocks[1] * coarse_count, blocks[2] * coarse_count
    )


def prolong(field, interp, blocks, fine_count, coarse_count):
    high = lax.Precision.HIGHEST
    block = field.reshape(blocks[0], coarse_count, blocks[1], coarse_count, blocks[2], coarse_count)
    one = jnp.einsum("ia,eafbgc->eifbgc", interp, block, precision=high)
    two = jnp.einsum("jb,eifbgc->eifjgc", interp, one, precision=high)
    three = jnp.einsum("kc,eifjgc->eifjgk", interp, two, precision=high)
    return three.reshape(blocks[0] * fine_count, blocks[1] * fine_count, blocks[2] * fine_count)


def distributed(forcing, kappa, sigma):
    blocks = kappa.shape
    counts = [8, 4, 2]
    tables = [lobatto(count) for count in counts]
    derivs = [jnp.asarray(table[2], jnp.float32) for table in tables]
    weights = [jnp.asarray(table[1], jnp.float32) for table in tables]
    interps = [
        jnp.asarray(lagrange(tables[level][0], tables[level + 1][0]), jnp.float32)
        for level in range(2)
    ]
    mults = [multiplicity(count, blocks) for count in counts]
    diags = [
        assemble(
            element_diagonal(kappa, sigma, derivs[level], weights[level]), counts[level], level == 0
        )
        for level in range(3)
    ]
    center = 1.65
    half = 1.35
    ratio = center / half

    def operate(field, level):
        return assemble(
            element_apply(field, kappa, sigma, derivs[level], weights[level]),
            counts[level],
            level == 0,
        )

    def smooth(resid, level, steps, keep_last):
        rho = 1.0 / ratio
        direction = resid / (center * diags[level])
        iterate = direction
        for step in range(steps):
            if step > 0:
                rho_next = 1.0 / (2.0 * ratio - rho)
                direction = (
                    rho_next * rho * direction + 2.0 * rho_next / half * resid / diags[level]
                )
                iterate = iterate + direction
                rho = rho_next
            if step < steps - 1 or keep_last:
                resid = resid - operate(direction, level)
        return (iterate, resid)

    def vcycle(resid, level):
        if level == 2:
            iterate, unused = smooth(resid, level, 2, False)
            return iterate
        iterate, resid = smooth(resid, level, 2, True)
        coarse = assemble(
            restrict(
                mults[level] * resid, interps[level], blocks, counts[level], counts[level + 1]
            ),
            counts[level + 1],
            False,
        )
        correction = prolong(
            vcycle(coarse, level + 1), interps[level], blocks, counts[level], counts[level + 1]
        )
        iterate = iterate + correction
        resid = resid - operate(correction, level)
        return iterate + resid / (center * diags[level])

    load = assemble(forcing, 8, True)
    first = vcycle(load, 0)
    image_first = operate(first, 0)
    second = vcycle(load - image_first, 0)
    combined = first + second
    image = operate(combined, 0)
    weight = mults[0]
    load_sq, load_image, image_sq = lax.psum(
        (
            jnp.sum(weight * load * load),
            jnp.sum(weight * load * image),
            jnp.sum(weight * image * image),
        ),
        ("gx", "gy"),
    )
    coef = load_image / image_sq
    solution = coef * combined
    residual = load - coef * image
    rel_residual = jnp.sqrt((load_sq - load_image * load_image / image_sq) / load_sq)
    return (solution, residual, rel_residual)


THETA = 1.65
DELTA = 1.35
RATIO = THETA / DELTA
RHO0 = 1.0 / RATIO
RHO1 = 1.0 / (2.0 * RATIO - RHO0)
KEEP = RHO1 * RHO0
PUSH = 2.0 * RHO1 / DELTA
LANES = 128
SUBS = 8


def triple(first, second, third):
    return np.kron(first, np.kron(second, third))


def split_const(matrix):
    high = matrix.astype(jnp.bfloat16)
    low = (matrix - high.astype(np.float64)).astype(jnp.bfloat16)
    return high, low


def stacked(matrix):
    high, low = split_const(matrix)
    return np.concatenate([high, high, low], axis=1)


J_ORDER = (0, 1, 2, 3, 7, 5, 6, 4)
PAIRS = ((0, 7), (1, 2), (3, 4), (5, 6))
FACE = (0, 1, 3, 2)
ROWS1 = tuple(
    (k * 4 + FACE[2 * ih + il]) * 4 + FACE[2 * jh + jl]
    for k in range(4) for ih in range(2) for jh in range(2) for il in range(2) for jl in range(2)
)
ROWS2 = tuple((k * 2 + i) * 2 + j for j in range(2) for k in range(2) for i in range(2))


def padded(matrix, rows, columns):
    return np.pad(matrix, ((0, rows - matrix.shape[0]), (0, columns - matrix.shape[1])))


class Tables:
    def __init__(self):
        tables = [lobatto(count) for count in (8, 4, 2)]
        self.weights = [table[1] for table in tables]
        stiff = [table[2].T @ np.diag(table[1]) @ table[2] for table in tables]
        self.squares = [np.sum(t[2] * t[2] * t[1][:, None], axis=0) for t in tables]
        interps = [lagrange(tables[level][0], tables[level + 1][0]) for level in range(2)]
        factor = [np.where((np.arange(n) == 0) | (np.arange(n) == n - 1), 0.5, 1.0) for n in (8, 4)]
        down = [interps[level].T * factor[level][None, :] for level in range(2)]
        flat = [i for pair in PAIRS for i in pair]
        rows0 = [(k * 8 + i) * 8 + j for k in range(8) for i in range(8) for j in J_ORDER]
        data0 = [(k * 8 + i) * 8 + j for k in range(8) for i in flat for j in J_ORDER]
        rows1, rows2 = list(ROWS1), list(ROWS2)
        w, k = np.diag(self.weights[0]), stiff[0]
        plane = np.kron(k, w) + np.kron(w, k)
        both = np.kron(w, w)
        flip = k[:4, ::-1][:, :4]
        half = np.kron(0.5 * w[:4, :4], plane)
        even = np.kron(0.5 * (k[:4, :4] + flip), both) + half
        odd = np.kron(0.5 * (k[:4, :4] - flip), both) + half
        self.even = stacked(even[np.ix_(rows0[:256], data0[:256])])
        self.odd = stacked(odd[np.ix_(rows0[:256], data0[:256])])
        high, low = split_const(triple(down[0], down[0], down[0])[np.ix_(rows1, data0)])
        self.down0 = np.concatenate([high, low], axis=0)
        self.up0 = stacked(triple(interps[0], interps[0], interps[0])[np.ix_(rows0, rows1)])
        w, k = np.diag(self.weights[1]), stiff[1]
        self.op1 = stacked((triple(k, w, w) + triple(w, k, w) + triple(w, w, k))[np.ix_(rows1, rows1)])
        self.down1 = padded(stacked(triple(down[1], down[1], down[1])[np.ix_(rows2, rows1)]), 16, 192)
        self.up1 = padded(stacked(triple(interps[1], interps[1], interps[1])[np.ix_(rows1, rows2)]), 64, 32)
        w, k = np.diag(self.weights[2]), stiff[2]
        self.op2 = padded(
            stacked((triple(k, w, w) + triple(w, k, w) + triple(w, w, k))[np.ix_(rows2, rows2)]), 16, 32)
        wide = lambda column: np.repeat(np.asarray(column, np.float32)[:, None], LANES, axis=1)
        blocks = [wide(self.weights[0][list(J_ORDER)]), wide(self.squares[0][list(J_ORDER)]),
                  wide(factor[0][list(J_ORDER)])]
        for level, order in ((1, rows1), (2, rows2)):
            a, b = self.weights[level], self.squares[level]
            blocks.append(wide(triple(a, a, a)[order]))
            blocks.append(wide((triple(b, a, a) + triple(a, b, a) + triple(a, a, b))[order]))
        self.rows = np.concatenate(blocks, axis=0)


def swap_rows(x, sub):
    return jnp.where(sub == 4, pltpu.roll(x, 5, 0), jnp.where(sub == 7, pltpu.roll(x, 3, 0), x))


def kernel(nx, ny, tables, meta, near, far, even, odd, down0, up0, op1, down1, up1, op2, rows,
           sol_ref, res_ref, rel_ref, b_ref, r_ref, d_ref, v_ref, p_ref, z_ref, re_ref, ro_ref,
           be_ref, bo_ref, c_ref, lane_ref):
    groups = nx // SUBS
    tiles = ny * groups
    wide = tiles * LANES
    own_x, own_y = meta[0], meta[1]
    sub = lax.broadcasted_iota(jnp.int32, (SUBS, LANES), 0)
    lane = lax.broadcasted_iota(jnp.int32, (SUBS, LANES), 1) % SUBS
    w = [float(x) for x in tables.weights[0]]
    q = [float(x) for x in tables.squares[0]]
    f = [0.5 if k in (0, 7) else 1.0 for k in range(8)]

    def cols(x):
        return [x[:, t * LANES:(t + 1) * LANES] for t in range(tiles)]

    def join(parts):
        return jnp.concatenate(parts, axis=1)

    def across(x):
        return join([x] * tiles)

    sub_w = across(sub)

    def x_up(x, more=0):
        parts, out = cols(x), []
        for t in range(tiles):
            if t % groups:
                prev = parts[t - 1]
                out.append(pltpu.roll(prev, more, 1) if more else prev)
            else:
                prev = parts[t + groups - 1]
                out.append(jnp.where(lane == 0, pltpu.roll(prev, (LANES - SUBS + 1 + more) % LANES, 1),
                                     pltpu.roll(prev, 1 + more, 1)))
        return join(out)

    def x_down(x, more=0):
        parts, out = cols(x), []
        for t in range(tiles):
            if t % groups < groups - 1:
                succ = parts[t + 1]
                out.append(pltpu.roll(succ, more, 1) if more else succ)
            else:
                succ = parts[t - groups + 1]
                out.append(jnp.where(lane == SUBS - 1, pltpu.roll(succ, SUBS - 1 + more, 1),
                                     pltpu.roll(succ, (LANES - 1 + more) % LANES, 1)))
        return join(out)

    up, down = SUBS, LANES - SUBS

    def z_up(x):
        return join([pltpu.roll(p, up, 1) for p in cols(x)])

    def z_down(x):
        return join([pltpu.roll(p, down, 1) for p in cols(x)])

    def y_fold(x, face):
        parts = cols(x)
        other = join([parts[(t + groups) % tiles] for t in range(tiles)])
        return x + jnp.where(face, pltpu.roll(other, 4, 0), 0.0)

    face0 = sub_w % 4 == 0
    face1 = sub_w % 2 == 0

    def row(k, i):
        return pl.ds(k * 64 + i * 8, 8)

    for t in range(tiles):
        y_index, part = t // groups, t % groups
        use_near = ((part ^ own_x) & 1) == 0
        slots = []
        for c in range(SUBS):
            delta = (c * groups + part) ^ own_x
            slot, bit = jnp.int32(0), 0
            if ny > 1:
                slot, bit = y_index ^ own_y, 1
            step = nx // 2
            while step > 1:
                flag = jnp.where((delta & step) != 0, 1, 0)
                slot = slot + flag * (1 << bit)
                bit += 1
                step //= 2
            slots.append(slot)
        for i in range(8):
            block = [jnp.where(use_near, near[slot, i], far[slot, i]) for slot in slots]
            for step in (1, 2, 4):
                out = list(block)
                for c in range(SUBS):
                    if not c & step:
                        a, b = block[c], block[c + step]
                        keep = (lane & step) == 0
                        out[c] = jnp.where(keep, a, pltpu.roll(b, step, 1))
                        out[c + step] = jnp.where(keep, pltpu.roll(a, LANES - step, 1), b)
                block = out
            for k in range(7):
                v_ref[row(k, i), t * LANES:(t + 1) * LANES] = block[k]
            v_ref[row(7, i), t * LANES:(t + 1) * LANES] = pltpu.roll(block[0], LANES - SUBS, 1)
            if i == 0:
                lane_ref[0:8, t * LANES:(t + 1) * LANES] = block[7]
    kap1 = lane_ref[0:1, :]
    sig1 = lane_ref[1:2, :]
    kap = jnp.broadcast_to(kap1, (SUBS, wide))
    sig = jnp.broadcast_to(sig1, (SUBS, wide))
    w_j = across(rows[0:8, :])
    q_j = across(rows[8:16, :])
    f_j = across(rows[16:24, :])
    sig_w = sig * w_j

    def store_split(kk, index, low_pair, high_pair):
        a = jnp.concatenate(low_pair, axis=0)
        b = jnp.concatenate(high_pair, axis=0)
        for ref, value in ((be_ref, a + b), (bo_ref, a - b)):
            high = value.astype(jnp.bfloat16)
            low = (value - high.astype(jnp.float32)).astype(jnp.bfloat16)
            at = kk * 64 + index * 16
            ref[at:at + 16, :] = high
            ref[256 + at:272 + at, :] = low
            ref[512 + at:528 + at, :] = high

    def fold_pairs(kk, get, index):
        out = []
        for i in PAIRS[index]:
            a, b = get(kk, i), get(7 - kk, i)
            out.append((a, b))
        return out

    def assemble_pairs(kk, index, values, with_z=True):
        vals = [list(v) for v in values]
        if kk == 0 and with_z:
            for v in vals:
                a, b = v
                v[0] = a + z_up(b)
                v[1] = b + z_down(a)
        if index == 0:
            for s in range(2):
                a, b = vals[0][s], vals[1][s]
                vals[0][s] = a + x_up(b)
                vals[1][s] = b + x_down(a)
        return [[y_fold(x, face0) for x in v] for v in vals]

    def point(k, i):
        s1 = q[k] * w[i] + w[k] * q[i]
        s2 = w[k] * w[i]
        return kap * (s1 * w_j + s2 * q_j) + s2 * sig_w

    for kk in range(4):
        for index, pair in enumerate(PAIRS):
            diag = assemble_pairs(kk, index, fold_pairs(kk, point, index))
            load = assemble_pairs(
                kk, index, fold_pairs(kk, lambda k, i: v_ref[row(k, i), :], index), with_z=False)
            dirs = []
            for s, k in enumerate((kk, 7 - kk)):
                group = []
                for n, i in enumerate(pair):
                    inverse = 1.0 / diag[n][s]
                    b_ref[row(k, i), :] = load[n][s]
                    r_ref[row(k, i), :] = load[n][s]
                    scaled = inverse * (1.0 / THETA)
                    p_ref[row(k, i), :] = inverse * PUSH
                    first = load[n][s] * scaled
                    d_ref[row(k, i), :] = first
                    group.append((first, scaled))
                dirs.append([g[0] for g in group])
                for n, i in enumerate(pair):
                    v_ref[row(k, i), :] = group[n][1]
            store_split(kk, index, dirs[0], dirs[1])

    def tile_rows(x):
        return jnp.concatenate([x] * tiles, axis=1)

    low_face = (sub_w // 2) % 2 == 0

    def fold1(x):
        p = [(x[16 * k:16 * k + 8], x[16 * k + 8:16 * k + 16]) for k in range(4)]
        out = []
        for k, (a, b) in enumerate(p):
            na, nb = x_up(b), x_down(a)
            if k in (0, 3):
                c, e = p[3 - k]
                move, amount = (z_up, up) if k == 0 else (z_down, down)
                na = na + x_up(e, amount)
                nb = nb + x_down(c, amount)
                a, b = a + move(c), b + move(e)
            out.append(y_fold(a + jnp.where(low_face, na, 0.0), face1))
            out.append(y_fold(b + jnp.where(low_face, nb, 0.0), face1))
        return jnp.concatenate(out, axis=0)

    first_k = (sub_w // 2) % 2 == 0
    first_i = sub_w % 2 == 0

    def fold2(x):
        other_k = jnp.where(first_k, pltpu.roll(x, 6, 0), pltpu.roll(x, 2, 0))
        other_i = jnp.where(first_i, pltpu.roll(x, 7, 0), pltpu.roll(x, 1, 0))
        both = jnp.where(first_i, pltpu.roll(other_k, 7, 0), pltpu.roll(other_k, 1, 0))
        x = x + jnp.where(first_k, z_up(other_k), z_down(other_k))
        x = x + jnp.where(first_i, x_up(other_i), x_down(other_i))
        x = x + jnp.where(first_k, jnp.where(first_i, x_up(both, up), x_down(both, up)),
                          jnp.where(first_i, x_up(both, down), x_down(both, down)))
        return y_fold(x, sub_w >= 0)

    def cat3(x):
        high = x.astype(jnp.bfloat16)
        low = (x - high.astype(jnp.float32)).astype(jnp.bfloat16)
        return jnp.concatenate([high, low, high], axis=0)

    def cat3_small(x):
        high = x.astype(jnp.bfloat16).astype(jnp.float32)
        return jnp.concatenate([high, x - high, high, jnp.zeros_like(x)], axis=0).astype(jnp.bfloat16)

    def dot(a, b):
        return jnp.dot(a, b, preferred_element_type=jnp.float32)

    mass1 = tile_rows(rows[24:88, :])
    point1 = tile_rows(rows[88:152, :])
    mass2 = tile_rows(rows[152:160, :])
    point2 = tile_rows(rows[160:168, :])
    inv1_ref, mass1_ref = lane_ref.at[8:72, :], lane_ref.at[72:136, :]
    inv1_ref[...] = 1.0 / fold1(kap1 * point1 + sig1 * mass1)
    mass1_ref[...] = sig1 * mass1
    inv2 = 1.0 / fold2(kap1 * point2 + sig1 * mass2)
    lane_ref[136:144, :] = inv2
    lane_ref[144:152, :] = sig1 * mass2

    def apply1(v):
        return fold1(kap1 * dot(op1[...], cat3(v)) + mass1_ref[...] * v)

    def apply2(v):
        return fold2(kap1 * dot(op2[...], cat3_small(v))[0:8] + lane_ref[144:152, :] * v)

    def coarse(resid):
        inverse = inv1_ref[...]
        d = resid * inverse * (1.0 / THETA)
        x = d
        resid = resid - apply1(d)
        d = KEEP * d + PUSH * (resid * inverse)
        x = x + d
        resid = resid - apply1(d)
        low = fold2(dot(down1[...], cat3(resid))[0:8])
        inverse2 = lane_ref[136:144, :]
        d = low * inverse2 * (1.0 / THETA)
        y = d
        low = low - apply2(d)
        y = y + KEEP * d + PUSH * (low * inverse2)
        e = dot(up1[...], cat3_small(y))
        x = x + e
        resid = resid - apply1(e)
        return x + resid * inverse * (1.0 / THETA)

    def multiply():
        re_ref[...] = dot(even[...], be_ref[...])
        ro_ref[...] = dot(odd[...], bo_ref[...])

    def image(kk, index):
        values = []
        for i in PAIRS[index]:
            e = re_ref[row(kk, i), :]
            o = ro_ref[row(kk, i), :]
            scale = sig_w * (w[kk] * w[i])
            values.append((kap * (e + o) + scale * d_ref[row(kk, i), :],
                           kap * (e - o) + scale * d_ref[row(7 - kk, i), :]))
        return assemble_pairs(kk, index, values)

    def sweep(update):
        multiply()
        for kk in range(4):
            for index, pair in enumerate(PAIRS):
                out = image(kk, index)
                dirs = []
                for s, k in enumerate((kk, 7 - kk)):
                    dirs.append([update(k, i, out[n][s]) for n, i in enumerate(pair)])
                yield kk, index, dirs

    def second_direction(k, i, value):
        r = r_ref[row(k, i), :] - value
        r_ref[row(k, i), :] = r
        first = d_ref[row(k, i), :]
        return KEEP * first + r * p_ref[row(k, i), :]

    def residual_only(k, i, value):
        r = r_ref[row(k, i), :] - value
        r_ref[row(k, i), :] = r
        return r

    def next_direction(k, i, value):
        r = r_ref[row(k, i), :] - value
        r_ref[row(k, i), :] = r
        return r * v_ref[row(k, i), :]

    def run(update, keep):
        for kk, index, dirs in sweep(update):
            if keep:
                for s, k in enumerate((kk, 7 - kk)):
                    for n, i in enumerate(PAIRS[index]):
                        d_ref[row(k, i), :] = dirs[s][n]
                store_split(kk, index, dirs[0], dirs[1])
            else:
                for s, k in enumerate((kk, 7 - kk)):
                    value = jnp.concatenate(dirs[s], axis=0)
                    high = value.astype(jnp.bfloat16)
                    low = (value - high.astype(jnp.float32)).astype(jnp.bfloat16)
                    at = k * 64 + index * 16
                    c_ref[at:at + 16, :] = high
                    c_ref[512 + at:528 + at, :] = low

    start = pl.multiple_of((own_y * groups + own_x % groups) * LANES, LANES)
    window = pl.ds(start, LANES)
    z_ref[...] = jnp.zeros((512, LANES), jnp.float32)

    def collect():
        z_ref[...] = z_ref[...] + d_ref[:, window]

    def cycle(step, carry):
        collect()
        run(second_direction, True)
        collect()
        run(residual_only, False)
        both = dot(down0[...], c_ref[0:512, :])
        low = both[0:64] + both[64:128] + dot(down0[0:64, :], c_ref[512:1024, :])
        correction = coarse(fold1(low))
        d_ref[...] = dot(up0[...], cat3(correction))
        collect()
        for kk in range(4):
            for index, pair in enumerate(PAIRS):
                store_split(kk, index, *[[d_ref[row(k, i), :] for i in pair] for k in (kk, 7 - kk)])
        run(next_direction, True)
        collect()
        run(next_direction, True)
        return carry

    lax.fori_loop(0, 2, cycle, 0)

    zero = jnp.zeros((SUBS, wide), jnp.float32)
    bw, ww, bb = zero, zero, zero
    for k in range(8):
        for i in range(8):
            b = b_ref[row(k, i), :]
            image_all = b - r_ref[row(k, i), :]
            fb = b * (f[k] * f[i])
            bw = bw + fb * image_all
            ww = ww + image_all * image_all * (f[k] * f[i])
            bb = bb + fb * b
    bw, ww, bb = jnp.sum(bw * f_j), jnp.sum(ww * f_j), jnp.sum(bb * f_j)
    coef = bw / ww
    rr = zero
    for k in range(8):
        for i in range(8):
            b = b_ref[row(k, i), :]
            res = b - coef * (b - r_ref[row(k, i), :])
            rr = rr + res * res * (f[k] * f[i])
    rr = jnp.sum(rr * f_j)
    rel_ref[0] = jnp.sqrt(rr / bb)
    place = own_x // groups
    for i in range(8):
        sol = jnp.zeros((SUBS, LANES), jnp.float32)
        res = sol
        for k in range(8):
            b = b_ref[row(k, i), window]
            z = z_ref[row(k, i), :]
            r = b - coef * (b - r_ref[row(k, i), window])
            turn = (k - place) % LANES
            sol = jnp.where(lane == k, pltpu.roll(z, turn, 1), sol)
            res = jnp.where(lane == k, pltpu.roll(r, turn, 1), res)
        sol_ref[i] = swap_rows(coef * sol, sub)
        res_ref[i] = swap_rows(res, sub)


def solve_all(nx, ny, meta, near, far, interpret=False):
    tables = Tables()
    wide = ny * nx // SUBS * LANES
    consts = [tables.even, tables.odd, tables.down0, tables.up0, tables.op1, tables.down1,
              tables.up1, tables.op2, tables.rows]
    vmem = pl.BlockSpec(memory_space=pltpu.VMEM)
    field = pltpu.VMEM((512, wide), jnp.float32)
    return pl.pallas_call(
        lambda *refs: kernel(nx, ny, tables, *refs),
        in_specs=[pl.BlockSpec(memory_space=pltpu.SMEM)] + [vmem] * 11,
        out_specs=[vmem, vmem, pl.BlockSpec(memory_space=pltpu.SMEM)],
        out_shape=[
            jax.ShapeDtypeStruct(near.shape[1:], jnp.float32),
            jax.ShapeDtypeStruct(near.shape[1:], jnp.float32),
            jax.ShapeDtypeStruct((1,), jnp.float32),
        ],
        scratch_shapes=[
            field, field, field, field, field, pltpu.VMEM((512, LANES), jnp.float32),
            pltpu.VMEM((256, wide), jnp.float32), pltpu.VMEM((256, wide), jnp.float32),
            pltpu.VMEM((768, wide), jnp.bfloat16), pltpu.VMEM((768, wide), jnp.bfloat16),
            pltpu.VMEM((1024, wide), jnp.bfloat16), pltpu.VMEM((152, wide), jnp.float32),
        ],
        name="solve_all",
        interpret=interpret,
    )(meta, *[pltpu.with_memory_space_constraint(x, pltpu.VMEM)
             for x in (near, far, *[jnp.asarray(c) for c in consts])])


def pack_kernel(forcing, kappa, sigma, out_ref, coef_ref):
    sub = lax.broadcasted_iota(jnp.int32, (SUBS, LANES), 0)
    lane = lax.broadcasted_iota(jnp.int32, (SUBS, LANES), 1)
    count = kappa.shape[2]
    coef_ref[...] = jnp.zeros((SUBS, LANES), jnp.float32)
    coef_ref[0:1, 0:count] = kappa[0]
    coef_ref[1:2, 0:count] = sigma[0]
    spread = jnp.take_along_axis(coef_ref[...], lane // SUBS, axis=1)
    for i in range(SUBS):
        x = swap_rows(forcing[i], sub)
        x = x + jnp.where(lane % SUBS == 0, pltpu.roll(x, 1, 1), 0.0)
        if i == 0:
            x = jnp.where(lane % SUBS == SUBS - 1, spread, x)
        out_ref[0, i] = x


def packed_block(forcing, kappa, sigma):
    vmem = pl.BlockSpec(memory_space=pltpu.VMEM)
    return pl.pallas_call(
        pack_kernel,
        in_specs=[vmem] * 3,
        out_specs=vmem,
        out_shape=jax.ShapeDtypeStruct((1, *forcing.shape), jnp.float32),
        scratch_shapes=[pltpu.VMEM((SUBS, LANES), jnp.float32)],
        name="pack_block",
    )(forcing, kappa, sigma)


def gathered(forcing, kappa, sigma):
    nx, ny = lax.axis_size("gx"), lax.axis_size("gy")
    block = packed_block(forcing, kappa, sigma)
    if ny > 1:
        other = lax.ppermute(block, "gy", [(i, i ^ 1) for i in range(ny)])
        block = jnp.concatenate([block, other], axis=0)
    step = nx // 2
    while step:
        other = lax.ppermute(block, "gx", [(i, i ^ step) for i in range(nx)])
        if step > 1:
            block = jnp.concatenate([block, other], axis=0)
        step //= 2
    meta = jnp.stack([lax.axis_index("gx"), lax.axis_index("gy")]).astype(jnp.int32)
    sol, res, rel = solve_all(nx, ny, meta, block, other)
    return sol, res, rel.reshape(())


def fits_one_device(mesh):
    nx, ny = mesh.shape["gx"], mesh.shape["gy"]
    power = nx & (nx - 1) == 0
    return power and nx % SUBS == 0 and ny <= 2 and nx * ny <= 64


def solution(mesh):
    spec = P("gx", "gy", None)
    small = fits_one_device(mesh)

    def local(forcing, kappa, sigma):
        plain = forcing.shape == (SUBS, SUBS, LANES) and kappa.shape == (1, 1, LANES // SUBS)
        return (gathered if small and plain else distributed)(forcing, kappa, sigma)

    return jax.shard_map(
        local, mesh=mesh, in_specs=(spec, spec, spec), out_specs=(spec, spec, P()),
        check_vma=False,
    )
```

```python
import jax
import jax.numpy as jnp
import numpy as np
from jax import lax
from jax.experimental import pallas as pl
from jax.experimental.pallas import tpu as pltpu
from jax.sharding import PartitionSpec as P


def with_halo(cells, sides, width):
    for axis, dim in sides:
        count = lax.axis_size(axis)
        head = lax.slice_in_dim(cells, 0, width, axis=dim)
        tail = lax.slice_in_dim(cells, cells.shape[dim] - width, cells.shape[dim], axis=dim)
        cells = jnp.concatenate(
            [
                lax.ppermute(tail, axis, [(i, (i + 1) % count) for i in range(count)]),
                cells,
                lax.ppermute(head, axis, [((i + 1) % count, i) for i in range(count)]),
            ],
            axis=dim,
        )
    return cells


def legendre_table(points, order):
    columns = [points * 0.0 + 1.0, points]
    for degree in range(2, order + 1):
        columns.append(
            ((2 * degree - 1) * points * columns[-1] - (degree - 1) * columns[-2]) / degree
        )
    return np.stack(columns, axis=1)


def lobatto(count):
    order = count - 1
    points = np.cos(np.pi * np.arange(count) / order)
    for sweep in range(60):
        table = legendre_table(points, order)
        points = points - (points * table[:, order] - table[:, order - 1]) / (
            count * table[:, order]
        )
    table = legendre_table(points, order)
    weights = 2.0 / (order * count * table[:, order] ** 2)
    values = table[:, order]
    points, weights, values = (points[::-1], weights[::-1], values[::-1])
    spread = points[:, None] - points[None, :] + np.eye(count)
    deriv = values[:, None] / values[None, :] / spread * (1.0 - np.eye(count))
    corner = order * (order + 1) / 4.0
    ends = np.array([-corner] + [0.0] * (count - 2) + [corner])
    return (points, weights, deriv + np.eye(count) * ends[None, :])


def lagrange(fine_points, coarse_points):
    columns = []
    for column in range(len(coarse_points)):
        value = fine_points * 0.0 + 1.0
        for other in range(len(coarse_points)):
            if other != column:
                value = (
                    value
                    * (fine_points - coarse_points[other])
                    / (coarse_points[column] - coarse_points[other])
                )
        columns.append(value)
    return np.stack(columns, axis=1)


def edge_factor(count, blocks):
    index = jnp.arange(count)
    single = jnp.where((index == 0) | (index == count - 1), 0.5, 1.0).astype(jnp.float32)
    return jnp.tile(single, blocks)


def multiplicity(count, blocks):
    first = edge_factor(count, blocks[0])
    second = edge_factor(count, blocks[1])
    third = edge_factor(count, blocks[2])
    return first[:, None, None] * second[None, :, None] * third[None, None, :]


def element_apply(field, kappa, sigma, deriv, weights):
    count = deriv.shape[0]
    ex, ey, ez = kappa.shape
    high = lax.Precision.HIGHEST
    block = field.reshape(ex, count, ey, count, ez, count)
    mass = (weights[:, None, None] * weights[None, :, None] * weights[None, None, :])[
        None, :, None, :, None, :
    ]
    first = jnp.einsum("ai,eifjgk->eafjgk", deriv, block, precision=high)
    total = jnp.einsum("ai,eafjgk->eifjgk", deriv, first * mass, precision=high)
    second = jnp.einsum("aj,eifjgk->eifagk", deriv, block, precision=high)
    total = total + jnp.einsum("aj,eifagk->eifjgk", deriv, second * mass, precision=high)
    third = jnp.einsum("ak,eifjgk->eifjga", deriv, block, precision=high)
    total = total + jnp.einsum("ak,eifjga->eifjgk", deriv, third * mass, precision=high)
    coeff = kappa[:, None, :, None, :, None]
    shift = sigma[:, None, :, None, :, None]
    return (coeff * total + shift * mass * block).reshape(field.shape)


def element_diagonal(kappa, sigma, deriv, weights):
    count = deriv.shape[0]
    ex, ey, ez = kappa.shape
    stiff = jnp.sum(deriv * deriv * weights[:, None], axis=0)
    term = stiff[:, None, None] * weights[None, :, None] * weights[None, None, :]
    term = term + weights[:, None, None] * stiff[None, :, None] * weights[None, None, :]
    term = term + weights[:, None, None] * weights[None, :, None] * stiff[None, None, :]
    mass = weights[:, None, None] * weights[None, :, None] * weights[None, None, :]
    coeff = kappa[:, None, :, None, :, None]
    shift = sigma[:, None, :, None, :, None]
    full = coeff * term[None, :, None, :, None, :] + shift * mass[None, :, None, :, None, :]
    return full.reshape(ex * count, ey * count, ez * count)


def fold_axis(field, dim, count):
    size = field.shape[dim]
    position = jnp.arange(size) % count
    shape = [1, 1, 1]
    shape[dim] = size
    first = (position == 0).reshape(shape)
    last = (position == count - 1).reshape(shape)
    before = jnp.roll(field, 1, dim)
    after = jnp.roll(field, -1, dim)
    return field + jnp.where(first, before, 0.0) + jnp.where(last, after, 0.0)


def fold_padded(padded, dim, count):
    size = padded.shape[dim] - 2
    center = lax.slice_in_dim(padded, 1, size + 1, axis=dim)
    before = lax.slice_in_dim(padded, 0, size, axis=dim)
    after = lax.slice_in_dim(padded, 2, size + 2, axis=dim)
    position = jnp.arange(size) % count
    shape = [1, 1, 1]
    shape[dim] = size
    first = (position == 0).reshape(shape)
    last = (position == count - 1).reshape(shape)
    return center + jnp.where(first, before, 0.0) + jnp.where(last, after, 0.0)


def assemble(field, count, finest):
    if finest:
        padded = with_halo(field, (("gx", 0), ("gy", 1)), 1)
        field = fold_padded(fold_padded(padded, 0, count), 1, count)
    else:
        padded = with_halo(field, (("gx", 0), ("gy", 1)), 1)
        field = fold_padded(fold_padded(padded, 0, count), 1, count)
    return fold_axis(field, 2, count)


def restrict(field, interp, blocks, fine_count, coarse_count):
    high = lax.Precision.HIGHEST
    block = field.reshape(blocks[0], fine_count, blocks[1], fine_count, blocks[2], fine_count)
    one = jnp.einsum("ia,eifjgk->eafjgk", interp, block, precision=high)
    two = jnp.einsum("jb,eafjgk->eafbgk", interp, one, precision=high)
    three = jnp.einsum("kc,eafbgk->eafbgc", interp, two, precision=high)
    return three.reshape(
        blocks[0] * coarse_count, blocks[1] * coarse_count, blocks[2] * coarse_count
    )


def prolong(field, interp, blocks, fine_count, coarse_count):
    high = lax.Precision.HIGHEST
    block = field.reshape(blocks[0], coarse_count, blocks[1], coarse_count, blocks[2], coarse_count)
    one = jnp.einsum("ia,eafbgc->eifbgc", interp, block, precision=high)
    two = jnp.einsum("jb,eifbgc->eifjgc", interp, one, precision=high)
    three = jnp.einsum("kc,eifjgc->eifjgk", interp, two, precision=high)
    return three.reshape(blocks[0] * fine_count, blocks[1] * fine_count, blocks[2] * fine_count)


def distributed(forcing, kappa, sigma):
    blocks = kappa.shape
    counts = [8, 4, 2]
    tables = [lobatto(count) for count in counts]
    derivs = [jnp.asarray(table[2], jnp.float32) for table in tables]
    weights = [jnp.asarray(table[1], jnp.float32) for table in tables]
    interps = [
        jnp.asarray(lagrange(tables[level][0], tables[level + 1][0]), jnp.float32)
        for level in range(2)
    ]
    mults = [multiplicity(count, blocks) for count in counts]
    diags = [
        assemble(
            element_diagonal(kappa, sigma, derivs[level], weights[level]), counts[level], level == 0
        )
        for level in range(3)
    ]
    center = 1.65
    half = 1.35
    ratio = center / half

    def operate(field, level):
        return assemble(
            element_apply(field, kappa, sigma, derivs[level], weights[level]),
            counts[level],
            level == 0,
        )

    def smooth(resid, level, steps, keep_last):
        rho = 1.0 / ratio
        direction = resid / (center * diags[level])
        iterate = direction
        for step in range(steps):
            if step > 0:
                rho_next = 1.0 / (2.0 * ratio - rho)
                direction = (
                    rho_next * rho * direction + 2.0 * rho_next / half * resid / diags[level]
                )
                iterate = iterate + direction
                rho = rho_next
            if step < steps - 1 or keep_last:
                resid = resid - operate(direction, level)
        return (iterate, resid)

    def vcycle(resid, level):
        if level == 2:
            iterate, unused = smooth(resid, level, 2, False)
            return iterate
        iterate, resid = smooth(resid, level, 2, True)
        coarse = assemble(
            restrict(
                mults[level] * resid, interps[level], blocks, counts[level], counts[level + 1]
            ),
            counts[level + 1],
            False,
        )
        correction = prolong(
            vcycle(coarse, level + 1), interps[level], blocks, counts[level], counts[level + 1]
        )
        iterate = iterate + correction
        resid = resid - operate(correction, level)
        return iterate + resid / (center * diags[level])

    load = assemble(forcing, 8, True)
    first = vcycle(load, 0)
    image_first = operate(first, 0)
    second = vcycle(load - image_first, 0)
    combined = first + second
    image = operate(combined, 0)
    weight = mults[0]
    load_sq, load_image, image_sq = lax.psum(
        (
            jnp.sum(weight * load * load),
            jnp.sum(weight * load * image),
            jnp.sum(weight * image * image),
        ),
        ("gx", "gy"),
    )
    coef = load_image / image_sq
    solution = coef * combined
    residual = load - coef * image
    rel_residual = jnp.sqrt((load_sq - load_image * load_image / image_sq) / load_sq)
    return (solution, residual, rel_residual)


THETA = 1.65
DELTA = 1.35
RATIO = THETA / DELTA
RHO0 = 1.0 / RATIO
RHO1 = 1.0 / (2.0 * RATIO - RHO0)
KEEP = RHO1 * RHO0
PUSH = 2.0 * RHO1 / DELTA
LANES = 128
SUBS = 8


def triple(first, second, third):
    return np.kron(first, np.kron(second, third))


def split_const(matrix):
    high = matrix.astype(jnp.bfloat16)
    low = (matrix - high.astype(np.float64)).astype(jnp.bfloat16)
    return high, low


def stacked(matrix):
    high, low = split_const(matrix)
    return np.concatenate([high, high, low], axis=1)


J_ORDER = (0, 1, 2, 3, 7, 5, 6, 4)
PAIRS = ((0, 7), (1, 2), (3, 4), (5, 6))
FACE = (0, 1, 3, 2)
ROWS1 = tuple(
    (k * 4 + FACE[2 * ih + il]) * 4 + FACE[2 * jh + jl]
    for k in range(4) for ih in range(2) for jh in range(2) for il in range(2) for jl in range(2)
)
ROWS2 = tuple((k * 2 + i) * 2 + j for j in range(2) for k in range(2) for i in range(2))


def padded(matrix, rows, columns):
    return np.pad(matrix, ((0, rows - matrix.shape[0]), (0, columns - matrix.shape[1])))


class Tables:
    def __init__(self):
        tables = [lobatto(count) for count in (8, 4, 2)]
        self.weights = [table[1] for table in tables]
        stiff = [table[2].T @ np.diag(table[1]) @ table[2] for table in tables]
        self.squares = [np.sum(t[2] * t[2] * t[1][:, None], axis=0) for t in tables]
        interps = [lagrange(tables[level][0], tables[level + 1][0]) for level in range(2)]
        factor = [np.where((np.arange(n) == 0) | (np.arange(n) == n - 1), 0.5, 1.0) for n in (8, 4)]
        down = [interps[level].T * factor[level][None, :] for level in range(2)]
        flat = [i for pair in PAIRS for i in pair]
        rows0 = [(k * 8 + i) * 8 + j for k in range(8) for i in range(8) for j in J_ORDER]
        data0 = [(k * 8 + i) * 8 + j for k in range(8) for i in flat for j in J_ORDER]
        rows1, rows2 = list(ROWS1), list(ROWS2)
        w, k = np.diag(self.weights[0]), stiff[0]
        plane = np.kron(k, w) + np.kron(w, k)
        both = np.kron(w, w)
        flip = k[:4, ::-1][:, :4]
        half = np.kron(0.5 * w[:4, :4], plane)
        even = np.kron(0.5 * (k[:4, :4] + flip), both) + half
        odd = np.kron(0.5 * (k[:4, :4] - flip), both) + half
        self.even = stacked(even[np.ix_(rows0[:256], data0[:256])])
        self.odd = stacked(odd[np.ix_(rows0[:256], data0[:256])])
        high, low = split_const(triple(down[0], down[0], down[0])[np.ix_(rows1, data0)])
        self.down0 = np.concatenate([high, low], axis=0)
        self.up0 = stacked(triple(interps[0], interps[0], interps[0])[np.ix_(rows0, rows1)])
        w, k = np.diag(self.weights[1]), stiff[1]
        self.op1 = stacked((triple(k, w, w) + triple(w, k, w) + triple(w, w, k))[np.ix_(rows1, rows1)])
        self.down1 = padded(stacked(triple(down[1], down[1], down[1])[np.ix_(rows2, rows1)]), 16, 192)
        self.up1 = padded(stacked(triple(interps[1], interps[1], interps[1])[np.ix_(rows1, rows2)]), 64, 32)
        w, k = np.diag(self.weights[2]), stiff[2]
        self.op2 = padded(
            stacked((triple(k, w, w) + triple(w, k, w) + triple(w, w, k))[np.ix_(rows2, rows2)]), 16, 32)
        wide = lambda column: np.repeat(np.asarray(column, np.float32)[:, None], LANES, axis=1)
        blocks = [wide(self.weights[0][list(J_ORDER)]), wide(self.squares[0][list(J_ORDER)]),
                  wide(factor[0][list(J_ORDER)])]
        for level, order in ((1, rows1), (2, rows2)):
            a, b = self.weights[level], self.squares[level]
            blocks.append(wide(triple(a, a, a)[order]))
            blocks.append(wide((triple(b, a, a) + triple(a, b, a) + triple(a, a, b))[order]))
        self.rows = np.concatenate(blocks, axis=0)


def swap_rows(x, sub):
    return jnp.where(sub == 4, pltpu.roll(x, 5, 0), jnp.where(sub == 7, pltpu.roll(x, 3, 0), x))


def kernel(nx, ny, tables, near, far, even, odd, down0, up0, op1, down1, up1, op2, rows,
           sol_ref, res_ref, rel_ref, b_ref, r_ref, d_ref, v_ref, p_ref, z_ref, re_ref, ro_ref,
           be_ref, bo_ref, c_ref, lane_ref):
    groups = nx // SUBS
    tiles = ny * groups
    wide = tiles * LANES
    own_x, own_y = lax.axis_index("gx"), lax.axis_index("gy")
    sub = lax.broadcasted_iota(jnp.int32, (SUBS, LANES), 0)
    lane = lax.broadcasted_iota(jnp.int32, (SUBS, LANES), 1) % SUBS
    w = [float(x) for x in tables.weights[0]]
    q = [float(x) for x in tables.squares[0]]
    f = [0.5 if k in (0, 7) else 1.0 for k in range(8)]

    def cols(x):
        return [x[:, t * LANES:(t + 1) * LANES] for t in range(tiles)]

    def join(parts):
        return jnp.concatenate(parts, axis=1)

    def across(x):
        return join([x] * tiles)

    sub_w = across(sub)

    def x_up(x, more=0):
        parts, out = cols(x), []
        for t in range(tiles):
            if t % groups:
                prev = parts[t - 1]
                out.append(pltpu.roll(prev, more, 1) if more else prev)
            else:
                prev = parts[t + groups - 1]
                out.append(jnp.where(lane == 0, pltpu.roll(prev, (LANES - SUBS + 1 + more) % LANES, 1),
                                     pltpu.roll(prev, 1 + more, 1)))
        return join(out)

    def x_down(x, more=0):
        parts, out = cols(x), []
        for t in range(tiles):
            if t % groups < groups - 1:
                succ = parts[t + 1]
                out.append(pltpu.roll(succ, more, 1) if more else succ)
            else:
                succ = parts[t - groups + 1]
                out.append(jnp.where(lane == SUBS - 1, pltpu.roll(succ, SUBS - 1 + more, 1),
                                     pltpu.roll(succ, (LANES - 1 + more) % LANES, 1)))
        return join(out)

    up, down = SUBS, LANES - SUBS

    def z_up(x):
        return join([pltpu.roll(p, up, 1) for p in cols(x)])

    def z_down(x):
        return join([pltpu.roll(p, down, 1) for p in cols(x)])

    def y_fold(x, face):
        parts = cols(x)
        other = join([parts[(t + groups) % tiles] for t in range(tiles)])
        return x + jnp.where(face, pltpu.roll(other, 4, 0), 0.0)

    face0 = sub_w % 4 == 0
    face1 = sub_w % 2 == 0

    def row(k, i):
        return pl.ds(k * 64 + i * 8, 8)

    for t in range(tiles):
        y_index, part = t // groups, t % groups
        use_near = ((part ^ own_x) & 1) == 0
        slots = []
        for c in range(SUBS):
            delta = (c * groups + part) ^ own_x
            slot, bit = jnp.int32(0), 0
            if ny > 1:
                slot, bit = y_index ^ own_y, 1
            step = nx // 2
            while step > 1:
                flag = jnp.where((delta & step) != 0, 1, 0)
                slot = slot + flag * (1 << bit)
                bit += 1
                step //= 2
            slots.append(slot)
        for i in range(8):
            block = [jnp.where(use_near, near[slot, i], far[slot, i]) for slot in slots]
            for step in (1, 2, 4):
                out = list(block)
                for c in range(SUBS):
                    if not c & step:
                        a, b = block[c], block[c + step]
                        keep = (lane & step) == 0
                        out[c] = jnp.where(keep, a, pltpu.roll(b, step, 1))
                        out[c + step] = jnp.where(keep, pltpu.roll(a, LANES - step, 1), b)
                block = out
            for k in range(7):
                v_ref[row(k, i), t * LANES:(t + 1) * LANES] = block[k]
            v_ref[row(7, i), t * LANES:(t + 1) * LANES] = pltpu.roll(block[0], LANES - SUBS, 1)
            if i == 0:
                lane_ref[0:8, t * LANES:(t + 1) * LANES] = block[7]
    kap1 = lane_ref[0:1, :]
    sig1 = lane_ref[1:2, :]
    kap = jnp.broadcast_to(kap1, (SUBS, wide))
    sig = jnp.broadcast_to(sig1, (SUBS, wide))
    w_j = across(rows[0:8, :])
    q_j = across(rows[8:16, :])
    f_j = across(rows[16:24, :])
    sig_w = sig * w_j

    def store_split(kk, index, low_pair, high_pair):
        a = jnp.concatenate(low_pair, axis=0)
        b = jnp.concatenate(high_pair, axis=0)
        for ref, value in ((be_ref, a + b), (bo_ref, a - b)):
            high = value.astype(jnp.bfloat16)
            low = (value - high.astype(jnp.float32)).astype(jnp.bfloat16)
            at = kk * 64 + index * 16
            ref[at:at + 16, :] = high
            ref[256 + at:272 + at, :] = low
            ref[512 + at:528 + at, :] = high

    def fold_pairs(kk, get, index):
        out = []
        for i in PAIRS[index]:
            a, b = get(kk, i), get(7 - kk, i)
            out.append((a, b))
        return out

    def assemble_pairs(kk, index, values, with_z=True):
        vals = [list(v) for v in values]
        if kk == 0 and with_z:
            for v in vals:
                a, b = v
                v[0] = a + z_up(b)
                v[1] = b + z_down(a)
        if index == 0:
            for s in range(2):
                a, b = vals[0][s], vals[1][s]
                vals[0][s] = a + x_up(b)
                vals[1][s] = b + x_down(a)
        return [[y_fold(x, face0) for x in v] for v in vals]

    def point(k, i):
        s1 = q[k] * w[i] + w[k] * q[i]
        s2 = w[k] * w[i]
        return kap * (s1 * w_j + s2 * q_j) + s2 * sig_w

    for kk in range(4):
        for index, pair in enumerate(PAIRS):
            diag = assemble_pairs(kk, index, fold_pairs(kk, point, index))
            load = assemble_pairs(
                kk, index, fold_pairs(kk, lambda k, i: v_ref[row(k, i), :], index), with_z=False)
            dirs = []
            for s, k in enumerate((kk, 7 - kk)):
                group = []
                for n, i in enumerate(pair):
                    inverse = 1.0 / diag[n][s]
                    b_ref[row(k, i), :] = load[n][s]
                    r_ref[row(k, i), :] = load[n][s]
                    scaled = inverse * (1.0 / THETA)
                    p_ref[row(k, i), :] = inverse * PUSH
                    first = load[n][s] * scaled
                    d_ref[row(k, i), :] = first
                    group.append((first, scaled))
                dirs.append([g[0] for g in group])
                for n, i in enumerate(pair):
                    v_ref[row(k, i), :] = group[n][1]
            store_split(kk, index, dirs[0], dirs[1])

    def tile_rows(x):
        return jnp.concatenate([x] * tiles, axis=1)

    low_face = (sub_w // 2) % 2 == 0

    def fold1(x):
        p = [(x[16 * k:16 * k + 8], x[16 * k + 8:16 * k + 16]) for k in range(4)]
        out = []
        for k, (a, b) in enumerate(p):
            na, nb = x_up(b), x_down(a)
            if k in (0, 3):
                c, e = p[3 - k]
                move, amount = (z_up, up) if k == 0 else (z_down, down)
                na = na + x_up(e, amount)
                nb = nb + x_down(c, amount)
                a, b = a + move(c), b + move(e)
            out.append(y_fold(a + jnp.where(low_face, na, 0.0), face1))
            out.append(y_fold(b + jnp.where(low_face, nb, 0.0), face1))
        return jnp.concatenate(out, axis=0)

    first_k = (sub_w // 2) % 2 == 0
    first_i = sub_w % 2 == 0

    def fold2(x):
        other_k = jnp.where(first_k, pltpu.roll(x, 6, 0), pltpu.roll(x, 2, 0))
        other_i = jnp.where(first_i, pltpu.roll(x, 7, 0), pltpu.roll(x, 1, 0))
        both = jnp.where(first_i, pltpu.roll(other_k, 7, 0), pltpu.roll(other_k, 1, 0))
        x = x + jnp.where(first_k, z_up(other_k), z_down(other_k))
        x = x + jnp.where(first_i, x_up(other_i), x_down(other_i))
        x = x + jnp.where(first_k, jnp.where(first_i, x_up(both, up), x_down(both, up)),
                          jnp.where(first_i, x_up(both, down), x_down(both, down)))
        return y_fold(x, sub_w >= 0)

    def cat3(x):
        high = x.astype(jnp.bfloat16)
        low = (x - high.astype(jnp.float32)).astype(jnp.bfloat16)
        return jnp.concatenate([high, low, high], axis=0)

    def cat3_small(x):
        high = x.astype(jnp.bfloat16).astype(jnp.float32)
        return jnp.concatenate([high, x - high, high, jnp.zeros_like(x)], axis=0).astype(jnp.bfloat16)

    def dot(a, b):
        return jnp.dot(a, b, preferred_element_type=jnp.float32)

    mass1 = tile_rows(rows[24:88, :])
    point1 = tile_rows(rows[88:152, :])
    mass2 = tile_rows(rows[152:160, :])
    point2 = tile_rows(rows[160:168, :])
    inv1_ref, mass1_ref = lane_ref.at[8:72, :], lane_ref.at[72:136, :]
    inv1_ref[...] = 1.0 / fold1(kap1 * point1 + sig1 * mass1)
    mass1_ref[...] = sig1 * mass1
    inv2 = 1.0 / fold2(kap1 * point2 + sig1 * mass2)
    lane_ref[136:144, :] = inv2
    lane_ref[144:152, :] = sig1 * mass2

    def apply1(v):
        return fold1(kap1 * dot(op1[...], cat3(v)) + mass1_ref[...] * v)

    def apply2(v):
        return fold2(kap1 * dot(op2[...], cat3_small(v))[0:8] + lane_ref[144:152, :] * v)

    def coarse(resid):
        inverse = inv1_ref[...]
        d = resid * inverse * (1.0 / THETA)
        x = d
        resid = resid - apply1(d)
        d = KEEP * d + PUSH * (resid * inverse)
        x = x + d
        resid = resid - apply1(d)
        low = fold2(dot(down1[...], cat3(resid))[0:8])
        inverse2 = lane_ref[136:144, :]
        d = low * inverse2 * (1.0 / THETA)
        y = d
        low = low - apply2(d)
        y = y + KEEP * d + PUSH * (low * inverse2)
        e = dot(up1[...], cat3_small(y))
        x = x + e
        resid = resid - apply1(e)
        return x + resid * inverse * (1.0 / THETA)

    def multiply():
        re_ref[...] = dot(even[...], be_ref[...])
        ro_ref[...] = dot(odd[...], bo_ref[...])

    def image(kk, index):
        values = []
        for i in PAIRS[index]:
            e = re_ref[row(kk, i), :]
            o = ro_ref[row(kk, i), :]
            scale = sig_w * (w[kk] * w[i])
            values.append((kap * (e + o) + scale * d_ref[row(kk, i), :],
                           kap * (e - o) + scale * d_ref[row(7 - kk, i), :]))
        return assemble_pairs(kk, index, values)

    def sweep(update):
        multiply()
        for kk in range(4):
            for index, pair in enumerate(PAIRS):
                out = image(kk, index)
                dirs = []
                for s, k in enumerate((kk, 7 - kk)):
                    dirs.append([update(k, i, out[n][s]) for n, i in enumerate(pair)])
                yield kk, index, dirs

    def second_direction(k, i, value):
        r = r_ref[row(k, i), :] - value
        r_ref[row(k, i), :] = r
        first = d_ref[row(k, i), :]
        return KEEP * first + r * p_ref[row(k, i), :]

    def residual_only(k, i, value):
        r = r_ref[row(k, i), :] - value
        r_ref[row(k, i), :] = r
        return r

    def next_direction(k, i, value):
        r = r_ref[row(k, i), :] - value
        r_ref[row(k, i), :] = r
        return r * v_ref[row(k, i), :]

    def run(update, keep):
        for kk, index, dirs in sweep(update):
            if keep:
                for s, k in enumerate((kk, 7 - kk)):
                    for n, i in enumerate(PAIRS[index]):
                        d_ref[row(k, i), :] = dirs[s][n]
                store_split(kk, index, dirs[0], dirs[1])
            else:
                for s, k in enumerate((kk, 7 - kk)):
                    value = jnp.concatenate(dirs[s], axis=0)
                    high = value.astype(jnp.bfloat16)
                    low = (value - high.astype(jnp.float32)).astype(jnp.bfloat16)
                    at = k * 64 + index * 16
                    c_ref[at:at + 16, :] = high
                    c_ref[512 + at:528 + at, :] = low

    start = pl.multiple_of((own_y * groups + own_x % groups) * LANES, LANES)
    window = pl.ds(start, LANES)
    z_ref[...] = jnp.zeros((512, LANES), jnp.float32)

    def collect():
        z_ref[...] = z_ref[...] + d_ref[:, window]

    def cycle():
        collect()
        run(second_direction, True)
        collect()
        run(residual_only, False)
        both = dot(down0[...], c_ref[0:512, :])
        low = both[0:64] + both[64:128] + dot(down0[0:64, :], c_ref[512:1024, :])
        correction = coarse(fold1(low))
        d_ref[...] = dot(up0[...], cat3(correction))
        collect()
        for kk in range(4):
            for index, pair in enumerate(PAIRS):
                store_split(kk, index, *[[d_ref[row(k, i), :] for i in pair] for k in (kk, 7 - kk)])
        run(next_direction, True)
        collect()
        run(next_direction, True)

    cycle()
    cycle()

    zero = jnp.zeros((SUBS, wide), jnp.float32)
    bw, ww, bb = zero, zero, zero
    for k in range(8):
        for i in range(8):
            b = b_ref[row(k, i), :]
            image_all = b - r_ref[row(k, i), :]
            fb = b * (f[k] * f[i])
            bw = bw + fb * image_all
            ww = ww + image_all * image_all * (f[k] * f[i])
            bb = bb + fb * b
    bw, ww, bb = jnp.sum(bw * f_j), jnp.sum(ww * f_j), jnp.sum(bb * f_j)
    coef = bw / ww
    rr = zero
    for k in range(8):
        for i in range(8):
            b = b_ref[row(k, i), :]
            res = b - coef * (b - r_ref[row(k, i), :])
            rr = rr + res * res * (f[k] * f[i])
    rr = jnp.sum(rr * f_j)
    rel_ref[0] = jnp.sqrt(rr / bb)
    place = own_x // groups
    for i in range(8):
        sol = jnp.zeros((SUBS, LANES), jnp.float32)
        res = sol
        for k in range(8):
            b = b_ref[row(k, i), window]
            z = z_ref[row(k, i), :]
            r = b - coef * (b - r_ref[row(k, i), window])
            turn = (k - place) % LANES
            sol = jnp.where(lane == k, pltpu.roll(z, turn, 1), sol)
            res = jnp.where(lane == k, pltpu.roll(r, turn, 1), res)
        sol_ref[i] = swap_rows(coef * sol, sub)
        res_ref[i] = swap_rows(res, sub)


def solve_all(nx, ny, near, far):
    tables = Tables()
    wide = ny * nx // SUBS * LANES
    consts = [tables.even, tables.odd, tables.down0, tables.up0, tables.op1, tables.down1,
              tables.up1, tables.op2, tables.rows]
    vmem = pl.BlockSpec(memory_space=pltpu.VMEM)
    field = pltpu.VMEM((512, wide), jnp.float32)
    return pl.pallas_call(
        lambda *refs: kernel(nx, ny, tables, *refs),
        in_specs=[vmem] * 11,
        out_specs=[vmem, vmem, pl.BlockSpec(memory_space=pltpu.SMEM)],
        out_shape=[
            jax.ShapeDtypeStruct(near.shape[1:], jnp.float32),
            jax.ShapeDtypeStruct(near.shape[1:], jnp.float32),
            jax.ShapeDtypeStruct((1,), jnp.float32),
        ],
        scratch_shapes=[
            field, field, field, field, field, pltpu.VMEM((512, LANES), jnp.float32),
            pltpu.VMEM((256, wide), jnp.float32), pltpu.VMEM((256, wide), jnp.float32),
            pltpu.VMEM((768, wide), jnp.bfloat16), pltpu.VMEM((768, wide), jnp.bfloat16),
            pltpu.VMEM((1024, wide), jnp.bfloat16), pltpu.VMEM((152, wide), jnp.float32),
        ],
        name="solve_all",
    )(*[pltpu.with_memory_space_constraint(x, pltpu.VMEM)
             for x in (near, far, *[jnp.asarray(c) for c in consts])])


def pack_kernel(forcing, kappa, sigma, out_ref, coef_ref):
    sub = lax.broadcasted_iota(jnp.int32, (SUBS, LANES), 0)
    lane = lax.broadcasted_iota(jnp.int32, (SUBS, LANES), 1)
    count = kappa.shape[2]
    coef_ref[...] = jnp.zeros((SUBS, LANES), jnp.float32)
    coef_ref[0:1, 0:count] = kappa[0]
    coef_ref[1:2, 0:count] = sigma[0]
    spread = jnp.take_along_axis(coef_ref[...], lane // SUBS, axis=1)
    for i in range(SUBS):
        x = swap_rows(forcing[i], sub)
        x = x + jnp.where(lane % SUBS == 0, pltpu.roll(x, 1, 1), 0.0)
        if i == 0:
            x = jnp.where(lane % SUBS == SUBS - 1, spread, x)
        out_ref[0, i] = x


def packed_block(forcing, kappa, sigma):
    vmem = pl.BlockSpec(memory_space=pltpu.VMEM)
    return pl.pallas_call(
        pack_kernel,
        in_specs=[vmem] * 3,
        out_specs=vmem,
        out_shape=pltpu.VMEM((1, *forcing.shape), jnp.float32),
        scratch_shapes=[pltpu.VMEM((SUBS, LANES), jnp.float32)],
        name="pack_block",
    )(forcing, kappa, sigma)


def gathered(forcing, kappa, sigma):
    nx, ny = lax.axis_size("gx"), lax.axis_size("gy")
    block = packed_block(forcing, kappa, sigma)
    if ny > 1:
        other = lax.ppermute(block, "gy", [(i, i ^ 1) for i in range(ny)])
        block = jnp.concatenate([block, other], axis=0)
    step = nx // 2
    while step:
        other = lax.ppermute(block, "gx", [(i, i ^ step) for i in range(nx)])
        if step > 1:
            block = jnp.concatenate([block, other], axis=0)
        step //= 2
    sol, res, rel = solve_all(nx, ny, block, other)
    return sol, res, rel.reshape(())


def fits_one_device(mesh):
    nx, ny = mesh.shape["gx"], mesh.shape["gy"]
    power = nx & (nx - 1) == 0
    return power and nx % SUBS == 0 and ny <= 2 and nx * ny <= 64


def solution(mesh):
    spec = P("gx", "gy", None)
    small = fits_one_device(mesh)

    def local(forcing, kappa, sigma):
        plain = forcing.shape == (SUBS, SUBS, LANES) and kappa.shape == (1, 1, LANES // SUBS)
        return (gathered if small and plain else distributed)(forcing, kappa, sigma)

    return jax.shard_map(
        local, mesh=mesh, in_specs=(spec, spec, spec), out_specs=(spec, spec, P()),
        check_vma=False,
    )
```

```python
import jax
import jax.numpy as jnp
import numpy as np
from jax import lax
from jax.experimental import pallas as pl
from jax.experimental.pallas import tpu as pltpu
from jax.sharding import PartitionSpec as P


def with_halo(cells, sides, width):
    for axis, dim in sides:
        count = lax.axis_size(axis)
        head = lax.slice_in_dim(cells, 0, width, axis=dim)
        tail = lax.slice_in_dim(cells, cells.shape[dim] - width, cells.shape[dim], axis=dim)
        cells = jnp.concatenate(
            [
                lax.ppermute(tail, axis, [(i, (i + 1) % count) for i in range(count)]),
                cells,
                lax.ppermute(head, axis, [((i + 1) % count, i) for i in range(count)]),
            ],
            axis=dim,
        )
    return cells


def legendre_table(points, order):
    columns = [points * 0.0 + 1.0, points]
    for degree in range(2, order + 1):
        columns.append(
            ((2 * degree - 1) * points * columns[-1] - (degree - 1) * columns[-2]) / degree
        )
    return np.stack(columns, axis=1)


def lobatto(count):
    order = count - 1
    points = np.cos(np.pi * np.arange(count) / order)
    for sweep in range(60):
        table = legendre_table(points, order)
        points = points - (points * table[:, order] - table[:, order - 1]) / (
            count * table[:, order]
        )
    table = legendre_table(points, order)
    weights = 2.0 / (order * count * table[:, order] ** 2)
    values = table[:, order]
    points, weights, values = (points[::-1], weights[::-1], values[::-1])
    spread = points[:, None] - points[None, :] + np.eye(count)
    deriv = values[:, None] / values[None, :] / spread * (1.0 - np.eye(count))
    corner = order * (order + 1) / 4.0
    ends = np.array([-corner] + [0.0] * (count - 2) + [corner])
    return (points, weights, deriv + np.eye(count) * ends[None, :])


def lagrange(fine_points, coarse_points):
    columns = []
    for column in range(len(coarse_points)):
        value = fine_points * 0.0 + 1.0
        for other in range(len(coarse_points)):
            if other != column:
                value = (
                    value
                    * (fine_points - coarse_points[other])
                    / (coarse_points[column] - coarse_points[other])
                )
        columns.append(value)
    return np.stack(columns, axis=1)


def edge_factor(count, blocks):
    index = jnp.arange(count)
    single = jnp.where((index == 0) | (index == count - 1), 0.5, 1.0).astype(jnp.float32)
    return jnp.tile(single, blocks)


def multiplicity(count, blocks):
    first = edge_factor(count, blocks[0])
    second = edge_factor(count, blocks[1])
    third = edge_factor(count, blocks[2])
    return first[:, None, None] * second[None, :, None] * third[None, None, :]


def element_apply(field, kappa, sigma, deriv, weights):
    count = deriv.shape[0]
    ex, ey, ez = kappa.shape
    high = lax.Precision.HIGHEST
    block = field.reshape(ex, count, ey, count, ez, count)
    mass = (weights[:, None, None] * weights[None, :, None] * weights[None, None, :])[
        None, :, None, :, None, :
    ]
    first = jnp.einsum("ai,eifjgk->eafjgk", deriv, block, precision=high)
    total = jnp.einsum("ai,eafjgk->eifjgk", deriv, first * mass, precision=high)
    second = jnp.einsum("aj,eifjgk->eifagk", deriv, block, precision=high)
    total = total + jnp.einsum("aj,eifagk->eifjgk", deriv, second * mass, precision=high)
    third = jnp.einsum("ak,eifjgk->eifjga", deriv, block, precision=high)
    total = total + jnp.einsum("ak,eifjga->eifjgk", deriv, third * mass, precision=high)
    coeff = kappa[:, None, :, None, :, None]
    shift = sigma[:, None, :, None, :, None]
    return (coeff * total + shift * mass * block).reshape(field.shape)


def element_diagonal(kappa, sigma, deriv, weights):
    count = deriv.shape[0]
    ex, ey, ez = kappa.shape
    stiff = jnp.sum(deriv * deriv * weights[:, None], axis=0)
    term = stiff[:, None, None] * weights[None, :, None] * weights[None, None, :]
    term = term + weights[:, None, None] * stiff[None, :, None] * weights[None, None, :]
    term = term + weights[:, None, None] * weights[None, :, None] * stiff[None, None, :]
    mass = weights[:, None, None] * weights[None, :, None] * weights[None, None, :]
    coeff = kappa[:, None, :, None, :, None]
    shift = sigma[:, None, :, None, :, None]
    full = coeff * term[None, :, None, :, None, :] + shift * mass[None, :, None, :, None, :]
    return full.reshape(ex * count, ey * count, ez * count)


def fold_axis(field, dim, count):
    size = field.shape[dim]
    position = jnp.arange(size) % count
    shape = [1, 1, 1]
    shape[dim] = size
    first = (position == 0).reshape(shape)
    last = (position == count - 1).reshape(shape)
    before = jnp.roll(field, 1, dim)
    after = jnp.roll(field, -1, dim)
    return field + jnp.where(first, before, 0.0) + jnp.where(last, after, 0.0)


def fold_padded(padded, dim, count):
    size = padded.shape[dim] - 2
    center = lax.slice_in_dim(padded, 1, size + 1, axis=dim)
    before = lax.slice_in_dim(padded, 0, size, axis=dim)
    after = lax.slice_in_dim(padded, 2, size + 2, axis=dim)
    position = jnp.arange(size) % count
    shape = [1, 1, 1]
    shape[dim] = size
    first = (position == 0).reshape(shape)
    last = (position == count - 1).reshape(shape)
    return center + jnp.where(first, before, 0.0) + jnp.where(last, after, 0.0)


def assemble(field, count, finest):
    if finest:
        padded = with_halo(field, (("gx", 0), ("gy", 1)), 1)
        field = fold_padded(fold_padded(padded, 0, count), 1, count)
    else:
        padded = with_halo(field, (("gx", 0), ("gy", 1)), 1)
        field = fold_padded(fold_padded(padded, 0, count), 1, count)
    return fold_axis(field, 2, count)


def restrict(field, interp, blocks, fine_count, coarse_count):
    high = lax.Precision.HIGHEST
    block = field.reshape(blocks[0], fine_count, blocks[1], fine_count, blocks[2], fine_count)
    one = jnp.einsum("ia,eifjgk->eafjgk", interp, block, precision=high)
    two = jnp.einsum("jb,eafjgk->eafbgk", interp, one, precision=high)
    three = jnp.einsum("kc,eafbgk->eafbgc", interp, two, precision=high)
    return three.reshape(
        blocks[0] * coarse_count, blocks[1] * coarse_count, blocks[2] * coarse_count
    )


def prolong(field, interp, blocks, fine_count, coarse_count):
    high = lax.Precision.HIGHEST
    block = field.reshape(blocks[0], coarse_count, blocks[1], coarse_count, blocks[2], coarse_count)
    one = jnp.einsum("ia,eafbgc->eifbgc", interp, block, precision=high)
    two = jnp.einsum("jb,eifbgc->eifjgc", interp, one, precision=high)
    three = jnp.einsum("kc,eifjgc->eifjgk", interp, two, precision=high)
    return three.reshape(blocks[0] * fine_count, blocks[1] * fine_count, blocks[2] * fine_count)


def distributed(forcing, kappa, sigma):
    blocks = kappa.shape
    counts = [8, 4, 2]
    tables = [lobatto(count) for count in counts]
    derivs = [jnp.asarray(table[2], jnp.float32) for table in tables]
    weights = [jnp.asarray(table[1], jnp.float32) for table in tables]
    interps = [
        jnp.asarray(lagrange(tables[level][0], tables[level + 1][0]), jnp.float32)
        for level in range(2)
    ]
    mults = [multiplicity(count, blocks) for count in counts]
    diags = [
        assemble(
            element_diagonal(kappa, sigma, derivs[level], weights[level]), counts[level], level == 0
        )
        for level in range(3)
    ]
    center = 1.65
    half = 1.35
    ratio = center / half

    def operate(field, level):
        return assemble(
            element_apply(field, kappa, sigma, derivs[level], weights[level]),
            counts[level],
            level == 0,
        )

    def smooth(resid, level, steps, keep_last):
        rho = 1.0 / ratio
        direction = resid / (center * diags[level])
        iterate = direction
        for step in range(steps):
            if step > 0:
                rho_next = 1.0 / (2.0 * ratio - rho)
                direction = (
                    rho_next * rho * direction + 2.0 * rho_next / half * resid / diags[level]
                )
                iterate = iterate + direction
                rho = rho_next
            if step < steps - 1 or keep_last:
                resid = resid - operate(direction, level)
        return (iterate, resid)

    def vcycle(resid, level):
        if level == 2:
            iterate, unused = smooth(resid, level, 2, False)
            return iterate
        iterate, resid = smooth(resid, level, 2, True)
        coarse = assemble(
            restrict(
                mults[level] * resid, interps[level], blocks, counts[level], counts[level + 1]
            ),
            counts[level + 1],
            False,
        )
        correction = prolong(
            vcycle(coarse, level + 1), interps[level], blocks, counts[level], counts[level + 1]
        )
        iterate = iterate + correction
        resid = resid - operate(correction, level)
        return iterate + resid / (center * diags[level])

    load = assemble(forcing, 8, True)
    first = vcycle(load, 0)
    image_first = operate(first, 0)
    second = vcycle(load - image_first, 0)
    combined = first + second
    image = operate(combined, 0)
    weight = mults[0]
    load_sq, load_image, image_sq = lax.psum(
        (
            jnp.sum(weight * load * load),
            jnp.sum(weight * load * image),
            jnp.sum(weight * image * image),
        ),
        ("gx", "gy"),
    )
    coef = load_image / image_sq
    solution = coef * combined
    residual = load - coef * image
    rel_residual = jnp.sqrt((load_sq - load_image * load_image / image_sq) / load_sq)
    return (solution, residual, rel_residual)


THETA = 1.65
DELTA = 1.35
RATIO = THETA / DELTA
RHO0 = 1.0 / RATIO
RHO1 = 1.0 / (2.0 * RATIO - RHO0)
KEEP = RHO1 * RHO0
PUSH = 2.0 * RHO1 / DELTA
LANES = 128
SUBS = 8


def triple(first, second, third):
    return np.kron(first, np.kron(second, third))


def split_const(matrix):
    high = matrix.astype(jnp.bfloat16)
    low = (matrix - high.astype(np.float64)).astype(jnp.bfloat16)
    return high, low


def stacked(matrix):
    high, low = split_const(matrix)
    return np.concatenate([high, high, low], axis=1)


J_ORDER = (0, 1, 2, 3, 7, 5, 6, 4)
PAIRS = ((0, 7), (1, 2), (3, 4), (5, 6))
FACE = (0, 1, 3, 2)
ROWS1 = tuple(
    (k * 4 + FACE[2 * ih + il]) * 4 + FACE[2 * jh + jl]
    for k in range(4) for ih in range(2) for jh in range(2) for il in range(2) for jl in range(2)
)
ROWS2 = tuple((k * 2 + i) * 2 + j for j in range(2) for k in range(2) for i in range(2))


def padded(matrix, rows, columns):
    return np.pad(matrix, ((0, rows - matrix.shape[0]), (0, columns - matrix.shape[1])))


class Tables:
    def __init__(self):
        tables = [lobatto(count) for count in (8, 4, 2)]
        self.weights = [table[1] for table in tables]
        stiff = [table[2].T @ np.diag(table[1]) @ table[2] for table in tables]
        self.squares = [np.sum(t[2] * t[2] * t[1][:, None], axis=0) for t in tables]
        interps = [lagrange(tables[level][0], tables[level + 1][0]) for level in range(2)]
        factor = [np.where((np.arange(n) == 0) | (np.arange(n) == n - 1), 0.5, 1.0) for n in (8, 4)]
        down = [interps[level].T * factor[level][None, :] for level in range(2)]
        flat = [i for pair in PAIRS for i in pair]
        rows0 = [(k * 8 + i) * 8 + j for k in range(8) for i in range(8) for j in J_ORDER]
        data0 = [(k * 8 + i) * 8 + j for k in range(8) for i in flat for j in J_ORDER]
        rows1, rows2 = list(ROWS1), list(ROWS2)
        w, k = np.diag(self.weights[0]), stiff[0]
        plane = np.kron(k, w) + np.kron(w, k)
        both = np.kron(w, w)
        flip = k[:4, ::-1][:, :4]
        half = np.kron(0.5 * w[:4, :4], plane)
        even = np.kron(0.5 * (k[:4, :4] + flip), both) + half
        odd = np.kron(0.5 * (k[:4, :4] - flip), both) + half
        self.even = stacked(even[np.ix_(rows0[:256], data0[:256])])
        self.odd = stacked(odd[np.ix_(rows0[:256], data0[:256])])
        high, low = split_const(triple(down[0], down[0], down[0])[np.ix_(rows1, data0)])
        self.down0 = np.concatenate([high, low], axis=0)
        up = triple(interps[0], interps[0], interps[0])
        stiffness = np.kron(k, both) + np.kron(w, plane)
        self.up0 = stacked(np.concatenate([up[np.ix_(rows0, rows1)], (stiffness @ up)[np.ix_(rows0, rows1)]]))
        w, k = np.diag(self.weights[1]), stiff[1]
        stiffness = triple(k, w, w) + triple(w, k, w) + triple(w, w, k)
        up = triple(interps[1], interps[1], interps[1])
        self.op1 = stacked(stiffness[np.ix_(rows1, rows1)])
        self.down1 = padded(stacked(triple(down[1], down[1], down[1])[np.ix_(rows2, rows1)]), 16, 192)
        self.up1 = padded(stacked(
            np.concatenate([up[np.ix_(rows1, rows2)], (stiffness @ up)[np.ix_(rows1, rows2)]])), 128, 32)
        w, k = np.diag(self.weights[2]), stiff[2]
        self.op2 = padded(
            stacked((triple(k, w, w) + triple(w, k, w) + triple(w, w, k))[np.ix_(rows2, rows2)]), 16, 32)
        wide = lambda column: np.repeat(np.asarray(column, np.float32)[:, None], LANES, axis=1)
        blocks = [wide(self.weights[0][list(J_ORDER)]), wide(self.squares[0][list(J_ORDER)]),
                  wide(factor[0][list(J_ORDER)])]
        for level, order in ((1, rows1), (2, rows2)):
            a, b = self.weights[level], self.squares[level]
            blocks.append(wide(triple(a, a, a)[order]))
            blocks.append(wide((triple(b, a, a) + triple(a, b, a) + triple(a, a, b))[order]))
        self.rows = np.concatenate(blocks, axis=0)


def swap_rows(x, sub):
    return jnp.where(sub == 4, pltpu.roll(x, 5, 0), jnp.where(sub == 7, pltpu.roll(x, 3, 0), x))


def kernel(nx, ny, tables, near, far, even, odd, down0, up0, op1, down1, up1, op2, rows,
           sol_ref, res_ref, rel_ref, b_ref, r_ref, d_ref, v_ref, p_ref, t_ref, a_ref, z_ref,
           be_ref, bo_ref, c_ref, lane_ref):
    groups = nx // SUBS
    tiles = ny * groups
    part_wide = ny * LANES
    wide = tiles * LANES
    own_x, own_y = lax.axis_index("gx"), lax.axis_index("gy")
    sub = lax.broadcasted_iota(jnp.int32, (SUBS, LANES), 0)
    lanes = lax.broadcasted_iota(jnp.int32, (SUBS, LANES), 1)
    lane = lanes % SUBS
    w = [float(x) for x in tables.weights[0]]
    q = [float(x) for x in tables.squares[0]]
    f = [0.5 if k in (0, 7) else 1.0 for k in range(8)]
    parts = range(groups)

    def cut(x):
        return [x[:, t * LANES:(t + 1) * LANES] for t in range(x.shape[1] // LANES)]

    def join(pieces):
        return jnp.concatenate(pieces, axis=1)

    def ls(p):
        return slice(p * part_wide, (p + 1) * part_wide)

    def split_parts(x):
        return [x[:, ls(p)] for p in parts]

    def across(x, count):
        return join([x] * count)

    sub_w = across(sub, tiles)
    sub_p = across(sub, ny)

    def move(x, amount):
        amount %= LANES
        return join([pltpu.roll(t, amount, 1) for t in cut(x)]) if amount else x

    def x_up(x, p, more=0):
        if p:
            return move(x[p - 1], more)
        prev = cut(x[groups - 1])
        return join([jnp.where(lane == 0, pltpu.roll(t, (LANES - SUBS + 1 + more) % LANES, 1),
                               pltpu.roll(t, 1 + more, 1)) for t in prev])

    def x_down(x, p, more=0):
        if p < groups - 1:
            return move(x[p + 1], more)
        succ = cut(x[0])
        return join([jnp.where(lane == SUBS - 1, pltpu.roll(t, SUBS - 1 + more, 1),
                               pltpu.roll(t, (LANES - 1 + more) % LANES, 1)) for t in succ])

    up, down = SUBS, LANES - SUBS

    def y_fold(x, face):
        t = cut(x)
        other = join([t[(n // ny) * ny + (n + 1) % ny] for n in range(len(t))])
        return x + jnp.where(face, pltpu.roll(other, 4, 0), 0.0)

    face0 = sub_p % 4 == 0
    face1 = sub_w % 2 == 0

    def row(k, i):
        return pl.ds(k * 64 + i * 8, 8)

    for t in range(tiles):
        part, y_index = t // ny, t % ny
        at = slice(t * LANES, (t + 1) * LANES)
        use_near = ((part ^ own_x) & 1) == 0
        slots = []
        for c in range(SUBS):
            delta = (c * groups + part) ^ own_x
            slot, bit = jnp.int32(0), 0
            if ny > 1:
                slot, bit = y_index ^ own_y, 1
            step = nx // 2
            while step > 1:
                flag = jnp.where((delta & step) != 0, 1, 0)
                slot = slot + flag * (1 << bit)
                bit += 1
                step //= 2
            slots.append(slot)
        blocks = [[jnp.where(use_near, near[slot, i], far[slot, i]) for slot in slots]
                  for i in range(8)]
        for step in (1, 2, 4):
            keep = (lane & step) == 0
            low = [c for c in range(SUBS) if not c & step]
            turned = [[jnp.take_along_axis(jnp.where(keep, b[c + step], b[c]), lanes ^ step, axis=1)
                       for c in low] for b in blocks]
            fresh = []
            for b, turn in zip(blocks, turned):
                out = list(b)
                for c, x in zip(low, turn):
                    out[c] = jnp.where(keep, b[c], x)
                    out[c + step] = jnp.where(keep, x, b[c + step])
                fresh.append(out)
            blocks = fresh
        for i, b in enumerate(blocks):
            for k in range(7):
                v_ref[row(k, i), at] = b[k]
            v_ref[row(7, i), at] = pltpu.roll(b[0], down, 1)
        lane_ref[0:8, at] = blocks[0][7]
    kap1 = lane_ref[0:1, :]
    sig1 = lane_ref[1:2, :]
    w_j = across(rows[0:8, :], ny)
    q_j = across(rows[8:16, :], ny)
    f_j = across(rows[16:24, :], tiles)
    kap = [jnp.broadcast_to(kap1[:, ls(p)], (SUBS, part_wide)) for p in parts]
    sig_w = [jnp.broadcast_to(sig1[:, ls(p)], (SUBS, part_wide)) * w_j for p in parts]

    def split(value):
        high = value.astype(jnp.bfloat16)
        return high, (value - high.astype(jnp.float32)).astype(jnp.bfloat16)

    def store_split(kk, index, p, low_pair, high_pair):
        a = jnp.concatenate(low_pair, axis=0)
        b = jnp.concatenate(high_pair, axis=0)
        for ref, value in ((be_ref, a + b), (bo_ref, a - b)):
            high, low = split(value)
            at = kk * 64 + index * 16
            ref[at:at + 16, ls(p)] = high
            ref[256 + at:272 + at, ls(p)] = low
            ref[512 + at:528 + at, ls(p)] = high

    def fold_z(kk, pair):
        a, b = pair
        return (a + move(b, up), b + move(a, down)) if kk == 0 else (a, b)

    def inner(p, kk, index, get, with_z=True):
        out = []
        for i in PAIRS[index]:
            pair = get(p, kk, i)
            pair = fold_z(kk, pair) if with_z else pair
            out.append([y_fold(x, face0) for x in pair])
        return out

    def faces(kk, get, with_z=True):
        first, last = [], []
        for p in parts:
            a, b = get(p, kk, 0), get(p, kk, 7)
            first.append(fold_z(kk, a) if with_z else a)
            last.append(fold_z(kk, b) if with_z else b)
        out = []
        for p in parts:
            a, b = [], []
            for s in range(2):
                firsts, lasts = [x[s] for x in first], [x[s] for x in last]
                a.append(y_fold(firsts[p] + x_up(lasts, p), face0))
                b.append(y_fold(lasts[p] + x_down(firsts, p), face0))
            out.append([a, b])
        return out

    def walk(get, handle, after, with_z=True):
        for p in parts:
            for kk in range(4):
                for index in (1, 2, 3):
                    handle(p, kk, index, inner(p, kk, index, get, with_z))
            if p == 0:
                for kk in range(4):
                    for n, values in enumerate(faces(kk, get, with_z)):
                        handle(n, kk, 0, values)
            after(p)

    def dot(a, b):
        return jnp.dot(a, b, preferred_element_type=jnp.float32)

    def multiply(p):
        a_ref[0:256, ls(p)] = dot(even[...], be_ref[:, ls(p)])
        a_ref[256:512, ls(p)] = dot(odd[...], bo_ref[:, ls(p)])

    def point(p, kk, i):
        out = []
        for k in (kk, 7 - kk):
            s1 = q[k] * w[i] + w[k] * q[i]
            s2 = w[k] * w[i]
            out.append(kap[p] * (s1 * w_j + s2 * q_j) + s2 * sig_w[p])
        return out

    def put_diag(p, kk, index, values):
        for s, k in enumerate((kk, 7 - kk)):
            for n, i in enumerate(PAIRS[index]):
                inverse = 1.0 / values[n][s]
                p_ref[row(k, i), ls(p)] = inverse * PUSH
                t_ref[row(k, i), ls(p)] = inverse * (1.0 / THETA)

    def put_load(p, kk, index, values):
        dirs = []
        for s, k in enumerate((kk, 7 - kk)):
            group = []
            for n, i in enumerate(PAIRS[index]):
                at = (row(k, i), ls(p))
                b_ref[at] = values[n][s]
                r_ref[at] = values[n][s]
                group.append(values[n][s] * t_ref[at])
                d_ref[at] = group[-1]
            dirs.append(group)
        store_split(kk, index, p, dirs[0], dirs[1])

    walk(point, put_diag, lambda p: None)
    walk(lambda p, kk, i: (v_ref[row(kk, i), ls(p)], v_ref[row(7 - kk, i), ls(p)]),
         put_load, multiply, with_z=False)

    low_face = (sub_w // 2) % 2 == 0

    def x_up_all(x, more=0):
        return join([x_up(split_parts(x), p, more) for p in parts])

    def x_down_all(x, more=0):
        return join([x_down(split_parts(x), p, more) for p in parts])

    def fold1(x):
        c = [(x[16 * k:16 * k + 8], x[16 * k + 8:16 * k + 16]) for k in range(4)]
        out = []
        for k, (a, b) in enumerate(c):
            na, nb = x_up_all(b), x_down_all(a)
            if k in (0, 3):
                g, h = c[3 - k]
                amount = up if k == 0 else down
                na = na + x_up_all(h, amount)
                nb = nb + x_down_all(g, amount)
                a, b = a + move(g, amount), b + move(h, amount)
            out.append(y_fold(a + jnp.where(low_face, na, 0.0), face1))
            out.append(y_fold(b + jnp.where(low_face, nb, 0.0), face1))
        return jnp.concatenate(out, axis=0)

    first_k = (sub_w // 2) % 2 == 0
    first_i = sub_w % 2 == 0

    def fold2(x):
        other_k = jnp.where(first_k, pltpu.roll(x, 6, 0), pltpu.roll(x, 2, 0))
        other_i = jnp.where(first_i, pltpu.roll(x, 7, 0), pltpu.roll(x, 1, 0))
        both = jnp.where(first_i, pltpu.roll(other_k, 7, 0), pltpu.roll(other_k, 1, 0))
        x = x + jnp.where(first_k, move(other_k, up), move(other_k, down))
        x = x + jnp.where(first_i, x_up_all(other_i), x_down_all(other_i))
        x = x + jnp.where(first_k, jnp.where(first_i, x_up_all(both, up), x_down_all(both, up)),
                          jnp.where(first_i, x_up_all(both, down), x_down_all(both, down)))
        return y_fold(x, sub_w >= 0)

    def cat3(x):
        high, low = split(x)
        return jnp.concatenate([high, low, high], axis=0)

    def cat3_small(x):
        high = x.astype(jnp.bfloat16).astype(jnp.float32)
        return jnp.concatenate([high, x - high, high, jnp.zeros_like(x)], axis=0).astype(jnp.bfloat16)

    mass1 = across(rows[24:88, :], tiles)
    point1 = across(rows[88:152, :], tiles)
    mass2 = across(rows[152:160, :], tiles)
    point2 = across(rows[160:168, :], tiles)
    inv1_ref, mass1_ref = lane_ref.at[8:72, :], lane_ref.at[72:136, :]
    inv1_ref[...] = 1.0 / fold1(kap1 * point1 + sig1 * mass1)
    mass1_ref[...] = sig1 * mass1
    lane_ref[136:144, :] = 1.0 / fold2(kap1 * point2 + sig1 * mass2)
    lane_ref[144:152, :] = sig1 * mass2

    def apply1(v):
        return fold1(kap1 * dot(op1[...], cat3(v)) + mass1_ref[...] * v)

    def apply2(v):
        return fold2(kap1 * dot(op2[...], cat3_small(v))[0:8] + lane_ref[144:152, :] * v)

    def coarse(resid):
        inverse = inv1_ref[...]
        d = resid * inverse * (1.0 / THETA)
        x = d
        resid = resid - apply1(d)
        d = KEEP * d + PUSH * (resid * inverse)
        x = x + d
        resid = resid - apply1(d)
        low = fold2(dot(down1[...], cat3(resid))[0:8])
        inverse2 = lane_ref[136:144, :]
        d = low * inverse2 * (1.0 / THETA)
        y = d
        low = low - apply2(d)
        y = y + KEEP * d + PUSH * (low * inverse2)
        both = dot(up1[...], cat3_small(y))
        e = both[0:64]
        x = x + e
        resid = resid - fold1(kap1 * both[64:128] + mass1_ref[...] * e)
        return x + resid * inverse * (1.0 / THETA)

    def weighted(p, kk, i, a, b):
        scale = sig_w[p] * (w[kk] * w[i])
        return (kap[p] * a + scale * d_ref[row(kk, i), ls(p)],
                kap[p] * b + scale * d_ref[row(7 - kk, i), ls(p)])

    def from_halves(p, kk, i):
        e = a_ref[row(kk, i), ls(p)]
        o = a_ref[row(4 + kk, i), ls(p)]
        return weighted(p, kk, i, e + o, e - o)

    def from_whole(p, kk, i):
        return weighted(p, kk, i, a_ref[row(kk, i), ls(p)], a_ref[row(7 - kk, i), ls(p)])

    def lower(at, value):
        r = r_ref[at] - value
        r_ref[at] = r
        return r

    def second_direction(at, value):
        return KEEP * d_ref[at] + lower(at, value) * p_ref[at]

    def next_direction(at, value):
        return lower(at, value) * t_ref[at]

    def put(update):
        def handle(p, kk, index, values):
            dirs = []
            for s, k in enumerate((kk, 7 - kk)):
                group = []
                for n, i in enumerate(PAIRS[index]):
                    at = (row(k, i), ls(p))
                    group.append(update(at, values[n][s]))
                    d_ref[at] = group[-1]
                dirs.append(group)
            store_split(kk, index, p, dirs[0], dirs[1])
        return handle

    def put_resid(p, kk, index, values):
        for s, k in enumerate((kk, 7 - kk)):
            pair = [lower((row(k, i), ls(p)), values[n][s]) for n, i in enumerate(PAIRS[index])]
            high, low = split(jnp.concatenate(pair, axis=0))
            at = k * 64 + index * 16
            c_ref[at:at + 16, ls(p)] = high
            c_ref[512 + at:528 + at, ls(p)] = low

    def put_last(p, kk, index, values):
        for s, k in enumerate((kk, 7 - kk)):
            for n, i in enumerate(PAIRS[index]):
                lower((row(k, i), ls(p)), values[n][s])

    window = pl.ds(pl.multiple_of((own_x % groups * ny + own_y) * LANES, LANES), LANES)
    z_ref[...] = jnp.zeros((512, LANES), jnp.float32)

    def collect():
        z_ref[...] = z_ref[...] + d_ref[:, window]

    for step in range(2):
        collect()
        walk(from_halves, put(second_direction), multiply)
        collect()
        low = {}

        def reduce(p):
            both = dot(down0[...], c_ref[0:512, ls(p)])
            low[p] = both[0:64] + both[64:128] + dot(down0[0:64, :], c_ref[512:1024, ls(p)])

        walk(from_halves, put_resid, reduce)
        correction = cat3(coarse(fold1(join([low[p] for p in parts]))))
        for p in parts:
            d_ref[:, ls(p)] = dot(up0[0:512, :], correction[:, ls(p)])
            a_ref[:, ls(p)] = dot(up0[512:1024, :], correction[:, ls(p)])
        collect()
        walk(from_whole, put(next_direction), multiply)
        collect()
        if step == 0:
            walk(from_halves, put(next_direction), multiply)
        else:
            walk(from_halves, put_last, lambda p: None)

    zero = jnp.zeros((SUBS, wide), jnp.float32)
    bw, ww, bb = zero, zero, zero
    for k in range(8):
        for i in range(8):
            b = b_ref[row(k, i), :]
            image_all = b - r_ref[row(k, i), :]
            fb = b * (f[k] * f[i])
            bw = bw + fb * image_all
            ww = ww + image_all * image_all * (f[k] * f[i])
            bb = bb + fb * b
    bw, ww, bb = jnp.sum(bw * f_j), jnp.sum(ww * f_j), jnp.sum(bb * f_j)
    coef = bw / ww
    rr = zero
    for k in range(8):
        for i in range(8):
            b = b_ref[row(k, i), :]
            res = b - coef * (b - r_ref[row(k, i), :])
            rr = rr + res * res * (f[k] * f[i])
    rr = jnp.sum(rr * f_j)
    rel_ref[0] = jnp.sqrt(rr / bb)
    place = own_x // groups
    for i in range(8):
        sol = jnp.zeros((SUBS, LANES), jnp.float32)
        res = sol
        for k in range(8):
            b = b_ref[row(k, i), window]
            r = b - coef * (b - r_ref[row(k, i), window])
            turn = (k - place) % LANES
            sol = jnp.where(lane == k, pltpu.roll(z_ref[row(k, i), :], turn, 1), sol)
            res = jnp.where(lane == k, pltpu.roll(r, turn, 1), res)
        sol_ref[i] = swap_rows(coef * sol, sub)
        res_ref[i] = swap_rows(res, sub)


def solve_all(nx, ny, near, far):
    tables = Tables()
    wide = ny * nx // SUBS * LANES
    consts = [tables.even, tables.odd, tables.down0, tables.up0, tables.op1, tables.down1,
              tables.up1, tables.op2, tables.rows]
    vmem = pl.BlockSpec(memory_space=pltpu.VMEM)
    field = pltpu.VMEM((512, wide), jnp.float32)
    return pl.pallas_call(
        lambda *refs: kernel(nx, ny, tables, *refs),
        in_specs=[vmem] * 11,
        out_specs=[vmem, vmem, pl.BlockSpec(memory_space=pltpu.SMEM)],
        out_shape=[
            jax.ShapeDtypeStruct(near.shape[1:], jnp.float32),
            jax.ShapeDtypeStruct(near.shape[1:], jnp.float32),
            jax.ShapeDtypeStruct((1,), jnp.float32),
        ],
        scratch_shapes=[
            field, field, field, field, field, field, field,
            pltpu.VMEM((512, LANES), jnp.float32),
            pltpu.VMEM((768, wide), jnp.bfloat16), pltpu.VMEM((768, wide), jnp.bfloat16),
            pltpu.VMEM((1024, wide), jnp.bfloat16), pltpu.VMEM((152, wide), jnp.float32),
        ],
        name="solve_all",
    )(*[pltpu.with_memory_space_constraint(x, pltpu.VMEM)
             for x in (near, far, *[jnp.asarray(c) for c in consts])])


def pack_kernel(forcing, kappa, sigma, out_ref, coef_ref):
    sub = lax.broadcasted_iota(jnp.int32, (SUBS, LANES), 0)
    lane = lax.broadcasted_iota(jnp.int32, (SUBS, LANES), 1)
    count = kappa.shape[2]
    coef_ref[...] = jnp.zeros((SUBS, LANES), jnp.float32)
    coef_ref[0:1, 0:count] = kappa[0]
    coef_ref[1:2, 0:count] = sigma[0]
    spread = jnp.take_along_axis(coef_ref[...], lane // SUBS, axis=1)
    for i in range(SUBS):
        x = swap_rows(forcing[i], sub)
        x = x + jnp.where(lane % SUBS == 0, pltpu.roll(x, 1, 1), 0.0)
        if i == 0:
            x = jnp.where(lane % SUBS == SUBS - 1, spread, x)
        out_ref[0, i] = x


def packed_block(forcing, kappa, sigma):
    vmem = pl.BlockSpec(memory_space=pltpu.VMEM)
    return pl.pallas_call(
        pack_kernel,
        in_specs=[vmem] * 3,
        out_specs=vmem,
        out_shape=pltpu.VMEM((1, *forcing.shape), jnp.float32),
        scratch_shapes=[pltpu.VMEM((SUBS, LANES), jnp.float32)],
        name="pack_block",
    )(forcing, kappa, sigma)


def gathered(forcing, kappa, sigma):
    nx, ny = lax.axis_size("gx"), lax.axis_size("gy")
    block = packed_block(forcing, kappa, sigma)
    if ny > 1:
        other = lax.ppermute(block, "gy", [(i, i ^ 1) for i in range(ny)])
        block = jnp.concatenate([block, other], axis=0)
    step = nx // 2
    while step:
        other = lax.ppermute(block, "gx", [(i, i ^ step) for i in range(nx)])
        if step > 1:
            block = jnp.concatenate([block, other], axis=0)
        step //= 2
    sol, res, rel = solve_all(nx, ny, block, other)
    return sol, res, rel.reshape(())


def fits_one_device(mesh):
    nx, ny = mesh.shape["gx"], mesh.shape["gy"]
    power = nx & (nx - 1) == 0
    return power and nx % SUBS == 0 and ny <= 2 and nx * ny <= 64


def solution(mesh):
    spec = P("gx", "gy", None)
    small = fits_one_device(mesh)

    def local(forcing, kappa, sigma):
        plain = forcing.shape == (SUBS, SUBS, LANES) and kappa.shape == (1, 1, LANES // SUBS)
        return (gathered if small and plain else distributed)(forcing, kappa, sigma)

    return jax.shard_map(
        local, mesh=mesh, in_specs=(spec, spec, spec), out_specs=(spec, spec, P()),
        check_vma=False,
    )
```

```python
import jax
import jax.numpy as jnp
import numpy as np
from jax import lax
from jax.experimental import pallas as pl
from jax.experimental.pallas import tpu as pltpu
from jax.sharding import PartitionSpec as P


def with_halo(cells, sides, width):
    for axis, dim in sides:
        count = lax.axis_size(axis)
        head = lax.slice_in_dim(cells, 0, width, axis=dim)
        tail = lax.slice_in_dim(cells, cells.shape[dim] - width, cells.shape[dim], axis=dim)
        cells = jnp.concatenate(
            [
                lax.ppermute(tail, axis, [(i, (i + 1) % count) for i in range(count)]),
                cells,
                lax.ppermute(head, axis, [((i + 1) % count, i) for i in range(count)]),
            ],
            axis=dim,
        )
    return cells


def legendre_table(points, order):
    columns = [points * 0.0 + 1.0, points]
    for degree in range(2, order + 1):
        columns.append(
            ((2 * degree - 1) * points * columns[-1] - (degree - 1) * columns[-2]) / degree
        )
    return np.stack(columns, axis=1)


def lobatto(count):
    order = count - 1
    points = np.cos(np.pi * np.arange(count) / order)
    for sweep in range(60):
        table = legendre_table(points, order)
        points = points - (points * table[:, order] - table[:, order - 1]) / (
            count * table[:, order]
        )
    table = legendre_table(points, order)
    weights = 2.0 / (order * count * table[:, order] ** 2)
    values = table[:, order]
    points, weights, values = (points[::-1], weights[::-1], values[::-1])
    spread = points[:, None] - points[None, :] + np.eye(count)
    deriv = values[:, None] / values[None, :] / spread * (1.0 - np.eye(count))
    corner = order * (order + 1) / 4.0
    ends = np.array([-corner] + [0.0] * (count - 2) + [corner])
    return (points, weights, deriv + np.eye(count) * ends[None, :])


def lagrange(fine_points, coarse_points):
    columns = []
    for column in range(len(coarse_points)):
        value = fine_points * 0.0 + 1.0
        for other in range(len(coarse_points)):
            if other != column:
                value = (
                    value
                    * (fine_points - coarse_points[other])
                    / (coarse_points[column] - coarse_points[other])
                )
        columns.append(value)
    return np.stack(columns, axis=1)


def edge_factor(count, blocks):
    index = jnp.arange(count)
    single = jnp.where((index == 0) | (index == count - 1), 0.5, 1.0).astype(jnp.float32)
    return jnp.tile(single, blocks)


def multiplicity(count, blocks):
    first = edge_factor(count, blocks[0])
    second = edge_factor(count, blocks[1])
    third = edge_factor(count, blocks[2])
    return first[:, None, None] * second[None, :, None] * third[None, None, :]


def element_apply(field, kappa, sigma, deriv, weights):
    count = deriv.shape[0]
    ex, ey, ez = kappa.shape
    high = lax.Precision.HIGHEST
    block = field.reshape(ex, count, ey, count, ez, count)
    mass = (weights[:, None, None] * weights[None, :, None] * weights[None, None, :])[
        None, :, None, :, None, :
    ]
    first = jnp.einsum("ai,eifjgk->eafjgk", deriv, block, precision=high)
    total = jnp.einsum("ai,eafjgk->eifjgk", deriv, first * mass, precision=high)
    second = jnp.einsum("aj,eifjgk->eifagk", deriv, block, precision=high)
    total = total + jnp.einsum("aj,eifagk->eifjgk", deriv, second * mass, precision=high)
    third = jnp.einsum("ak,eifjgk->eifjga", deriv, block, precision=high)
    total = total + jnp.einsum("ak,eifjga->eifjgk", deriv, third * mass, precision=high)
    coeff = kappa[:, None, :, None, :, None]
    shift = sigma[:, None, :, None, :, None]
    return (coeff * total + shift * mass * block).reshape(field.shape)


def element_diagonal(kappa, sigma, deriv, weights):
    count = deriv.shape[0]
    ex, ey, ez = kappa.shape
    stiff = jnp.sum(deriv * deriv * weights[:, None], axis=0)
    term = stiff[:, None, None] * weights[None, :, None] * weights[None, None, :]
    term = term + weights[:, None, None] * stiff[None, :, None] * weights[None, None, :]
    term = term + weights[:, None, None] * weights[None, :, None] * stiff[None, None, :]
    mass = weights[:, None, None] * weights[None, :, None] * weights[None, None, :]
    coeff = kappa[:, None, :, None, :, None]
    shift = sigma[:, None, :, None, :, None]
    full = coeff * term[None, :, None, :, None, :] + shift * mass[None, :, None, :, None, :]
    return full.reshape(ex * count, ey * count, ez * count)


def fold_axis(field, dim, count):
    size = field.shape[dim]
    position = jnp.arange(size) % count
    shape = [1, 1, 1]
    shape[dim] = size
    first = (position == 0).reshape(shape)
    last = (position == count - 1).reshape(shape)
    before = jnp.roll(field, 1, dim)
    after = jnp.roll(field, -1, dim)
    return field + jnp.where(first, before, 0.0) + jnp.where(last, after, 0.0)


def fold_padded(padded, dim, count):
    size = padded.shape[dim] - 2
    center = lax.slice_in_dim(padded, 1, size + 1, axis=dim)
    before = lax.slice_in_dim(padded, 0, size, axis=dim)
    after = lax.slice_in_dim(padded, 2, size + 2, axis=dim)
    position = jnp.arange(size) % count
    shape = [1, 1, 1]
    shape[dim] = size
    first = (position == 0).reshape(shape)
    last = (position == count - 1).reshape(shape)
    return center + jnp.where(first, before, 0.0) + jnp.where(last, after, 0.0)


def assemble(field, count, finest):
    if finest:
        padded = with_halo(field, (("gx", 0), ("gy", 1)), 1)
        field = fold_padded(fold_padded(padded, 0, count), 1, count)
    else:
        padded = with_halo(field, (("gx", 0), ("gy", 1)), 1)
        field = fold_padded(fold_padded(padded, 0, count), 1, count)
    return fold_axis(field, 2, count)


def restrict(field, interp, blocks, fine_count, coarse_count):
    high = lax.Precision.HIGHEST
    block = field.reshape(blocks[0], fine_count, blocks[1], fine_count, blocks[2], fine_count)
    one = jnp.einsum("ia,eifjgk->eafjgk", interp, block, precision=high)
    two = jnp.einsum("jb,eafjgk->eafbgk", interp, one, precision=high)
    three = jnp.einsum("kc,eafbgk->eafbgc", interp, two, precision=high)
    return three.reshape(
        blocks[0] * coarse_count, blocks[1] * coarse_count, blocks[2] * coarse_count
    )


def prolong(field, interp, blocks, fine_count, coarse_count):
    high = lax.Precision.HIGHEST
    block = field.reshape(blocks[0], coarse_count, blocks[1], coarse_count, blocks[2], coarse_count)
    one = jnp.einsum("ia,eafbgc->eifbgc", interp, block, precision=high)
    two = jnp.einsum("jb,eifbgc->eifjgc", interp, one, precision=high)
    three = jnp.einsum("kc,eifjgc->eifjgk", interp, two, precision=high)
    return three.reshape(blocks[0] * fine_count, blocks[1] * fine_count, blocks[2] * fine_count)


def distributed(forcing, kappa, sigma):
    blocks = kappa.shape
    counts = [8, 4, 2]
    tables = [lobatto(count) for count in counts]
    derivs = [jnp.asarray(table[2], jnp.float32) for table in tables]
    weights = [jnp.asarray(table[1], jnp.float32) for table in tables]
    interps = [
        jnp.asarray(lagrange(tables[level][0], tables[level + 1][0]), jnp.float32)
        for level in range(2)
    ]
    mults = [multiplicity(count, blocks) for count in counts]
    diags = [
        assemble(
            element_diagonal(kappa, sigma, derivs[level], weights[level]), counts[level], level == 0
        )
        for level in range(3)
    ]
    center = 1.65
    half = 1.35
    ratio = center / half

    def operate(field, level):
        return assemble(
            element_apply(field, kappa, sigma, derivs[level], weights[level]),
            counts[level],
            level == 0,
        )

    def smooth(resid, level, steps, keep_last):
        rho = 1.0 / ratio
        direction = resid / (center * diags[level])
        iterate = direction
        for step in range(steps):
            if step > 0:
                rho_next = 1.0 / (2.0 * ratio - rho)
                direction = (
                    rho_next * rho * direction + 2.0 * rho_next / half * resid / diags[level]
                )
                iterate = iterate + direction
                rho = rho_next
            if step < steps - 1 or keep_last:
                resid = resid - operate(direction, level)
        return (iterate, resid)

    def vcycle(resid, level):
        if level == 2:
            iterate, unused = smooth(resid, level, 2, False)
            return iterate
        iterate, resid = smooth(resid, level, 2, True)
        coarse = assemble(
            restrict(
                mults[level] * resid, interps[level], blocks, counts[level], counts[level + 1]
            ),
            counts[level + 1],
            False,
        )
        correction = prolong(
            vcycle(coarse, level + 1), interps[level], blocks, counts[level], counts[level + 1]
        )
        iterate = iterate + correction
        resid = resid - operate(correction, level)
        return iterate + resid / (center * diags[level])

    load = assemble(forcing, 8, True)
    first = vcycle(load, 0)
    image_first = operate(first, 0)
    second = vcycle(load - image_first, 0)
    combined = first + second
    image = operate(combined, 0)
    weight = mults[0]
    load_sq, load_image, image_sq = lax.psum(
        (
            jnp.sum(weight * load * load),
            jnp.sum(weight * load * image),
            jnp.sum(weight * image * image),
        ),
        ("gx", "gy"),
    )
    coef = load_image / image_sq
    solution = coef * combined
    residual = load - coef * image
    rel_residual = jnp.sqrt((load_sq - load_image * load_image / image_sq) / load_sq)
    return (solution, residual, rel_residual)


THETA = 1.65
DELTA = 1.35
RATIO = THETA / DELTA
RHO0 = 1.0 / RATIO
RHO1 = 1.0 / (2.0 * RATIO - RHO0)
KEEP = RHO1 * RHO0
PUSH = 2.0 * RHO1 / DELTA
LANES = 128
SUBS = 8


def triple(first, second, third):
    return np.kron(first, np.kron(second, third))


def split_const(matrix):
    high = matrix.astype(jnp.bfloat16)
    low = (matrix - high.astype(np.float64)).astype(jnp.bfloat16)
    return high, low


def stacked(matrix):
    high, low = split_const(matrix)
    return np.concatenate([high, high, low], axis=1)


J_ORDER = (0, 1, 2, 3, 7, 5, 6, 4)
SPLIT_AT = ((0, 1), (2, 1))
PAIRS = ((0, 7), (1, 2), (3, 4), (5, 6))
FACE = (0, 1, 3, 2)
ROWS1 = tuple(
    (k * 4 + FACE[2 * ih + il]) * 4 + FACE[2 * jh + jl]
    for k in range(4) for ih in range(2) for jh in range(2) for il in range(2) for jl in range(2)
)
ROWS2 = tuple((k * 2 + i) * 2 + j for j in range(2) for k in range(2) for i in range(2))


def padded(matrix, rows, columns):
    return np.pad(matrix, ((0, rows - matrix.shape[0]), (0, columns - matrix.shape[1])))


class Tables:
    def __init__(self):
        tables = [lobatto(count) for count in (8, 4, 2)]
        self.weights = [table[1] for table in tables]
        stiff = [table[2].T @ np.diag(table[1]) @ table[2] for table in tables]
        self.squares = [np.sum(t[2] * t[2] * t[1][:, None], axis=0) for t in tables]
        interps = [lagrange(tables[level][0], tables[level + 1][0]) for level in range(2)]
        factor = [np.where((np.arange(n) == 0) | (np.arange(n) == n - 1), 0.5, 1.0) for n in (8, 4)]
        down = [interps[level].T * factor[level][None, :] for level in range(2)]
        flat = [i for pair in PAIRS for i in pair]
        rows0 = [(k * 8 + i) * 8 + j for k in range(8) for i in range(8) for j in J_ORDER]
        data0 = [(k * 8 + i) * 8 + j for k in range(8) for i in flat for j in J_ORDER]
        rows1, rows2 = list(ROWS1), list(ROWS2)
        w, k = np.diag(self.weights[0]), stiff[0]
        plane = np.kron(k, w) + np.kron(w, k)
        both = np.kron(w, w)
        flip = k[:4, ::-1][:, :4]
        half = np.kron(0.5 * w[:4, :4], plane)
        even = np.kron(0.5 * (k[:4, :4] + flip), both) + half
        odd = np.kron(0.5 * (k[:4, :4] - flip), both) + half
        self.even = stacked(even[np.ix_(rows0[:256], data0[:256])])
        self.odd = stacked(odd[np.ix_(rows0[:256], data0[:256])])
        high, low = split_const(triple(down[0], down[0], down[0])[np.ix_(rows1, data0)])
        self.down0 = np.concatenate([high, low], axis=0)
        up = triple(interps[0], interps[0], interps[0])
        stiffness = np.kron(k, both) + np.kron(w, plane)
        self.up0 = stacked(np.concatenate([up[np.ix_(rows0, rows1)], (stiffness @ up)[np.ix_(rows0, rows1)]]))
        w, k = np.diag(self.weights[1]), stiff[1]
        stiffness = triple(k, w, w) + triple(w, k, w) + triple(w, w, k)
        up = triple(interps[1], interps[1], interps[1])
        self.op1 = stacked(stiffness[np.ix_(rows1, rows1)])
        self.down1 = padded(stacked(triple(down[1], down[1], down[1])[np.ix_(rows2, rows1)]), 16, 192)
        self.up1 = padded(stacked(
            np.concatenate([up[np.ix_(rows1, rows2)], (stiffness @ up)[np.ix_(rows1, rows2)]])), 128, 32)
        w, k = np.diag(self.weights[2]), stiff[2]
        op2 = (triple(k, w, w) + triple(w, k, w) + triple(w, w, k))[np.ix_(rows2, rows2)]
        wide = lambda column: np.repeat(np.asarray(column, np.float32)[:, None], LANES, axis=1)
        blocks = [wide(self.weights[0][list(J_ORDER)]), wide(self.squares[0][list(J_ORDER)]),
                  wide(factor[0][list(J_ORDER)])]
        for level, order in ((1, rows1), (2, rows2)):
            a, b = self.weights[level], self.squares[level]
            blocks.append(wide(triple(a, a, a)[order]))
            blocks.append(wide((triple(b, a, a) + triple(a, b, a) + triple(a, a, b))[order]))
        at = np.arange(SUBS)
        self.op2 = np.concatenate([wide(op2[at, (at - turn) % SUBS]) for turn in range(SUBS)], axis=0)
        self.rows = np.concatenate(blocks, axis=0)


def swap_rows(x, sub):
    return jnp.where(sub == 4, pltpu.roll(x, 5, 0), jnp.where(sub == 7, pltpu.roll(x, 3, 0), x))


def kernel(nx, ny, tables, near, far, even, odd, down0, up0, op1, down1, up1, op2, rows,
           sol_ref, res_ref, rel_ref, b_ref, r_ref, d_ref, other_ref, v_ref, p_ref, t_ref, a_ref, z_ref,
           be_ref, bo_ref, c_ref, lane_ref, low_ref, cor_ref):
    groups = nx // SUBS
    tiles = ny * groups
    part_wide = ny * LANES
    wide = tiles * LANES
    own_x, own_y = lax.axis_index("gx"), lax.axis_index("gy")
    sub = lax.broadcasted_iota(jnp.int32, (SUBS, LANES), 0)
    lanes = lax.broadcasted_iota(jnp.int32, (SUBS, LANES), 1)
    lane = lanes % SUBS
    w = [float(x) for x in tables.weights[0]]
    q = [float(x) for x in tables.squares[0]]
    parts = range(groups)

    def cut(x):
        return [x[:, t * LANES:(t + 1) * LANES] for t in range(x.shape[1] // LANES)]

    def join(pieces):
        return jnp.concatenate(pieces, axis=1)

    def ls(p):
        return slice(p * part_wide, (p + 1) * part_wide)

    def split_parts(x):
        return [x[:, ls(p)] for p in parts]

    def across(x, count):
        return join([x] * count)

    sub_w = across(sub, tiles)
    sub_p = across(sub, ny)

    def move(x, amount):
        amount %= LANES
        return join([pltpu.roll(t, amount, 1) for t in cut(x)]) if amount else x

    def x_up(x, p, more=0):
        if p:
            return move(x[p - 1], more)
        prev = cut(x[groups - 1])
        return join([jnp.where(lane == 0, pltpu.roll(t, (LANES - SUBS + 1 + more) % LANES, 1),
                               pltpu.roll(t, 1 + more, 1)) for t in prev])

    def x_down(x, p, more=0):
        if p < groups - 1:
            return move(x[p + 1], more)
        succ = cut(x[0])
        return join([jnp.where(lane == SUBS - 1, pltpu.roll(t, SUBS - 1 + more, 1),
                               pltpu.roll(t, (LANES - 1 + more) % LANES, 1)) for t in succ])

    up, down = SUBS, LANES - SUBS

    def y_fold(x, face):
        t = cut(x)
        other = join([t[(n // ny) * ny + (n + 1) % ny] for n in range(len(t))])
        return x + jnp.where(face, pltpu.roll(other, 4, 0), 0.0)

    face0 = sub_p % 4 == 0
    face1 = sub_w % 2 == 0

    def row(k, i):
        return pl.ds(k * 64 + i * 8, 8)

    for t in range(tiles):
        part, y_index = t // ny, t % ny
        at = slice(t * LANES, (t + 1) * LANES)
        use_near = ((part ^ own_x) & 1) == 0
        slots = []
        for c in range(SUBS):
            delta = (c * groups + part) ^ own_x
            slot, bit = jnp.int32(0), 0
            if ny > 1:
                slot, bit = y_index ^ own_y, 1
            step = nx // 2
            while step > 1:
                flag = jnp.where((delta & step) != 0, 1, 0)
                slot = slot + flag * (1 << bit)
                bit += 1
                step //= 2
            slots.append(slot)
        blocks = [[jnp.where(use_near, near[slot, i], far[slot, i]) for slot in slots]
                  for i in range(8)]
        for step in (1, 2, 4):
            keep = (lane & step) == 0
            low = [c for c in range(SUBS) if not c & step]
            turned = [[jnp.take_along_axis(jnp.where(keep, b[c + step], b[c]), lanes ^ step, axis=1)
                       for c in low] for b in blocks]
            fresh = []
            for b, turn in zip(blocks, turned):
                out = list(b)
                for c, x in zip(low, turn):
                    out[c] = jnp.where(keep, b[c], x)
                    out[c + step] = jnp.where(keep, x, b[c + step])
                fresh.append(out)
            blocks = fresh
        for i, b in enumerate(blocks):
            for k in range(7):
                v_ref[row(k, i), at] = b[k]
            v_ref[row(7, i), at] = pltpu.roll(b[0], down, 1)
        lane_ref[0:8, at] = blocks[0][7]
    kap1 = lane_ref[0:1, :]
    sig1 = lane_ref[1:2, :]
    w_j = across(rows[0:8, :], ny)
    q_j = across(rows[8:16, :], ny)
    f_j = across(rows[16:24, :], tiles)
    kap = [jnp.broadcast_to(kap1[:, ls(p)], (SUBS, part_wide)) for p in parts]
    sig_w = [jnp.broadcast_to(sig1[:, ls(p)], (SUBS, part_wide)) * w_j for p in parts]

    def split(value):
        high = value.astype(jnp.bfloat16)
        return high, (value - high.astype(jnp.float32)).astype(jnp.bfloat16)

    def store_split(kk, index, p, low_pair, high_pair):
        a = jnp.concatenate(low_pair, axis=0)
        b = jnp.concatenate(high_pair, axis=0)
        for ref, value in ((be_ref, a + b), (bo_ref, a - b)):
            high, low = split(value)
            at = kk * 64 + index * 16
            ref[at:at + 16, ls(p)] = high
            ref[256 + at:272 + at, ls(p)] = low

    def fold_z(kk, pair):
        a, b = pair
        return (a + move(b, up), b + move(a, down)) if kk == 0 else (a, b)

    def inner(p, kk, index, get, with_z=True):
        out = []
        for i in PAIRS[index]:
            pair = get(p, kk, i)
            pair = fold_z(kk, pair) if with_z else pair
            out.append([y_fold(x, face0) for x in pair])
        return out

    def faces(kk, get, with_z=True):
        first, last = [], []
        for p in parts:
            a, b = get(p, kk, 0), get(p, kk, 7)
            first.append(fold_z(kk, a) if with_z else a)
            last.append(fold_z(kk, b) if with_z else b)
        out = []
        for p in parts:
            a, b = [], []
            for s in range(2):
                firsts, lasts = [x[s] for x in first], [x[s] for x in last]
                a.append(y_fold(firsts[p] + x_up(lasts, p), face0))
                b.append(y_fold(lasts[p] + x_down(firsts, p), face0))
            out.append([a, b])
        return out

    pending = []

    def flush():
        while pending:
            pending.pop(0)()

    def walk(get, handle, after, with_z=True):
        for p in parts:
            for kk in range(4):
                for index in (1, 2, 3):
                    if pending and (kk, index) in SPLIT_AT:
                        pending.pop(0)()
                    handle(p, kk, index, inner(p, kk, index, get, with_z))
            flush()
            if p == 0:
                for kk in range(4):
                    for n, values in enumerate(faces(kk, get, with_z)):
                        handle(n, kk, 0, values)
            pending.extend(after(p))

    def dot(a, b):
        return jnp.dot(a, b, preferred_element_type=jnp.float32)

    def rows_of(ref, p):
        return jnp.concatenate([ref[:, ls(p)], ref[0:256, ls(p)]], axis=0)

    def multiply(p):
        def first():
            a_ref[0:256, ls(p)] = dot(even[...], rows_of(be_ref, p))

        def second():
            a_ref[256:512, ls(p)] = dot(odd[...], rows_of(bo_ref, p))

        return first, second

    def point(p, kk, i):
        out = []
        for k in (kk, 7 - kk):
            s1 = q[k] * w[i] + w[k] * q[i]
            s2 = w[k] * w[i]
            out.append(kap[p] * (s1 * w_j + s2 * q_j) + s2 * sig_w[p])
        return out

    def put_diag(p, kk, index, values):
        for s, k in enumerate((kk, 7 - kk)):
            for n, i in enumerate(PAIRS[index]):
                inverse = 1.0 / values[n][s]
                p_ref[row(k, i), ls(p)] = inverse * PUSH
                t_ref[row(k, i), ls(p)] = inverse * (1.0 / THETA)

    def put_load(p, kk, index, values):
        dirs = []
        for s, k in enumerate((kk, 7 - kk)):
            group = []
            for n, i in enumerate(PAIRS[index]):
                at = (row(k, i), ls(p))
                b_ref[at] = values[n][s]
                r_ref[at] = values[n][s]
                group.append(values[n][s] * t_ref[at])
                d_ref[at] = group[-1]
            dirs.append(group)
        store_split(kk, index, p, dirs[0], dirs[1])

    walk(point, put_diag, lambda p: ())
    walk(lambda p, kk, i: (v_ref[row(kk, i), ls(p)], v_ref[row(7 - kk, i), ls(p)]),
         put_load, multiply, with_z=False)

    low_face = (sub_w // 2) % 2 == 0

    def x_up_all(x, more=0):
        return join([x_up(split_parts(x), p, more) for p in parts])

    def x_down_all(x, more=0):
        return join([x_down(split_parts(x), p, more) for p in parts])

    def fold1(x):
        c = [(x[16 * k:16 * k + 8], x[16 * k + 8:16 * k + 16]) for k in range(4)]
        out = []
        for k, (a, b) in enumerate(c):
            na, nb = x_up_all(b), x_down_all(a)
            if k in (0, 3):
                g, h = c[3 - k]
                amount = up if k == 0 else down
                na = na + x_up_all(h, amount)
                nb = nb + x_down_all(g, amount)
                a, b = a + move(g, amount), b + move(h, amount)
            out.append(y_fold(a + jnp.where(low_face, na, 0.0), face1))
            out.append(y_fold(b + jnp.where(low_face, nb, 0.0), face1))
        return jnp.concatenate(out, axis=0)

    first_k = (sub_w // 2) % 2 == 0
    first_i = sub_w % 2 == 0

    def fold2(x):
        other_k = jnp.where(first_k, pltpu.roll(x, 6, 0), pltpu.roll(x, 2, 0))
        other_i = jnp.where(first_i, pltpu.roll(x, 7, 0), pltpu.roll(x, 1, 0))
        both = jnp.where(first_i, pltpu.roll(other_k, 7, 0), pltpu.roll(other_k, 1, 0))
        x = x + jnp.where(first_k, move(other_k, up), move(other_k, down))
        x = x + jnp.where(first_i, x_up_all(other_i), x_down_all(other_i))
        x = x + jnp.where(first_k, jnp.where(first_i, x_up_all(both, up), x_down_all(both, up)),
                          jnp.where(first_i, x_up_all(both, down), x_down_all(both, down)))
        return y_fold(x, sub_w >= 0)

    def cat3(x):
        high, low = split(x)
        return jnp.concatenate([high, low, high], axis=0)

    def cat3_small(x):
        high = x.astype(jnp.bfloat16).astype(jnp.float32)
        return jnp.concatenate([high, x - high, high, jnp.zeros_like(x)], axis=0).astype(jnp.bfloat16)

    mass1 = across(rows[24:88, :], tiles)
    point1 = across(rows[88:152, :], tiles)
    mass2 = across(rows[152:160, :], tiles)
    point2 = across(rows[160:168, :], tiles)
    inv1_ref, mass1_ref = lane_ref.at[8:72, :], lane_ref.at[72:136, :]
    inv1_ref[...] = 1.0 / fold1(kap1 * point1 + sig1 * mass1)
    mass1_ref[...] = sig1 * mass1
    lane_ref[136:144, :] = 1.0 / fold2(kap1 * point2 + sig1 * mass2)
    lane_ref[144:152, :] = sig1 * mass2

    def apply1(v):
        return fold1(kap1 * dot(op1[...], cat3(v)) + mass1_ref[...] * v)

    def apply2(v):
        terms = [across(op2[8 * n:8 * n + 8, :], tiles) * (pltpu.roll(v, n, 0) if n else v)
                 for n in range(SUBS)]
        while len(terms) > 1:
            terms = [x + y for x, y in zip(terms[::2], terms[1::2])]
        return fold2(kap1 * terms[0] + lane_ref[144:152, :] * v)

    def coarse(resid):
        inverse = inv1_ref[...]
        d = resid * inverse * (1.0 / THETA)
        x = d
        resid = resid - apply1(d)
        d = KEEP * d + PUSH * (resid * inverse)
        x = x + d
        resid = resid - apply1(d)
        low = fold2(dot(down1[...], cat3(resid))[0:8])
        inverse2 = lane_ref[136:144, :]
        d = low * inverse2 * (1.0 / THETA)
        y = d
        low = low - apply2(d)
        y = y + KEEP * d + PUSH * (low * inverse2)
        both = dot(up1[...], cat3_small(y))
        e = both[0:64]
        x = x + e
        resid = resid - fold1(kap1 * both[64:128] + mass1_ref[...] * e)
        return x + resid * inverse * (1.0 / THETA)

    d_refs = [d_ref, other_ref]

    def turn_over():
        d_refs.reverse()

    def weighted(p, kk, i, a, b):
        scale = sig_w[p] * (w[kk] * w[i])
        return (kap[p] * a + scale * d_refs[0][row(kk, i), ls(p)],
                kap[p] * b + scale * d_refs[0][row(7 - kk, i), ls(p)])

    def from_halves(p, kk, i):
        e = a_ref[row(kk, i), ls(p)]
        o = a_ref[row(4 + kk, i), ls(p)]
        return weighted(p, kk, i, e + o, e - o)

    def from_whole(p, kk, i):
        return weighted(p, kk, i, a_ref[row(kk, i), ls(p)], a_ref[row(7 - kk, i), ls(p)])

    def lower(at, value):
        r = r_ref[at] - value
        r_ref[at] = r
        return r

    def second_direction(at, value):
        return KEEP * d_refs[0][at] + lower(at, value) * p_ref[at]

    def next_direction(at, value):
        return lower(at, value) * t_ref[at]

    def put(update):
        def handle(p, kk, index, values):
            dirs = []
            for s, k in enumerate((kk, 7 - kk)):
                group = []
                for n, i in enumerate(PAIRS[index]):
                    at = (row(k, i), ls(p))
                    group.append(update(at, values[n][s]))
                    d_refs[1][at] = group[-1]
                dirs.append(group)
            store_split(kk, index, p, dirs[0], dirs[1])
        return handle

    def put_resid(p, kk, index, values):
        for s, k in enumerate((kk, 7 - kk)):
            pair = [lower((row(k, i), ls(p)), values[n][s]) for n, i in enumerate(PAIRS[index])]
            high, low = split(jnp.concatenate(pair, axis=0))
            at = k * 64 + index * 16
            c_ref[at:at + 16, ls(p)] = high
            c_ref[512 + at:528 + at, ls(p)] = low

    def put_last(p, kk, index, values):
        for s, k in enumerate((kk, 7 - kk)):
            for n, i in enumerate(PAIRS[index]):
                lower((row(k, i), ls(p)), values[n][s])

    window = pl.ds(pl.multiple_of((own_x % groups * ny + own_y) * LANES, LANES), LANES)
    z_ref[...] = jnp.zeros((512, LANES), jnp.float32)

    def collect():
        z_ref[...] = z_ref[...] + d_refs[0][:, window]

    for step in range(2):
        collect()
        walk(from_halves, put(second_direction), multiply)
        turn_over()
        collect()
        def reduce(p):
            def first():
                both = dot(down0[...], c_ref[0:512, ls(p)])
                low_ref[:, ls(p)] = both[0:64] + both[64:128]

            def second():
                low_ref[:, ls(p)] = low_ref[:, ls(p)] + dot(down0[0:64, :], c_ref[512:1024, ls(p)])

            return first, second

        walk(from_halves, put_resid, reduce)
        flush()
        cor_ref[...] = cat3(coarse(fold1(low_ref[...])))
        turn_over()
        for p in parts:
            d_refs[0][:, ls(p)] = dot(up0[0:512, :], cor_ref[:, ls(p)])
            a_ref[:, ls(p)] = dot(up0[512:1024, :], cor_ref[:, ls(p)])
        collect()
        walk(from_whole, put(next_direction), multiply)
        turn_over()
        collect()
        if step == 0:
            walk(from_halves, put(next_direction), multiply)
            turn_over()
        else:
            walk(from_halves, put_last, lambda p: ())

    zero = jnp.zeros((SUBS, wide), jnp.float32)
    sums = [[zero] * 4 for weight in range(3)]
    for k in range(8):
        for i in range(8):
            b = b_ref[row(k, i), :]
            r = r_ref[row(k, i), :]
            image_all = b - r
            group = sums[(k in (0, 7)) + (i in (0, 7))]
            for n, (x, y) in enumerate(((r, image_all), (image_all, image_all), (r, r), (b, b))):
                group[n] = group[n] + x * y
    rw, ww, rr, bb = [jnp.sum((a + 0.5 * b + 0.25 * c) * f_j) for a, b, c in zip(*sums)]
    excess = rw / ww
    coef = 1.0 + excess
    rr = rr - rw * excess
    rel_ref[0] = jnp.sqrt(rr / bb)
    place = own_x // groups
    for i in range(8):
        sol = jnp.zeros((SUBS, LANES), jnp.float32)
        res = sol
        for k in range(8):
            r = r_ref[row(k, i), window]
            r = r - excess * (b_ref[row(k, i), window] - r)
            turn = (k - place) % LANES
            sol = jnp.where(lane == k, pltpu.roll(z_ref[row(k, i), :], turn, 1), sol)
            res = jnp.where(lane == k, pltpu.roll(r, turn, 1), res)
        sol_ref[i] = swap_rows(coef * sol, sub)
        res_ref[i] = swap_rows(res, sub)


def solve_all(nx, ny, near, far):
    tables = Tables()
    wide = ny * nx // SUBS * LANES
    consts = [tables.even, tables.odd, tables.down0, tables.up0, tables.op1, tables.down1,
              tables.up1, tables.op2, tables.rows]
    vmem = pl.BlockSpec(memory_space=pltpu.VMEM)
    field = pltpu.VMEM((512, wide), jnp.float32)
    return pl.pallas_call(
        lambda *refs: kernel(nx, ny, tables, *refs),
        in_specs=[vmem] * 11,
        out_specs=[vmem, vmem, pl.BlockSpec(memory_space=pltpu.SMEM)],
        out_shape=[
            jax.ShapeDtypeStruct(near.shape[1:], jnp.float32),
            jax.ShapeDtypeStruct(near.shape[1:], jnp.float32),
            jax.ShapeDtypeStruct((1,), jnp.float32),
        ],
        scratch_shapes=[
            field, field, field, field, field, field, field, field,
            pltpu.VMEM((512, LANES), jnp.float32),
            pltpu.VMEM((512, wide), jnp.bfloat16), pltpu.VMEM((512, wide), jnp.bfloat16),
            pltpu.VMEM((1024, wide), jnp.bfloat16), pltpu.VMEM((152, wide), jnp.float32),
            pltpu.VMEM((64, wide), jnp.float32), pltpu.VMEM((192, wide), jnp.bfloat16),
        ],
        name="solve_all",
    )(*[pltpu.with_memory_space_constraint(x, pltpu.VMEM)
             for x in (near, far, *[jnp.asarray(c) for c in consts])])


def pack_kernel(forcing, kappa, sigma, out_ref, coef_ref):
    sub = lax.broadcasted_iota(jnp.int32, (SUBS, LANES), 0)
    lane = lax.broadcasted_iota(jnp.int32, (SUBS, LANES), 1)
    count = kappa.shape[2]
    coef_ref[...] = jnp.zeros((SUBS, LANES), jnp.float32)
    coef_ref[0:1, 0:count] = kappa[0]
    coef_ref[1:2, 0:count] = sigma[0]
    spread = jnp.take_along_axis(coef_ref[...], lane // SUBS, axis=1)
    for i in range(SUBS):
        x = swap_rows(forcing[i], sub)
        x = x + jnp.where(lane % SUBS == 0, pltpu.roll(x, 1, 1), 0.0)
        if i == 0:
            x = jnp.where(lane % SUBS == SUBS - 1, spread, x)
        out_ref[0, i] = x


def packed_block(forcing, kappa, sigma):
    vmem = pl.BlockSpec(memory_space=pltpu.VMEM)
    return pl.pallas_call(
        pack_kernel,
        in_specs=[vmem] * 3,
        out_specs=vmem,
        out_shape=pltpu.VMEM((1, *forcing.shape), jnp.float32),
        scratch_shapes=[pltpu.VMEM((SUBS, LANES), jnp.float32)],
        name="pack_block",
    )(forcing, kappa, sigma)


def gathered(forcing, kappa, sigma):
    nx, ny = lax.axis_size("gx"), lax.axis_size("gy")
    block = packed_block(forcing, kappa, sigma)
    if ny > 1:
        other = lax.ppermute(block, "gy", [(i, i ^ 1) for i in range(ny)])
        block = jnp.concatenate([block, other], axis=0)
    step = nx // 2
    while step:
        other = lax.ppermute(block, "gx", [(i, i ^ step) for i in range(nx)])
        if step > 1:
            block = jnp.concatenate([block, other], axis=0)
        step //= 2
    sol, res, rel = solve_all(nx, ny, block, other)
    return sol, res, rel.reshape(())


def fits_one_device(mesh):
    nx, ny = mesh.shape["gx"], mesh.shape["gy"]
    power = nx & (nx - 1) == 0
    return power and nx % SUBS == 0 and ny <= 2 and nx * ny <= 64


def solution(mesh):
    spec = P("gx", "gy", None)
    small = fits_one_device(mesh)

    def local(forcing, kappa, sigma):
        plain = forcing.shape == (SUBS, SUBS, LANES) and kappa.shape == (1, 1, LANES // SUBS)
        return (gathered if small and plain else distributed)(forcing, kappa, sigma)

    return jax.shard_map(
        local, mesh=mesh, in_specs=(spec, spec, spec), out_specs=(spec, spec, P()),
        check_vma=False,
    )
```

```python
import jax
import jax.numpy as jnp
import numpy as np
from jax import lax
from jax.experimental import pallas as pl
from jax.experimental.pallas import tpu as pltpu
from jax.sharding import PartitionSpec as P


def with_halo(cells, sides, width):
    for axis, dim in sides:
        count = lax.axis_size(axis)
        head = lax.slice_in_dim(cells, 0, width, axis=dim)
        tail = lax.slice_in_dim(cells, cells.shape[dim] - width, cells.shape[dim], axis=dim)
        cells = jnp.concatenate(
            [
                lax.ppermute(tail, axis, [(i, (i + 1) % count) for i in range(count)]),
                cells,
                lax.ppermute(head, axis, [((i + 1) % count, i) for i in range(count)]),
            ],
            axis=dim,
        )
    return cells


def legendre_table(points, order):
    columns = [points * 0.0 + 1.0, points]
    for degree in range(2, order + 1):
        columns.append(
            ((2 * degree - 1) * points * columns[-1] - (degree - 1) * columns[-2]) / degree
        )
    return np.stack(columns, axis=1)


def lobatto(count):
    order = count - 1
    points = np.cos(np.pi * np.arange(count) / order)
    for sweep in range(60):
        table = legendre_table(points, order)
        points = points - (points * table[:, order] - table[:, order - 1]) / (
            count * table[:, order]
        )
    table = legendre_table(points, order)
    weights = 2.0 / (order * count * table[:, order] ** 2)
    values = table[:, order]
    points, weights, values = (points[::-1], weights[::-1], values[::-1])
    spread = points[:, None] - points[None, :] + np.eye(count)
    deriv = values[:, None] / values[None, :] / spread * (1.0 - np.eye(count))
    corner = order * (order + 1) / 4.0
    ends = np.array([-corner] + [0.0] * (count - 2) + [corner])
    return (points, weights, deriv + np.eye(count) * ends[None, :])


def lagrange(fine_points, coarse_points):
    columns = []
    for column in range(len(coarse_points)):
        value = fine_points * 0.0 + 1.0
        for other in range(len(coarse_points)):
            if other != column:
                value = (
                    value
                    * (fine_points - coarse_points[other])
                    / (coarse_points[column] - coarse_points[other])
                )
        columns.append(value)
    return np.stack(columns, axis=1)


def edge_factor(count, blocks):
    index = jnp.arange(count)
    single = jnp.where((index == 0) | (index == count - 1), 0.5, 1.0).astype(jnp.float32)
    return jnp.tile(single, blocks)


def multiplicity(count, blocks):
    first = edge_factor(count, blocks[0])
    second = edge_factor(count, blocks[1])
    third = edge_factor(count, blocks[2])
    return first[:, None, None] * second[None, :, None] * third[None, None, :]


def element_apply(field, kappa, sigma, deriv, weights):
    count = deriv.shape[0]
    ex, ey, ez = kappa.shape
    high = lax.Precision.HIGHEST
    block = field.reshape(ex, count, ey, count, ez, count)
    mass = (weights[:, None, None] * weights[None, :, None] * weights[None, None, :])[
        None, :, None, :, None, :
    ]
    first = jnp.einsum("ai,eifjgk->eafjgk", deriv, block, precision=high)
    total = jnp.einsum("ai,eafjgk->eifjgk", deriv, first * mass, precision=high)
    second = jnp.einsum("aj,eifjgk->eifagk", deriv, block, precision=high)
    total = total + jnp.einsum("aj,eifagk->eifjgk", deriv, second * mass, precision=high)
    third = jnp.einsum("ak,eifjgk->eifjga", deriv, block, precision=high)
    total = total + jnp.einsum("ak,eifjga->eifjgk", deriv, third * mass, precision=high)
    coeff = kappa[:, None, :, None, :, None]
    shift = sigma[:, None, :, None, :, None]
    return (coeff * total + shift * mass * block).reshape(field.shape)


def element_diagonal(kappa, sigma, deriv, weights):
    count = deriv.shape[0]
    ex, ey, ez = kappa.shape
    stiff = jnp.sum(deriv * deriv * weights[:, None], axis=0)
    term = stiff[:, None, None] * weights[None, :, None] * weights[None, None, :]
    term = term + weights[:, None, None] * stiff[None, :, None] * weights[None, None, :]
    term = term + weights[:, None, None] * weights[None, :, None] * stiff[None, None, :]
    mass = weights[:, None, None] * weights[None, :, None] * weights[None, None, :]
    coeff = kappa[:, None, :, None, :, None]
    shift = sigma[:, None, :, None, :, None]
    full = coeff * term[None, :, None, :, None, :] + shift * mass[None, :, None, :, None, :]
    return full.reshape(ex * count, ey * count, ez * count)


def fold_axis(field, dim, count):
    size = field.shape[dim]
    position = jnp.arange(size) % count
    shape = [1, 1, 1]
    shape[dim] = size
    first = (position == 0).reshape(shape)
    last = (position == count - 1).reshape(shape)
    before = jnp.roll(field, 1, dim)
    after = jnp.roll(field, -1, dim)
    return field + jnp.where(first, before, 0.0) + jnp.where(last, after, 0.0)


def fold_padded(padded, dim, count):
    size = padded.shape[dim] - 2
    center = lax.slice_in_dim(padded, 1, size + 1, axis=dim)
    before = lax.slice_in_dim(padded, 0, size, axis=dim)
    after = lax.slice_in_dim(padded, 2, size + 2, axis=dim)
    position = jnp.arange(size) % count
    shape = [1, 1, 1]
    shape[dim] = size
    first = (position == 0).reshape(shape)
    last = (position == count - 1).reshape(shape)
    return center + jnp.where(first, before, 0.0) + jnp.where(last, after, 0.0)


def assemble(field, count, finest):
    if finest:
        padded = with_halo(field, (("gx", 0), ("gy", 1)), 1)
        field = fold_padded(fold_padded(padded, 0, count), 1, count)
    else:
        padded = with_halo(field, (("gx", 0), ("gy", 1)), 1)
        field = fold_padded(fold_padded(padded, 0, count), 1, count)
    return fold_axis(field, 2, count)


def restrict(field, interp, blocks, fine_count, coarse_count):
    high = lax.Precision.HIGHEST
    block = field.reshape(blocks[0], fine_count, blocks[1], fine_count, blocks[2], fine_count)
    one = jnp.einsum("ia,eifjgk->eafjgk", interp, block, precision=high)
    two = jnp.einsum("jb,eafjgk->eafbgk", interp, one, precision=high)
    three = jnp.einsum("kc,eafbgk->eafbgc", interp, two, precision=high)
    return three.reshape(
        blocks[0] * coarse_count, blocks[1] * coarse_count, blocks[2] * coarse_count
    )


def prolong(field, interp, blocks, fine_count, coarse_count):
    high = lax.Precision.HIGHEST
    block = field.reshape(blocks[0], coarse_count, blocks[1], coarse_count, blocks[2], coarse_count)
    one = jnp.einsum("ia,eafbgc->eifbgc", interp, block, precision=high)
    two = jnp.einsum("jb,eifbgc->eifjgc", interp, one, precision=high)
    three = jnp.einsum("kc,eifjgc->eifjgk", interp, two, precision=high)
    return three.reshape(blocks[0] * fine_count, blocks[1] * fine_count, blocks[2] * fine_count)


def distributed(forcing, kappa, sigma):
    blocks = kappa.shape
    counts = [8, 4, 2]
    tables = [lobatto(count) for count in counts]
    derivs = [jnp.asarray(table[2], jnp.float32) for table in tables]
    weights = [jnp.asarray(table[1], jnp.float32) for table in tables]
    interps = [
        jnp.asarray(lagrange(tables[level][0], tables[level + 1][0]), jnp.float32)
        for level in range(2)
    ]
    mults = [multiplicity(count, blocks) for count in counts]
    diags = [
        assemble(
            element_diagonal(kappa, sigma, derivs[level], weights[level]), counts[level], level == 0
        )
        for level in range(3)
    ]
    center = 1.65
    half = 1.35
    ratio = center / half

    def operate(field, level):
        return assemble(
            element_apply(field, kappa, sigma, derivs[level], weights[level]),
            counts[level],
            level == 0,
        )

    def smooth(resid, level, steps, keep_last):
        rho = 1.0 / ratio
        direction = resid / (center * diags[level])
        iterate = direction
        for step in range(steps):
            if step > 0:
                rho_next = 1.0 / (2.0 * ratio - rho)
                direction = (
                    rho_next * rho * direction + 2.0 * rho_next / half * resid / diags[level]
                )
                iterate = iterate + direction
                rho = rho_next
            if step < steps - 1 or keep_last:
                resid = resid - operate(direction, level)
        return (iterate, resid)

    def vcycle(resid, level):
        if level == 2:
            iterate, unused = smooth(resid, level, 2, False)
            return iterate
        iterate, resid = smooth(resid, level, 2, True)
        coarse = assemble(
            restrict(
                mults[level] * resid, interps[level], blocks, counts[level], counts[level + 1]
            ),
            counts[level + 1],
            False,
        )
        correction = prolong(
            vcycle(coarse, level + 1), interps[level], blocks, counts[level], counts[level + 1]
        )
        iterate = iterate + correction
        resid = resid - operate(correction, level)
        return iterate + resid / (center * diags[level])

    load = assemble(forcing, 8, True)
    first = vcycle(load, 0)
    image_first = operate(first, 0)
    second = vcycle(load - image_first, 0)
    combined = first + second
    image = operate(combined, 0)
    weight = mults[0]
    load_sq, load_image, image_sq = lax.psum(
        (
            jnp.sum(weight * load * load),
            jnp.sum(weight * load * image),
            jnp.sum(weight * image * image),
        ),
        ("gx", "gy"),
    )
    coef = load_image / image_sq
    solution = coef * combined
    residual = load - coef * image
    rel_residual = jnp.sqrt((load_sq - load_image * load_image / image_sq) / load_sq)
    return (solution, residual, rel_residual)


THETA = 1.65
DELTA = 1.35
RATIO = THETA / DELTA
RHO0 = 1.0 / RATIO
RHO1 = 1.0 / (2.0 * RATIO - RHO0)
KEEP = RHO1 * RHO0
PUSH = 2.0 * RHO1 / DELTA
LANES = 128
SUBS = 8


def triple(first, second, third):
    return np.kron(first, np.kron(second, third))


def split_const(matrix):
    high = matrix.astype(jnp.bfloat16)
    low = (matrix - high.astype(np.float64)).astype(jnp.bfloat16)
    return high, low


def stacked(matrix):
    high, low = split_const(matrix)
    return np.concatenate([high, high, low], axis=1)


J_ORDER = (0, 1, 2, 3, 7, 5, 6, 4)
SPLIT_AT = ((0, 1), (2, 1))
PAIRS = ((0, 7), (1, 2), (3, 4), (5, 6))
FACE = (0, 1, 3, 2)
ROWS1 = tuple(
    (k * 4 + FACE[2 * ih + il]) * 4 + FACE[2 * jh + jl]
    for k in range(4) for ih in range(2) for jh in range(2) for il in range(2) for jl in range(2)
)
ROWS2 = tuple((k * 2 + i) * 2 + j for j in range(2) for k in range(2) for i in range(2))


def padded(matrix, rows, columns):
    return np.pad(matrix, ((0, rows - matrix.shape[0]), (0, columns - matrix.shape[1])))


class Tables:
    def __init__(self):
        tables = [lobatto(count) for count in (8, 4, 2)]
        self.weights = [table[1] for table in tables]
        stiff = [table[2].T @ np.diag(table[1]) @ table[2] for table in tables]
        self.squares = [np.sum(t[2] * t[2] * t[1][:, None], axis=0) for t in tables]
        interps = [lagrange(tables[level][0], tables[level + 1][0]) for level in range(2)]
        factor = [np.where((np.arange(n) == 0) | (np.arange(n) == n - 1), 0.5, 1.0) for n in (8, 4)]
        down = [interps[level].T * factor[level][None, :] for level in range(2)]
        flat = [i for pair in PAIRS for i in pair]
        rows0 = [(k * 8 + i) * 8 + j for k in range(8) for i in range(8) for j in J_ORDER]
        data0 = [(k * 8 + i) * 8 + j for k in range(8) for i in flat for j in J_ORDER]
        rows1, rows2 = list(ROWS1), list(ROWS2)
        w, k = np.diag(self.weights[0]), stiff[0]
        plane = np.kron(k, w) + np.kron(w, k)
        both = np.kron(w, w)
        flip = k[:4, ::-1][:, :4]
        half = np.kron(0.5 * w[:4, :4], plane)
        even = np.kron(0.5 * (k[:4, :4] + flip), both) + half
        odd = np.kron(0.5 * (k[:4, :4] - flip), both) + half
        self.even = stacked(even[np.ix_(rows0[:256], data0[:256])])
        self.odd = stacked(odd[np.ix_(rows0[:256], data0[:256])])
        high, low = split_const(triple(down[0], down[0], down[0])[np.ix_(rows1, data0)])
        self.down0 = np.concatenate([high, low], axis=0)
        up = triple(interps[0], interps[0], interps[0])
        stiffness = np.kron(k, both) + np.kron(w, plane)
        self.up0 = stacked(np.concatenate([up[np.ix_(rows0, rows1)], (stiffness @ up)[np.ix_(rows0, rows1)]]))
        w, k = np.diag(self.weights[1]), stiff[1]
        stiffness = triple(k, w, w) + triple(w, k, w) + triple(w, w, k)
        up = triple(interps[1], interps[1], interps[1])
        self.op1 = stacked(stiffness[np.ix_(rows1, rows1)])
        self.down1 = padded(stacked(triple(down[1], down[1], down[1])[np.ix_(rows2, rows1)]), 16, 192)
        self.up1 = padded(stacked(
            np.concatenate([up[np.ix_(rows1, rows2)], (stiffness @ up)[np.ix_(rows1, rows2)]])), 128, 32)
        w, k = np.diag(self.weights[2]), stiff[2]
        op2 = (triple(k, w, w) + triple(w, k, w) + triple(w, w, k))[np.ix_(rows2, rows2)]
        wide = lambda column: np.repeat(np.asarray(column, np.float32)[:, None], LANES, axis=1)
        blocks = [wide(self.weights[0][list(J_ORDER)]), wide(self.squares[0][list(J_ORDER)]),
                  wide(factor[0][list(J_ORDER)])]
        for level, order in ((1, rows1), (2, rows2)):
            a, b = self.weights[level], self.squares[level]
            blocks.append(wide(triple(a, a, a)[order]))
            blocks.append(wide((triple(b, a, a) + triple(a, b, a) + triple(a, a, b))[order]))
        at = np.arange(SUBS)
        self.op2 = np.concatenate([wide(op2[at, (at - turn) % SUBS]) for turn in range(SUBS)], axis=0)
        self.rows = np.concatenate(blocks, axis=0)


def gather_rounds(nx, ny):
    dims = []
    step = nx // 2
    while step > 1:
        dims.append((step, 0))
        step //= 2
    if ny > 1:
        dims.insert(len(dims) - 1, (0, 1))
    return [dims[n:n + 2] for n in range(0, len(dims), 2)]


def swap_rows(x, sub):
    return jnp.where(sub == 4, pltpu.roll(x, 5, 0), jnp.where(sub == 7, pltpu.roll(x, 3, 0), x))


def kernel(nx, ny, tables, near, far, even, odd, down0, up0, op1, down1, up1, op2, rows,
           sol_ref, res_ref, rel_ref, b_ref, r_ref, d_ref, other_ref, v_ref, p_ref, t_ref, a_ref, z_ref,
           be_ref, bo_ref, c_ref, lane_ref, low_ref, cor_ref):
    groups = nx // SUBS
    tiles = ny * groups
    part_wide = ny * LANES
    wide = tiles * LANES
    own_x, own_y = lax.axis_index("gx"), lax.axis_index("gy")
    sub = lax.broadcasted_iota(jnp.int32, (SUBS, LANES), 0)
    lanes = lax.broadcasted_iota(jnp.int32, (SUBS, LANES), 1)
    lane = lanes % SUBS
    w = [float(x) for x in tables.weights[0]]
    q = [float(x) for x in tables.squares[0]]
    parts = range(groups)

    def cut(x):
        return [x[:, t * LANES:(t + 1) * LANES] for t in range(x.shape[1] // LANES)]

    def join(pieces):
        return jnp.concatenate(pieces, axis=1)

    def ls(p):
        return slice(p * part_wide, (p + 1) * part_wide)

    def split_parts(x):
        return [x[:, ls(p)] for p in parts]

    def across(x, count):
        return join([x] * count)

    sub_w = across(sub, tiles)
    sub_p = across(sub, ny)

    def move(x, amount):
        amount %= LANES
        return join([pltpu.roll(t, amount, 1) for t in cut(x)]) if amount else x

    def x_up(x, p, more=0):
        if p:
            return move(x[p - 1], more)
        prev = cut(x[groups - 1])
        return join([jnp.where(lane == 0, pltpu.roll(t, (LANES - SUBS + 1 + more) % LANES, 1),
                               pltpu.roll(t, 1 + more, 1)) for t in prev])

    def x_down(x, p, more=0):
        if p < groups - 1:
            return move(x[p + 1], more)
        succ = cut(x[0])
        return join([jnp.where(lane == SUBS - 1, pltpu.roll(t, SUBS - 1 + more, 1),
                               pltpu.roll(t, (LANES - 1 + more) % LANES, 1)) for t in succ])

    up, down = SUBS, LANES - SUBS

    def y_fold(x, face):
        t = cut(x)
        other = join([t[(n // ny) * ny + (n + 1) % ny] for n in range(len(t))])
        return x + jnp.where(face, pltpu.roll(other, 4, 0), 0.0)

    face0 = sub_p % 4 == 0
    face1 = sub_w % 2 == 0

    def row(k, i):
        return pl.ds(k * 64 + i * 8, 8)

    for t in range(tiles):
        part, y_index = t // ny, t % ny
        at = slice(t * LANES, (t + 1) * LANES)
        use_near = ((part ^ own_x) & 1) == 0
        slots = []
        for c in range(SUBS):
            delta = (c * groups + part) ^ own_x
            slot, size = jnp.int32(0), 1
            for dims in gather_rounds(nx, ny):
                flags = [y_index ^ own_y if along_y else jnp.where((delta & along_x) != 0, 1, 0)
                         for along_x, along_y in dims]
                if len(dims) == 2:
                    place = flags[0] * 2 + flags[1] * 3 - flags[0] * flags[1] * 4
                else:
                    place = flags[0]
                slot = slot + place * size
                size *= 1 << len(dims)
            slots.append(slot)
        blocks = [[jnp.where(use_near, near[slot, i], far[slot, i]) for slot in slots]
                  for i in range(8)]
        for step in (1, 2, 4):
            keep = (lane & step) == 0
            low = [c for c in range(SUBS) if not c & step]
            turned = [[jnp.take_along_axis(jnp.where(keep, b[c + step], b[c]), lanes ^ step, axis=1)
                       for c in low] for b in blocks]
            fresh = []
            for b, turn in zip(blocks, turned):
                out = list(b)
                for c, x in zip(low, turn):
                    out[c] = jnp.where(keep, b[c], x)
                    out[c + step] = jnp.where(keep, x, b[c + step])
                fresh.append(out)
            blocks = fresh
        for i, b in enumerate(blocks):
            for k in range(7):
                v_ref[row(k, i), at] = b[k]
            v_ref[row(7, i), at] = pltpu.roll(b[0], down, 1)
        lane_ref[0:8, at] = blocks[0][7]
    kap1 = lane_ref[0:1, :]
    sig1 = lane_ref[1:2, :]
    w_j = across(rows[0:8, :], ny)
    q_j = across(rows[8:16, :], ny)
    f_j = across(rows[16:24, :], tiles)
    kap = [jnp.broadcast_to(kap1[:, ls(p)], (SUBS, part_wide)) for p in parts]
    sig_w = [jnp.broadcast_to(sig1[:, ls(p)], (SUBS, part_wide)) * w_j for p in parts]

    def split(value):
        high = value.astype(jnp.bfloat16)
        return high, (value - high.astype(jnp.float32)).astype(jnp.bfloat16)

    def store_split(kk, index, p, low_pair, high_pair):
        a = jnp.concatenate(low_pair, axis=0)
        b = jnp.concatenate(high_pair, axis=0)
        for ref, value in ((be_ref, a + b), (bo_ref, a - b)):
            high, low = split(value)
            at = kk * 64 + index * 16
            ref[at:at + 16, ls(p)] = high
            ref[256 + at:272 + at, ls(p)] = low

    def fold_z(kk, pair):
        a, b = pair
        return (a + move(b, up), b + move(a, down)) if kk == 0 else (a, b)

    def inner(p, kk, index, get, with_z=True):
        out = []
        for i in PAIRS[index]:
            pair = get(p, kk, i)
            pair = fold_z(kk, pair) if with_z else pair
            out.append([y_fold(x, face0) for x in pair])
        return out

    def faces(kk, get, with_z=True):
        first, last = [], []
        for p in parts:
            a, b = get(p, kk, 0), get(p, kk, 7)
            first.append(fold_z(kk, a) if with_z else a)
            last.append(fold_z(kk, b) if with_z else b)
        out = []
        for p in parts:
            a, b = [], []
            for s in range(2):
                firsts, lasts = [x[s] for x in first], [x[s] for x in last]
                a.append(y_fold(firsts[p] + x_up(lasts, p), face0))
                b.append(y_fold(lasts[p] + x_down(firsts, p), face0))
            out.append([a, b])
        return out

    pending = []

    def flush():
        while pending:
            pending.pop(0)()

    def walk(get, handle, after, with_z=True):
        for p in parts:
            for kk in range(4):
                for index in (1, 2, 3):
                    if pending and (kk, index) in SPLIT_AT:
                        pending.pop(0)()
                    handle(p, kk, index, inner(p, kk, index, get, with_z))
            flush()
            if p == 0:
                for kk in range(4):
                    for n, values in enumerate(faces(kk, get, with_z)):
                        handle(n, kk, 0, values)
            pending.extend(after(p))

    def dot(a, b):
        return jnp.dot(a, b, preferred_element_type=jnp.float32)

    def rows_of(ref, p):
        return jnp.concatenate([ref[:, ls(p)], ref[0:256, ls(p)]], axis=0)

    def multiply(p):
        def first():
            a_ref[0:256, ls(p)] = dot(even[...], rows_of(be_ref, p))

        def second():
            a_ref[256:512, ls(p)] = dot(odd[...], rows_of(bo_ref, p))

        return first, second

    def point(p, kk, i):
        out = []
        for k in (kk, 7 - kk):
            s1 = q[k] * w[i] + w[k] * q[i]
            s2 = w[k] * w[i]
            out.append(kap[p] * (s1 * w_j + s2 * q_j) + s2 * sig_w[p])
        return out

    def put_diag(p, kk, index, values):
        for s, k in enumerate((kk, 7 - kk)):
            for n, i in enumerate(PAIRS[index]):
                inverse = 1.0 / values[n][s]
                p_ref[row(k, i), ls(p)] = inverse * PUSH
                t_ref[row(k, i), ls(p)] = inverse * (1.0 / THETA)

    def put_load(p, kk, index, values):
        dirs = []
        for s, k in enumerate((kk, 7 - kk)):
            group = []
            for n, i in enumerate(PAIRS[index]):
                at = (row(k, i), ls(p))
                b_ref[at] = values[n][s]
                r_ref[at] = values[n][s]
                group.append(values[n][s] * t_ref[at])
                d_ref[at] = group[-1]
            dirs.append(group)
        store_split(kk, index, p, dirs[0], dirs[1])

    walk(point, put_diag, lambda p: ())
    walk(lambda p, kk, i: (v_ref[row(kk, i), ls(p)], v_ref[row(7 - kk, i), ls(p)]),
         put_load, multiply, with_z=False)

    low_face = (sub_w // 2) % 2 == 0

    def x_up_all(x, more=0):
        return join([x_up(split_parts(x), p, more) for p in parts])

    def x_down_all(x, more=0):
        return join([x_down(split_parts(x), p, more) for p in parts])

    def fold1(x):
        c = [(x[16 * k:16 * k + 8], x[16 * k + 8:16 * k + 16]) for k in range(4)]
        out = []
        for k, (a, b) in enumerate(c):
            na, nb = x_up_all(b), x_down_all(a)
            if k in (0, 3):
                g, h = c[3 - k]
                amount = up if k == 0 else down
                na = na + x_up_all(h, amount)
                nb = nb + x_down_all(g, amount)
                a, b = a + move(g, amount), b + move(h, amount)
            out.append(y_fold(a + jnp.where(low_face, na, 0.0), face1))
            out.append(y_fold(b + jnp.where(low_face, nb, 0.0), face1))
        return jnp.concatenate(out, axis=0)

    first_k = (sub_w // 2) % 2 == 0
    first_i = sub_w % 2 == 0

    def fold2(x):
        other_k = jnp.where(first_k, pltpu.roll(x, 6, 0), pltpu.roll(x, 2, 0))
        other_i = jnp.where(first_i, pltpu.roll(x, 7, 0), pltpu.roll(x, 1, 0))
        both = jnp.where(first_i, pltpu.roll(other_k, 7, 0), pltpu.roll(other_k, 1, 0))
        x = x + jnp.where(first_k, move(other_k, up), move(other_k, down))
        x = x + jnp.where(first_i, x_up_all(other_i), x_down_all(other_i))
        x = x + jnp.where(first_k, jnp.where(first_i, x_up_all(both, up), x_down_all(both, up)),
                          jnp.where(first_i, x_up_all(both, down), x_down_all(both, down)))
        return y_fold(x, sub_w >= 0)

    def cat3(x):
        high, low = split(x)
        return jnp.concatenate([high, low, high], axis=0)

    def cat3_small(x):
        high = x.astype(jnp.bfloat16).astype(jnp.float32)
        return jnp.concatenate([high, x - high, high, jnp.zeros_like(x)], axis=0).astype(jnp.bfloat16)

    mass1 = across(rows[24:88, :], tiles)
    point1 = across(rows[88:152, :], tiles)
    mass2 = across(rows[152:160, :], tiles)
    point2 = across(rows[160:168, :], tiles)
    inv1_ref, mass1_ref = lane_ref.at[8:72, :], lane_ref.at[72:136, :]
    inv1_ref[...] = 1.0 / fold1(kap1 * point1 + sig1 * mass1)
    mass1_ref[...] = sig1 * mass1
    lane_ref[136:144, :] = 1.0 / fold2(kap1 * point2 + sig1 * mass2)
    lane_ref[144:152, :] = sig1 * mass2

    def apply1(v):
        return fold1(kap1 * dot(op1[...], cat3(v)) + mass1_ref[...] * v)

    def apply2(v):
        terms = [across(op2[8 * n:8 * n + 8, :], tiles) * (pltpu.roll(v, n, 0) if n else v)
                 for n in range(SUBS)]
        while len(terms) > 1:
            terms = [x + y for x, y in zip(terms[::2], terms[1::2])]
        return fold2(kap1 * terms[0] + lane_ref[144:152, :] * v)

    def coarse(resid):
        inverse = inv1_ref[...]
        d = resid * inverse * (1.0 / THETA)
        x = d
        resid = resid - apply1(d)
        d = KEEP * d + PUSH * (resid * inverse)
        x = x + d
        resid = resid - apply1(d)
        low = fold2(dot(down1[...], cat3(resid))[0:8])
        inverse2 = lane_ref[136:144, :]
        d = low * inverse2 * (1.0 / THETA)
        y = d
        low = low - apply2(d)
        y = y + KEEP * d + PUSH * (low * inverse2)
        both = dot(up1[...], cat3_small(y))
        e = both[0:64]
        x = x + e
        resid = resid - fold1(kap1 * both[64:128] + mass1_ref[...] * e)
        return x + resid * inverse * (1.0 / THETA)

    d_refs = [d_ref, other_ref]

    def turn_over():
        d_refs.reverse()

    def weighted(p, kk, i, a, b):
        scale = sig_w[p] * (w[kk] * w[i])
        return (kap[p] * a + scale * d_refs[0][row(kk, i), ls(p)],
                kap[p] * b + scale * d_refs[0][row(7 - kk, i), ls(p)])

    def from_halves(p, kk, i):
        e = a_ref[row(kk, i), ls(p)]
        o = a_ref[row(4 + kk, i), ls(p)]
        return weighted(p, kk, i, e + o, e - o)

    def from_whole(p, kk, i):
        return weighted(p, kk, i, a_ref[row(kk, i), ls(p)], a_ref[row(7 - kk, i), ls(p)])

    def lower(at, value):
        r = r_ref[at] - value
        r_ref[at] = r
        return r

    def second_direction(at, value):
        return KEEP * d_refs[0][at] + lower(at, value) * p_ref[at]

    def next_direction(at, value):
        return lower(at, value) * t_ref[at]

    def put(update):
        def handle(p, kk, index, values):
            dirs = []
            for s, k in enumerate((kk, 7 - kk)):
                group = []
                for n, i in enumerate(PAIRS[index]):
                    at = (row(k, i), ls(p))
                    group.append(update(at, values[n][s]))
                    d_refs[1][at] = group[-1]
                dirs.append(group)
            store_split(kk, index, p, dirs[0], dirs[1])
        return handle

    def put_resid(p, kk, index, values):
        for s, k in enumerate((kk, 7 - kk)):
            pair = [lower((row(k, i), ls(p)), values[n][s]) for n, i in enumerate(PAIRS[index])]
            high, low = split(jnp.concatenate(pair, axis=0))
            at = k * 64 + index * 16
            c_ref[at:at + 16, ls(p)] = high
            c_ref[512 + at:528 + at, ls(p)] = low

    def put_last(p, kk, index, values):
        for s, k in enumerate((kk, 7 - kk)):
            for n, i in enumerate(PAIRS[index]):
                lower((row(k, i), ls(p)), values[n][s])

    window = pl.ds(pl.multiple_of((own_x % groups * ny + own_y) * LANES, LANES), LANES)
    z_ref[...] = jnp.zeros((512, LANES), jnp.float32)

    def collect():
        z_ref[...] = z_ref[...] + d_refs[0][:, window]

    for step in range(2):
        collect()
        walk(from_halves, put(second_direction), multiply)
        turn_over()
        collect()
        def reduce(p):
            def first():
                both = dot(down0[...], c_ref[0:512, ls(p)])
                low_ref[:, ls(p)] = both[0:64] + both[64:128]

            def second():
                low_ref[:, ls(p)] = low_ref[:, ls(p)] + dot(down0[0:64, :], c_ref[512:1024, ls(p)])

            return first, second

        walk(from_halves, put_resid, reduce)
        flush()
        cor_ref[...] = cat3(coarse(fold1(low_ref[...])))
        turn_over()
        for p in parts:
            d_refs[0][:, ls(p)] = dot(up0[0:512, :], cor_ref[:, ls(p)])
            a_ref[:, ls(p)] = dot(up0[512:1024, :], cor_ref[:, ls(p)])
        collect()
        walk(from_whole, put(next_direction), multiply)
        turn_over()
        collect()
        if step == 0:
            walk(from_halves, put(next_direction), multiply)
            turn_over()
        else:
            walk(from_halves, put_last, lambda p: ())

    zero = jnp.zeros((SUBS, wide), jnp.float32)
    sums = [[zero] * 4 for weight in range(3)]
    for k in range(8):
        for i in range(8):
            b = b_ref[row(k, i), :]
            r = r_ref[row(k, i), :]
            image_all = b - r
            group = sums[(k in (0, 7)) + (i in (0, 7))]
            for n, (x, y) in enumerate(((r, image_all), (image_all, image_all), (r, r), (b, b))):
                group[n] = group[n] + x * y
    rw, ww, rr, bb = [jnp.sum((a + 0.5 * b + 0.25 * c) * f_j) for a, b, c in zip(*sums)]
    excess = rw / ww
    coef = 1.0 + excess
    rr = rr - rw * excess
    rel_ref[0] = jnp.sqrt(rr / bb)
    place = own_x // groups
    for i in range(8):
        sol = jnp.zeros((SUBS, LANES), jnp.float32)
        res = sol
        for k in range(8):
            r = r_ref[row(k, i), window]
            r = r - excess * (b_ref[row(k, i), window] - r)
            turn = (k - place) % LANES
            sol = jnp.where(lane == k, pltpu.roll(z_ref[row(k, i), :], turn, 1), sol)
            res = jnp.where(lane == k, pltpu.roll(r, turn, 1), res)
        sol_ref[i] = swap_rows(coef * sol, sub)
        res_ref[i] = swap_rows(res, sub)


def solve_all(nx, ny, near, far):
    tables = Tables()
    wide = ny * nx // SUBS * LANES
    consts = [tables.even, tables.odd, tables.down0, tables.up0, tables.op1, tables.down1,
              tables.up1, tables.op2, tables.rows]
    vmem = pl.BlockSpec(memory_space=pltpu.VMEM)
    field = pltpu.VMEM((512, wide), jnp.float32)
    return pl.pallas_call(
        lambda *refs: kernel(nx, ny, tables, *refs),
        in_specs=[vmem] * 11,
        out_specs=[vmem, vmem, pl.BlockSpec(memory_space=pltpu.SMEM)],
        out_shape=[
            jax.ShapeDtypeStruct(near.shape[1:], jnp.float32),
            jax.ShapeDtypeStruct(near.shape[1:], jnp.float32),
            jax.ShapeDtypeStruct((1,), jnp.float32),
        ],
        scratch_shapes=[
            field, field, field, field, field, field, field, field,
            pltpu.VMEM((512, LANES), jnp.float32),
            pltpu.VMEM((512, wide), jnp.bfloat16), pltpu.VMEM((512, wide), jnp.bfloat16),
            pltpu.VMEM((1024, wide), jnp.bfloat16), pltpu.VMEM((152, wide), jnp.float32),
            pltpu.VMEM((64, wide), jnp.float32), pltpu.VMEM((192, wide), jnp.bfloat16),
        ],
        name="solve_all",
    )(*[pltpu.with_memory_space_constraint(x, pltpu.VMEM)
             for x in (near, far, *[jnp.asarray(c) for c in consts])])


def pack_kernel(forcing, kappa, sigma, out_ref, coef_ref):
    sub = lax.broadcasted_iota(jnp.int32, (SUBS, LANES), 0)
    lane = lax.broadcasted_iota(jnp.int32, (SUBS, LANES), 1)
    count = kappa.shape[2]
    coef_ref[...] = jnp.zeros((SUBS, LANES), jnp.float32)
    coef_ref[0:1, 0:count] = kappa[0]
    coef_ref[1:2, 0:count] = sigma[0]
    spread = jnp.take_along_axis(coef_ref[...], lane // SUBS, axis=1)
    for i in range(SUBS):
        x = swap_rows(forcing[i], sub)
        x = x + jnp.where(lane % SUBS == 0, pltpu.roll(x, 1, 1), 0.0)
        if i == 0:
            x = jnp.where(lane % SUBS == SUBS - 1, spread, x)
        out_ref[0, i] = x


def packed_block(forcing, kappa, sigma):
    vmem = pl.BlockSpec(memory_space=pltpu.VMEM)
    return pl.pallas_call(
        pack_kernel,
        in_specs=[vmem] * 3,
        out_specs=vmem,
        out_shape=pltpu.VMEM((1, *forcing.shape), jnp.float32),
        scratch_shapes=[pltpu.VMEM((SUBS, LANES), jnp.float32)],
        name="pack_block",
    )(forcing, kappa, sigma)


def gathered(forcing, kappa, sigma):
    nx, ny = lax.axis_size("gx"), lax.axis_size("gy")

    def swap(block, along_x, along_y):
        pairs = [(a * ny + b, (a ^ along_x) * ny + (b ^ along_y)) for a in range(nx) for b in range(ny)]
        return lax.ppermute(block, ("gx", "gy"), pairs)

    block = packed_block(forcing, kappa, sigma)
    for dims in gather_rounds(nx, ny):
        if len(dims) == 2:
            (x0, y0), (x1, y1) = dims
            masks = [(x0 ^ x1, y0 ^ y1), dims[0], dims[1]]
        else:
            masks = dims
        block = jnp.concatenate([block] + [swap(block, *mask) for mask in masks], axis=0)
    sol, res, rel = solve_all(nx, ny, block, swap(block, 1, 0))
    return sol, res, rel.reshape(())


def fits_one_device(mesh):
    nx, ny = mesh.shape["gx"], mesh.shape["gy"]
    power = nx & (nx - 1) == 0
    return power and nx % SUBS == 0 and ny <= 2 and nx * ny <= 64


def solution(mesh):
    spec = P("gx", "gy", None)
    small = fits_one_device(mesh)

    def local(forcing, kappa, sigma):
        plain = forcing.shape == (SUBS, SUBS, LANES) and kappa.shape == (1, 1, LANES // SUBS)
        return (gathered if small and plain else distributed)(forcing, kappa, sigma)

    return jax.shard_map(
        local, mesh=mesh, in_specs=(spec, spec, spec), out_specs=(spec, spec, P()),
        check_vma=False,
    )
```

```python
import jax
import jax.numpy as jnp
import numpy as np
from jax import lax
from jax.experimental import pallas as pl
from jax.experimental.pallas import tpu as pltpu
from jax.sharding import PartitionSpec as P


def with_halo(cells, sides, width):
    for axis, dim in sides:
        count = lax.axis_size(axis)
        head = lax.slice_in_dim(cells, 0, width, axis=dim)
        tail = lax.slice_in_dim(cells, cells.shape[dim] - width, cells.shape[dim], axis=dim)
        cells = jnp.concatenate(
            [
                lax.ppermute(tail, axis, [(i, (i + 1) % count) for i in range(count)]),
                cells,
                lax.ppermute(head, axis, [((i + 1) % count, i) for i in range(count)]),
            ],
            axis=dim,
        )
    return cells


def legendre_table(points, order):
    columns = [points * 0.0 + 1.0, points]
    for degree in range(2, order + 1):
        columns.append(
            ((2 * degree - 1) * points * columns[-1] - (degree - 1) * columns[-2]) / degree
        )
    return np.stack(columns, axis=1)


def lobatto(count):
    order = count - 1
    points = np.cos(np.pi * np.arange(count) / order)
    for sweep in range(60):
        table = legendre_table(points, order)
        points = points - (points * table[:, order] - table[:, order - 1]) / (
            count * table[:, order]
        )
    table = legendre_table(points, order)
    weights = 2.0 / (order * count * table[:, order] ** 2)
    values = table[:, order]
    points, weights, values = (points[::-1], weights[::-1], values[::-1])
    spread = points[:, None] - points[None, :] + np.eye(count)
    deriv = values[:, None] / values[None, :] / spread * (1.0 - np.eye(count))
    corner = order * (order + 1) / 4.0
    ends = np.array([-corner] + [0.0] * (count - 2) + [corner])
    return (points, weights, deriv + np.eye(count) * ends[None, :])


def lagrange(fine_points, coarse_points):
    columns = []
    for column in range(len(coarse_points)):
        value = fine_points * 0.0 + 1.0
        for other in range(len(coarse_points)):
            if other != column:
                value = (
                    value
                    * (fine_points - coarse_points[other])
                    / (coarse_points[column] - coarse_points[other])
                )
        columns.append(value)
    return np.stack(columns, axis=1)


def edge_factor(count, blocks):
    index = jnp.arange(count)
    single = jnp.where((index == 0) | (index == count - 1), 0.5, 1.0).astype(jnp.float32)
    return jnp.tile(single, blocks)


def multiplicity(count, blocks):
    first = edge_factor(count, blocks[0])
    second = edge_factor(count, blocks[1])
    third = edge_factor(count, blocks[2])
    return first[:, None, None] * second[None, :, None] * third[None, None, :]


def element_apply(field, kappa, sigma, deriv, weights):
    count = deriv.shape[0]
    ex, ey, ez = kappa.shape
    high = lax.Precision.HIGHEST
    block = field.reshape(ex, count, ey, count, ez, count)
    mass = (weights[:, None, None] * weights[None, :, None] * weights[None, None, :])[
        None, :, None, :, None, :
    ]
    first = jnp.einsum("ai,eifjgk->eafjgk", deriv, block, precision=high)
    total = jnp.einsum("ai,eafjgk->eifjgk", deriv, first * mass, precision=high)
    second = jnp.einsum("aj,eifjgk->eifagk", deriv, block, precision=high)
    total = total + jnp.einsum("aj,eifagk->eifjgk", deriv, second * mass, precision=high)
    third = jnp.einsum("ak,eifjgk->eifjga", deriv, block, precision=high)
    total = total + jnp.einsum("ak,eifjga->eifjgk", deriv, third * mass, precision=high)
    coeff = kappa[:, None, :, None, :, None]
    shift = sigma[:, None, :, None, :, None]
    return (coeff * total + shift * mass * block).reshape(field.shape)


def element_diagonal(kappa, sigma, deriv, weights):
    count = deriv.shape[0]
    ex, ey, ez = kappa.shape
    stiff = jnp.sum(deriv * deriv * weights[:, None], axis=0)
    term = stiff[:, None, None] * weights[None, :, None] * weights[None, None, :]
    term = term + weights[:, None, None] * stiff[None, :, None] * weights[None, None, :]
    term = term + weights[:, None, None] * weights[None, :, None] * stiff[None, None, :]
    mass = weights[:, None, None] * weights[None, :, None] * weights[None, None, :]
    coeff = kappa[:, None, :, None, :, None]
    shift = sigma[:, None, :, None, :, None]
    full = coeff * term[None, :, None, :, None, :] + shift * mass[None, :, None, :, None, :]
    return full.reshape(ex * count, ey * count, ez * count)


def fold_axis(field, dim, count):
    size = field.shape[dim]
    position = jnp.arange(size) % count
    shape = [1, 1, 1]
    shape[dim] = size
    first = (position == 0).reshape(shape)
    last = (position == count - 1).reshape(shape)
    before = jnp.roll(field, 1, dim)
    after = jnp.roll(field, -1, dim)
    return field + jnp.where(first, before, 0.0) + jnp.where(last, after, 0.0)


def fold_padded(padded, dim, count):
    size = padded.shape[dim] - 2
    center = lax.slice_in_dim(padded, 1, size + 1, axis=dim)
    before = lax.slice_in_dim(padded, 0, size, axis=dim)
    after = lax.slice_in_dim(padded, 2, size + 2, axis=dim)
    position = jnp.arange(size) % count
    shape = [1, 1, 1]
    shape[dim] = size
    first = (position == 0).reshape(shape)
    last = (position == count - 1).reshape(shape)
    return center + jnp.where(first, before, 0.0) + jnp.where(last, after, 0.0)


def assemble(field, count, finest):
    if finest:
        padded = with_halo(field, (("gx", 0), ("gy", 1)), 1)
        field = fold_padded(fold_padded(padded, 0, count), 1, count)
    else:
        padded = with_halo(field, (("gx", 0), ("gy", 1)), 1)
        field = fold_padded(fold_padded(padded, 0, count), 1, count)
    return fold_axis(field, 2, count)


def restrict(field, interp, blocks, fine_count, coarse_count):
    high = lax.Precision.HIGHEST
    block = field.reshape(blocks[0], fine_count, blocks[1], fine_count, blocks[2], fine_count)
    one = jnp.einsum("ia,eifjgk->eafjgk", interp, block, precision=high)
    two = jnp.einsum("jb,eafjgk->eafbgk", interp, one, precision=high)
    three = jnp.einsum("kc,eafbgk->eafbgc", interp, two, precision=high)
    return three.reshape(
        blocks[0] * coarse_count, blocks[1] * coarse_count, blocks[2] * coarse_count
    )


def prolong(field, interp, blocks, fine_count, coarse_count):
    high = lax.Precision.HIGHEST
    block = field.reshape(blocks[0], coarse_count, blocks[1], coarse_count, blocks[2], coarse_count)
    one = jnp.einsum("ia,eafbgc->eifbgc", interp, block, precision=high)
    two = jnp.einsum("jb,eifbgc->eifjgc", interp, one, precision=high)
    three = jnp.einsum("kc,eifjgc->eifjgk", interp, two, precision=high)
    return three.reshape(blocks[0] * fine_count, blocks[1] * fine_count, blocks[2] * fine_count)


def distributed(forcing, kappa, sigma):
    blocks = kappa.shape
    counts = [8, 4, 2]
    tables = [lobatto(count) for count in counts]
    derivs = [jnp.asarray(table[2], jnp.float32) for table in tables]
    weights = [jnp.asarray(table[1], jnp.float32) for table in tables]
    interps = [
        jnp.asarray(lagrange(tables[level][0], tables[level + 1][0]), jnp.float32)
        for level in range(2)
    ]
    mults = [multiplicity(count, blocks) for count in counts]
    diags = [
        assemble(
            element_diagonal(kappa, sigma, derivs[level], weights[level]), counts[level], level == 0
        )
        for level in range(3)
    ]
    center = 1.65
    half = 1.35
    ratio = center / half

    def operate(field, level):
        return assemble(
            element_apply(field, kappa, sigma, derivs[level], weights[level]),
            counts[level],
            level == 0,
        )

    def smooth(resid, level, steps, keep_last):
        rho = 1.0 / ratio
        direction = resid / (center * diags[level])
        iterate = direction
        for step in range(steps):
            if step > 0:
                rho_next = 1.0 / (2.0 * ratio - rho)
                direction = (
                    rho_next * rho * direction + 2.0 * rho_next / half * resid / diags[level]
                )
                iterate = iterate + direction
                rho = rho_next
            if step < steps - 1 or keep_last:
                resid = resid - operate(direction, level)
        return (iterate, resid)

    def vcycle(resid, level):
        if level == 2:
            iterate, unused = smooth(resid, level, 2, False)
            return iterate
        iterate, resid = smooth(resid, level, 2, True)
        coarse = assemble(
            restrict(
                mults[level] * resid, interps[level], blocks, counts[level], counts[level + 1]
            ),
            counts[level + 1],
            False,
        )
        correction = prolong(
            vcycle(coarse, level + 1), interps[level], blocks, counts[level], counts[level + 1]
        )
        iterate = iterate + correction
        resid = resid - operate(correction, level)
        return iterate + resid / (center * diags[level])

    load = assemble(forcing, 8, True)
    first = vcycle(load, 0)
    image_first = operate(first, 0)
    second = vcycle(load - image_first, 0)
    combined = first + second
    image = operate(combined, 0)
    weight = mults[0]
    load_sq, load_image, image_sq = lax.psum(
        (
            jnp.sum(weight * load * load),
            jnp.sum(weight * load * image),
            jnp.sum(weight * image * image),
        ),
        ("gx", "gy"),
    )
    coef = load_image / image_sq
    solution = coef * combined
    residual = load - coef * image
    rel_residual = jnp.sqrt((load_sq - load_image * load_image / image_sq) / load_sq)
    return (solution, residual, rel_residual)


THETA = 1.65
DELTA = 1.35
RATIO = THETA / DELTA
RHO0 = 1.0 / RATIO
RHO1 = 1.0 / (2.0 * RATIO - RHO0)
KEEP = RHO1 * RHO0
PUSH = 2.0 * RHO1 / DELTA
LANES = 128
SUBS = 8


def triple(first, second, third):
    return np.kron(first, np.kron(second, third))


def split_const(matrix):
    high = matrix.astype(jnp.bfloat16)
    low = (matrix - high.astype(np.float64)).astype(jnp.bfloat16)
    return high, low


def stacked(matrix):
    high, low = split_const(matrix)
    return np.concatenate([high, high, low], axis=1)


J_ORDER = (0, 1, 2, 3, 7, 5, 6, 4)
SPLIT_AT = ((0, 1), (2, 1))
PAIRS = ((0, 7), (1, 2), (3, 4), (5, 6))
FACE = (0, 1, 3, 2)
ROWS1 = tuple(
    (k * 4 + FACE[2 * ih + il]) * 4 + FACE[2 * jh + jl]
    for k in range(4) for ih in range(2) for jh in range(2) for il in range(2) for jl in range(2)
)
ROWS2 = tuple((k * 2 + i) * 2 + j for j in range(2) for k in range(2) for i in range(2))


def padded(matrix, rows, columns):
    return np.pad(matrix, ((0, rows - matrix.shape[0]), (0, columns - matrix.shape[1])))


class Tables:
    def __init__(self):
        tables = [lobatto(count) for count in (8, 4, 2)]
        self.weights = [table[1] for table in tables]
        stiff = [table[2].T @ np.diag(table[1]) @ table[2] for table in tables]
        self.squares = [np.sum(t[2] * t[2] * t[1][:, None], axis=0) for t in tables]
        interps = [lagrange(tables[level][0], tables[level + 1][0]) for level in range(2)]
        factor = [np.where((np.arange(n) == 0) | (np.arange(n) == n - 1), 0.5, 1.0) for n in (8, 4)]
        down = [interps[level].T * factor[level][None, :] for level in range(2)]
        flat = [i for pair in PAIRS for i in pair]
        rows0 = [(k * 8 + i) * 8 + j for k in range(8) for i in range(8) for j in J_ORDER]
        data0 = [(k * 8 + i) * 8 + j for k in range(8) for i in flat for j in J_ORDER]
        rows1, rows2 = list(ROWS1), list(ROWS2)
        w, k = np.diag(self.weights[0]), stiff[0]
        plane = np.kron(k, w) + np.kron(w, k)
        both = np.kron(w, w)
        flip = k[:4, ::-1][:, :4]
        half = np.kron(0.5 * w[:4, :4], plane)
        even = np.kron(0.5 * (k[:4, :4] + flip), both) + half
        odd = np.kron(0.5 * (k[:4, :4] - flip), both) + half
        self.even = stacked(even[np.ix_(rows0[:256], data0[:256])])
        self.odd = stacked(odd[np.ix_(rows0[:256], data0[:256])])
        high, low = split_const(triple(down[0], down[0], down[0])[np.ix_(rows1, data0)])
        self.down0 = np.concatenate([high, low], axis=0)
        up = triple(interps[0], interps[0], interps[0])
        stiffness = np.kron(k, both) + np.kron(w, plane)
        self.up0 = stacked(np.concatenate([up[np.ix_(rows0, rows1)], (stiffness @ up)[np.ix_(rows0, rows1)]]))
        w, k = np.diag(self.weights[1]), stiff[1]
        stiffness = triple(k, w, w) + triple(w, k, w) + triple(w, w, k)
        up = triple(interps[1], interps[1], interps[1])
        self.op1 = stacked(stiffness[np.ix_(rows1, rows1)])
        self.down1 = padded(stacked(triple(down[1], down[1], down[1])[np.ix_(rows2, rows1)]), 16, 192)
        self.up1 = padded(stacked(
            np.concatenate([up[np.ix_(rows1, rows2)], (stiffness @ up)[np.ix_(rows1, rows2)]])), 128, 32)
        w, k = np.diag(self.weights[2]), stiff[2]
        op2 = (triple(k, w, w) + triple(w, k, w) + triple(w, w, k))[np.ix_(rows2, rows2)]
        wide = lambda column: np.repeat(np.asarray(column, np.float32)[:, None], LANES, axis=1)
        blocks = [wide(self.weights[0][list(J_ORDER)]), wide(self.squares[0][list(J_ORDER)]),
                  wide(factor[0][list(J_ORDER)])]
        for level, order in ((1, rows1), (2, rows2)):
            a, b = self.weights[level], self.squares[level]
            blocks.append(wide(triple(a, a, a)[order]))
            blocks.append(wide((triple(b, a, a) + triple(a, b, a) + triple(a, a, b))[order]))
        at = np.arange(SUBS)
        self.op2 = np.concatenate([wide(op2[at, (at - turn) % SUBS]) for turn in range(SUBS)], axis=0)
        self.rows = np.concatenate(blocks, axis=0)


def gather_rounds(nx, ny):
    dims = []
    step = nx // 2
    while step > 1:
        dims.append((step, 0))
        step //= 2
    if ny > 1:
        dims.insert(len(dims) - 1, (0, 1))
    return [dims[n:n + 2] for n in range(0, len(dims), 2)]


def swap_rows(x, sub):
    return jnp.where(sub == 4, pltpu.roll(x, 5, 0), jnp.where(sub == 7, pltpu.roll(x, 3, 0), x))


def kernel(nx, ny, tables, near, far, *refs):
    count = (len(refs) - 19) // 2
    sources, rest = refs[:count], refs[count:]
    copies = [pltpu.make_async_copy(source, place, rest[-1].at[n])
              for n, (source, place) in enumerate(zip(sources, rest[-1 - count:-1]))]
    for copy in reversed(copies):
        copy.start()
    solve(nx, ny, tables, near, far, copies, *rest[-1 - count:-1], *rest[:-1 - count])


def solve(nx, ny, tables, near, far, copies, even, odd, down0, up0, op1, down1, up1, op2, rows,
           sol_ref, res_ref, rel_ref, b_ref, r_ref, d_ref, other_ref, v_ref, p_ref, t_ref, a_ref, z_ref,
           be_ref, bo_ref, c_ref, lane_ref, low_ref, cor_ref):
    groups = nx // SUBS
    tiles = ny * groups
    part_wide = ny * LANES
    wide = tiles * LANES
    own_x, own_y = lax.axis_index("gx"), lax.axis_index("gy")
    sub = lax.broadcasted_iota(jnp.int32, (SUBS, LANES), 0)
    lanes = lax.broadcasted_iota(jnp.int32, (SUBS, LANES), 1)
    lane = lanes % SUBS
    w = [float(x) for x in tables.weights[0]]
    q = [float(x) for x in tables.squares[0]]
    parts = range(groups)

    def cut(x):
        return [x[:, t * LANES:(t + 1) * LANES] for t in range(x.shape[1] // LANES)]

    def join(pieces):
        return jnp.concatenate(pieces, axis=1)

    def ls(p):
        return slice(p * part_wide, (p + 1) * part_wide)

    def split_parts(x):
        return [x[:, ls(p)] for p in parts]

    def across(x, count):
        return join([x] * count)

    sub_w = across(sub, tiles)
    sub_p = across(sub, ny)

    def move(x, amount):
        amount %= LANES
        return join([pltpu.roll(t, amount, 1) for t in cut(x)]) if amount else x

    def x_up(x, p, more=0):
        if p:
            return move(x[p - 1], more)
        prev = cut(x[groups - 1])
        return join([jnp.where(lane == 0, pltpu.roll(t, (LANES - SUBS + 1 + more) % LANES, 1),
                               pltpu.roll(t, 1 + more, 1)) for t in prev])

    def x_down(x, p, more=0):
        if p < groups - 1:
            return move(x[p + 1], more)
        succ = cut(x[0])
        return join([jnp.where(lane == SUBS - 1, pltpu.roll(t, SUBS - 1 + more, 1),
                               pltpu.roll(t, (LANES - 1 + more) % LANES, 1)) for t in succ])

    up, down = SUBS, LANES - SUBS

    def y_fold(x, face):
        t = cut(x)
        other = join([t[(n // ny) * ny + (n + 1) % ny] for n in range(len(t))])
        return x + jnp.where(face, pltpu.roll(other, 4, 0), 0.0)

    face0 = sub_p % 4 == 0
    face1 = sub_w % 2 == 0

    def row(k, i):
        return pl.ds(k * 64 + i * 8, 8)

    for t in range(tiles):
        part, y_index = t // ny, t % ny
        at = slice(t * LANES, (t + 1) * LANES)
        use_near = ((part ^ own_x) & 1) == 0
        slots = []
        for c in range(SUBS):
            delta = (c * groups + part) ^ own_x
            slot, size = jnp.int32(0), 1
            for dims in gather_rounds(nx, ny):
                flags = [y_index ^ own_y if along_y else jnp.where((delta & along_x) != 0, 1, 0)
                         for along_x, along_y in dims]
                if len(dims) == 2:
                    place = flags[0] * 2 + flags[1] * 3 - flags[0] * flags[1] * 4
                else:
                    place = flags[0]
                slot = slot + place * size
                size *= 1 << len(dims)
            slots.append(slot)
        blocks = [[jnp.where(use_near, near[slot, i], far[slot, i]) for slot in slots]
                  for i in range(8)]
        for step in (1, 2, 4):
            keep = (lane & step) == 0
            low = [c for c in range(SUBS) if not c & step]
            turned = [[jnp.take_along_axis(jnp.where(keep, b[c + step], b[c]), lanes ^ step, axis=1)
                       for c in low] for b in blocks]
            fresh = []
            for b, turn in zip(blocks, turned):
                out = list(b)
                for c, x in zip(low, turn):
                    out[c] = jnp.where(keep, b[c], x)
                    out[c + step] = jnp.where(keep, x, b[c + step])
                fresh.append(out)
            blocks = fresh
        for i, b in enumerate(blocks):
            for k in range(7):
                v_ref[row(k, i), at] = b[k]
            v_ref[row(7, i), at] = pltpu.roll(b[0], down, 1)
        lane_ref[0:8, at] = blocks[0][7]
    copies[-1].wait()
    kap1 = lane_ref[0:1, :]
    sig1 = lane_ref[1:2, :]
    w_j = across(rows[0:8, :], ny)
    q_j = across(rows[8:16, :], ny)
    f_j = across(rows[16:24, :], tiles)
    kap = [jnp.broadcast_to(kap1[:, ls(p)], (SUBS, part_wide)) for p in parts]
    sig_w = [jnp.broadcast_to(sig1[:, ls(p)], (SUBS, part_wide)) * w_j for p in parts]

    def split(value):
        high = value.astype(jnp.bfloat16)
        return high, (value - high.astype(jnp.float32)).astype(jnp.bfloat16)

    def store_split(kk, index, p, low_pair, high_pair):
        a = jnp.concatenate(low_pair, axis=0)
        b = jnp.concatenate(high_pair, axis=0)
        for ref, value in ((be_ref, a + b), (bo_ref, a - b)):
            high, low = split(value)
            at = kk * 64 + index * 16
            ref[at:at + 16, ls(p)] = high
            ref[256 + at:272 + at, ls(p)] = low

    def fold_z(kk, pair):
        a, b = pair
        return (a + move(b, up), b + move(a, down)) if kk == 0 else (a, b)

    def inner(p, kk, index, get, with_z=True):
        out = []
        for i in PAIRS[index]:
            pair = get(p, kk, i)
            pair = fold_z(kk, pair) if with_z else pair
            out.append([y_fold(x, face0) for x in pair])
        return out

    def faces(kk, get, with_z=True):
        first, last = [], []
        for p in parts:
            a, b = get(p, kk, 0), get(p, kk, 7)
            first.append(fold_z(kk, a) if with_z else a)
            last.append(fold_z(kk, b) if with_z else b)
        out = []
        for p in parts:
            a, b = [], []
            for s in range(2):
                firsts, lasts = [x[s] for x in first], [x[s] for x in last]
                a.append(y_fold(firsts[p] + x_up(lasts, p), face0))
                b.append(y_fold(lasts[p] + x_down(firsts, p), face0))
            out.append([a, b])
        return out

    pending = []

    def flush():
        while pending:
            pending.pop(0)()

    def walk(get, handle, after, with_z=True):
        for p in parts:
            for kk in range(4):
                for index in (1, 2, 3):
                    if pending and (kk, index) in SPLIT_AT:
                        pending.pop(0)()
                    handle(p, kk, index, inner(p, kk, index, get, with_z))
            flush()
            if p == 0:
                for kk in range(4):
                    for n, values in enumerate(faces(kk, get, with_z)):
                        handle(n, kk, 0, values)
            pending.extend(after(p))

    def dot(a, b):
        return jnp.dot(a, b, preferred_element_type=jnp.float32)

    def rows_of(ref, p):
        return jnp.concatenate([ref[:, ls(p)], ref[0:256, ls(p)]], axis=0)

    def multiply(p):
        def first():
            a_ref[0:256, ls(p)] = dot(even[...], rows_of(be_ref, p))

        def second():
            a_ref[256:512, ls(p)] = dot(odd[...], rows_of(bo_ref, p))

        return first, second

    def point(p, kk, i):
        out = []
        for k in (kk, 7 - kk):
            s1 = q[k] * w[i] + w[k] * q[i]
            s2 = w[k] * w[i]
            out.append(kap[p] * (s1 * w_j + s2 * q_j) + s2 * sig_w[p])
        return out

    def put_diag(p, kk, index, values):
        for s, k in enumerate((kk, 7 - kk)):
            for n, i in enumerate(PAIRS[index]):
                inverse = 1.0 / values[n][s]
                p_ref[row(k, i), ls(p)] = inverse * PUSH
                t_ref[row(k, i), ls(p)] = inverse * (1.0 / THETA)

    def put_load(p, kk, index, values):
        dirs = []
        for s, k in enumerate((kk, 7 - kk)):
            group = []
            for n, i in enumerate(PAIRS[index]):
                at = (row(k, i), ls(p))
                b_ref[at] = values[n][s]
                r_ref[at] = values[n][s]
                group.append(values[n][s] * t_ref[at])
                d_ref[at] = group[-1]
            dirs.append(group)
        store_split(kk, index, p, dirs[0], dirs[1])

    walk(point, put_diag, lambda p: ())
    for copy in copies[:-1]:
        copy.wait()
    walk(lambda p, kk, i: (v_ref[row(kk, i), ls(p)], v_ref[row(7 - kk, i), ls(p)]),
         put_load, multiply, with_z=False)

    low_face = (sub_w // 2) % 2 == 0

    def x_up_all(x, more=0):
        return join([x_up(split_parts(x), p, more) for p in parts])

    def x_down_all(x, more=0):
        return join([x_down(split_parts(x), p, more) for p in parts])

    def fold1(x):
        c = [(x[16 * k:16 * k + 8], x[16 * k + 8:16 * k + 16]) for k in range(4)]
        out = []
        for k, (a, b) in enumerate(c):
            na, nb = x_up_all(b), x_down_all(a)
            if k in (0, 3):
                g, h = c[3 - k]
                amount = up if k == 0 else down
                na = na + x_up_all(h, amount)
                nb = nb + x_down_all(g, amount)
                a, b = a + move(g, amount), b + move(h, amount)
            out.append(y_fold(a + jnp.where(low_face, na, 0.0), face1))
            out.append(y_fold(b + jnp.where(low_face, nb, 0.0), face1))
        return jnp.concatenate(out, axis=0)

    first_k = (sub_w // 2) % 2 == 0
    first_i = sub_w % 2 == 0

    def fold2(x):
        other_k = jnp.where(first_k, pltpu.roll(x, 6, 0), pltpu.roll(x, 2, 0))
        other_i = jnp.where(first_i, pltpu.roll(x, 7, 0), pltpu.roll(x, 1, 0))
        both = jnp.where(first_i, pltpu.roll(other_k, 7, 0), pltpu.roll(other_k, 1, 0))
        x = x + jnp.where(first_k, move(other_k, up), move(other_k, down))
        x = x + jnp.where(first_i, x_up_all(other_i), x_down_all(other_i))
        x = x + jnp.where(first_k, jnp.where(first_i, x_up_all(both, up), x_down_all(both, up)),
                          jnp.where(first_i, x_up_all(both, down), x_down_all(both, down)))
        return y_fold(x, sub_w >= 0)

    def cat3(x):
        high, low = split(x)
        return jnp.concatenate([high, low, high], axis=0)

    def cat3_small(x):
        high = x.astype(jnp.bfloat16).astype(jnp.float32)
        return jnp.concatenate([high, x - high, high, jnp.zeros_like(x)], axis=0).astype(jnp.bfloat16)

    mass1 = across(rows[24:88, :], tiles)
    point1 = across(rows[88:152, :], tiles)
    mass2 = across(rows[152:160, :], tiles)
    point2 = across(rows[160:168, :], tiles)
    inv1_ref, mass1_ref = lane_ref.at[8:72, :], lane_ref.at[72:136, :]
    inv1_ref[...] = 1.0 / fold1(kap1 * point1 + sig1 * mass1)
    mass1_ref[...] = sig1 * mass1
    lane_ref[136:144, :] = 1.0 / fold2(kap1 * point2 + sig1 * mass2)
    lane_ref[144:152, :] = sig1 * mass2

    def apply1(v):
        return fold1(kap1 * dot(op1[...], cat3(v)) + mass1_ref[...] * v)

    def apply2(v):
        terms = [across(op2[8 * n:8 * n + 8, :], tiles) * (pltpu.roll(v, n, 0) if n else v)
                 for n in range(SUBS)]
        while len(terms) > 1:
            terms = [x + y for x, y in zip(terms[::2], terms[1::2])]
        return fold2(kap1 * terms[0] + lane_ref[144:152, :] * v)

    def coarse(resid):
        inverse = inv1_ref[...]
        d = resid * inverse * (1.0 / THETA)
        x = d
        resid = resid - apply1(d)
        d = KEEP * d + PUSH * (resid * inverse)
        x = x + d
        resid = resid - apply1(d)
        low = fold2(dot(down1[...], cat3(resid))[0:8])
        inverse2 = lane_ref[136:144, :]
        d = low * inverse2 * (1.0 / THETA)
        y = d
        low = low - apply2(d)
        y = y + KEEP * d + PUSH * (low * inverse2)
        both = dot(up1[...], cat3_small(y))
        e = both[0:64]
        x = x + e
        resid = resid - fold1(kap1 * both[64:128] + mass1_ref[...] * e)
        return x + resid * inverse * (1.0 / THETA)

    d_refs = [d_ref, other_ref]

    def turn_over():
        d_refs.reverse()

    def weighted(p, kk, i, a, b):
        scale = sig_w[p] * (w[kk] * w[i])
        return (kap[p] * a + scale * d_refs[0][row(kk, i), ls(p)],
                kap[p] * b + scale * d_refs[0][row(7 - kk, i), ls(p)])

    def from_halves(p, kk, i):
        e = a_ref[row(kk, i), ls(p)]
        o = a_ref[row(4 + kk, i), ls(p)]
        return weighted(p, kk, i, e + o, e - o)

    def from_whole(p, kk, i):
        return weighted(p, kk, i, a_ref[row(kk, i), ls(p)], a_ref[row(7 - kk, i), ls(p)])

    def lower(at, value):
        r = r_ref[at] - value
        r_ref[at] = r
        return r

    def second_direction(at, value):
        return KEEP * d_refs[0][at] + lower(at, value) * p_ref[at]

    def next_direction(at, value):
        return lower(at, value) * t_ref[at]

    def put(update):
        def handle(p, kk, index, values):
            dirs = []
            for s, k in enumerate((kk, 7 - kk)):
                group = []
                for n, i in enumerate(PAIRS[index]):
                    at = (row(k, i), ls(p))
                    group.append(update(at, values[n][s]))
                    d_refs[1][at] = group[-1]
                dirs.append(group)
            store_split(kk, index, p, dirs[0], dirs[1])
        return handle

    def put_resid(p, kk, index, values):
        for s, k in enumerate((kk, 7 - kk)):
            pair = [lower((row(k, i), ls(p)), values[n][s]) for n, i in enumerate(PAIRS[index])]
            high, low = split(jnp.concatenate(pair, axis=0))
            at = k * 64 + index * 16
            c_ref[at:at + 16, ls(p)] = high
            c_ref[512 + at:528 + at, ls(p)] = low

    def put_last(p, kk, index, values):
        for s, k in enumerate((kk, 7 - kk)):
            for n, i in enumerate(PAIRS[index]):
                lower((row(k, i), ls(p)), values[n][s])

    window = pl.ds(pl.multiple_of((own_x % groups * ny + own_y) * LANES, LANES), LANES)
    z_ref[...] = jnp.zeros((512, LANES), jnp.float32)

    def collect():
        z_ref[...] = z_ref[...] + d_refs[0][:, window]

    for step in range(2):
        collect()
        walk(from_halves, put(second_direction), multiply)
        turn_over()
        collect()
        def reduce(p):
            def first():
                both = dot(down0[...], c_ref[0:512, ls(p)])
                low_ref[:, ls(p)] = both[0:64] + both[64:128]

            def second():
                low_ref[:, ls(p)] = low_ref[:, ls(p)] + dot(down0[0:64, :], c_ref[512:1024, ls(p)])

            return first, second

        walk(from_halves, put_resid, reduce)
        flush()
        cor_ref[...] = cat3(coarse(fold1(low_ref[...])))
        turn_over()
        for p in parts:
            d_refs[0][:, ls(p)] = dot(up0[0:512, :], cor_ref[:, ls(p)])
            a_ref[:, ls(p)] = dot(up0[512:1024, :], cor_ref[:, ls(p)])
        collect()
        walk(from_whole, put(next_direction), multiply)
        turn_over()
        collect()
        if step == 0:
            walk(from_halves, put(next_direction), multiply)
            turn_over()
        else:
            walk(from_halves, put_last, lambda p: ())

    zero = jnp.zeros((SUBS, wide), jnp.float32)
    sums = [[zero] * 4 for weight in range(3)]
    for k in range(8):
        for i in range(8):
            b = b_ref[row(k, i), :]
            r = r_ref[row(k, i), :]
            image_all = b - r
            group = sums[(k in (0, 7)) + (i in (0, 7))]
            for n, (x, y) in enumerate(((r, image_all), (image_all, image_all), (r, r), (b, b))):
                group[n] = group[n] + x * y
    rw, ww, rr, bb = [jnp.sum((a + 0.5 * b + 0.25 * c) * f_j) for a, b, c in zip(*sums)]
    excess = rw / ww
    coef = 1.0 + excess
    rr = rr - rw * excess
    rel_ref[0] = jnp.sqrt(rr / bb)
    place = own_x // groups
    for i in range(8):
        sol = jnp.zeros((SUBS, LANES), jnp.float32)
        res = sol
        for k in range(8):
            r = r_ref[row(k, i), window]
            r = r - excess * (b_ref[row(k, i), window] - r)
            turn = (k - place) % LANES
            sol = jnp.where(lane == k, pltpu.roll(z_ref[row(k, i), :], turn, 1), sol)
            res = jnp.where(lane == k, pltpu.roll(r, turn, 1), res)
        sol_ref[i] = swap_rows(coef * sol, sub)
        res_ref[i] = swap_rows(res, sub)


def solve_all(nx, ny, near, far):
    tables = Tables()
    wide = ny * nx // SUBS * LANES
    consts = [tables.even, tables.odd, tables.down0, tables.up0, tables.op1, tables.down1,
              tables.up1, tables.op2, tables.rows]
    vmem = pl.BlockSpec(memory_space=pltpu.VMEM)
    field = pltpu.VMEM((512, wide), jnp.float32)
    return pl.pallas_call(
        lambda *refs: kernel(nx, ny, tables, *refs),
        in_specs=[vmem] * 2 + [pl.BlockSpec(memory_space=pltpu.HBM)] * len(consts),
        out_specs=[vmem, vmem, pl.BlockSpec(memory_space=pltpu.SMEM)],
        out_shape=[
            jax.ShapeDtypeStruct(near.shape[1:], jnp.float32),
            jax.ShapeDtypeStruct(near.shape[1:], jnp.float32),
            jax.ShapeDtypeStruct((1,), jnp.float32),
        ],
        scratch_shapes=[
            field, field, field, field, field, field, field, field,
            pltpu.VMEM((512, LANES), jnp.float32),
            pltpu.VMEM((512, wide), jnp.bfloat16), pltpu.VMEM((512, wide), jnp.bfloat16),
            pltpu.VMEM((1024, wide), jnp.bfloat16), pltpu.VMEM((152, wide), jnp.float32),
            pltpu.VMEM((64, wide), jnp.float32), pltpu.VMEM((192, wide), jnp.bfloat16),
            *[pltpu.VMEM(c.shape, c.dtype) for c in consts],
            pltpu.SemaphoreType.DMA((len(consts),)),
        ],
        name="solve_all",
    )(*[pltpu.with_memory_space_constraint(x, pltpu.VMEM) for x in (near, far)],
      *[jnp.asarray(c) for c in consts])


def pack_kernel(forcing, kappa, sigma, out_ref, coef_ref):
    sub = lax.broadcasted_iota(jnp.int32, (SUBS, LANES), 0)
    lane = lax.broadcasted_iota(jnp.int32, (SUBS, LANES), 1)
    count = kappa.shape[2]
    coef_ref[...] = jnp.zeros((SUBS, LANES), jnp.float32)
    coef_ref[0:1, 0:count] = kappa[0]
    coef_ref[1:2, 0:count] = sigma[0]
    spread = jnp.take_along_axis(coef_ref[...], lane // SUBS, axis=1)
    for i in range(SUBS):
        x = swap_rows(forcing[i], sub)
        x = x + jnp.where(lane % SUBS == 0, pltpu.roll(x, 1, 1), 0.0)
        if i == 0:
            x = jnp.where(lane % SUBS == SUBS - 1, spread, x)
        out_ref[0, i] = x


def packed_block(forcing, kappa, sigma):
    vmem = pl.BlockSpec(memory_space=pltpu.VMEM)
    return pl.pallas_call(
        pack_kernel,
        in_specs=[vmem] * 3,
        out_specs=vmem,
        out_shape=pltpu.VMEM((1, *forcing.shape), jnp.float32),
        scratch_shapes=[pltpu.VMEM((SUBS, LANES), jnp.float32)],
        name="pack_block",
    )(forcing, kappa, sigma)


def gathered(forcing, kappa, sigma):
    nx, ny = lax.axis_size("gx"), lax.axis_size("gy")

    def swap(block, along_x, along_y):
        pairs = [(a * ny + b, (a ^ along_x) * ny + (b ^ along_y)) for a in range(nx) for b in range(ny)]
        return lax.ppermute(block, ("gx", "gy"), pairs)

    block = packed_block(forcing, kappa, sigma)
    for dims in gather_rounds(nx, ny):
        if len(dims) == 2:
            (x0, y0), (x1, y1) = dims
            masks = [(x0 ^ x1, y0 ^ y1), dims[0], dims[1]]
        else:
            masks = dims
        block = jnp.concatenate([block] + [swap(block, *mask) for mask in masks], axis=0)
    sol, res, rel = solve_all(nx, ny, block, swap(block, 1, 0))
    return sol, res, rel.reshape(())


def fits_one_device(mesh):
    nx, ny = mesh.shape["gx"], mesh.shape["gy"]
    power = nx & (nx - 1) == 0
    return power and nx % SUBS == 0 and ny <= 2 and nx * ny <= 64


def solution(mesh):
    spec = P("gx", "gy", None)
    small = fits_one_device(mesh)

    def local(forcing, kappa, sigma):
        plain = forcing.shape == (SUBS, SUBS, LANES) and kappa.shape == (1, 1, LANES // SUBS)
        return (gathered if small and plain else distributed)(forcing, kappa, sigma)

    return jax.shard_map(
        local, mesh=mesh, in_specs=(spec, spec, spec), out_specs=(spec, spec, P()),
        check_vma=False,
    )
```
